32 devices in a mesh: img: 4 (over y, core), depth: 8 (over z, x).
Axes of the slice: x: 2, y: 2, z: 4, core: 2. Of those that a mesh axis runs over, the one named last changes fastest.
Arguments:
- counts: int32 [256, 256, 512], P('depth', 'img'), may hold values from 0 to 5, as said below
Outputs:
- image: float32 [4, 256, 512], P(None, ('img', 'depth'))
The draws below stay inside these ranges and needn't reach their ends.
Inputs may be any that keep to these rules, and one draw needn't show every extreme that they name: `counts`: whole numbers of atoms.
All inputs are finite; a program needn't handle non-finite values.
Results may differ from the reference program's by a relative error of at most 0.0003.
Values sent between devices are 32-bit elements; how exact they have to be, the bound alone decides.
No kernel may reach another device: no remote copies, remote signals or barrier semaphores. Data moves between devices by JAX's collectives and lax.ppermute only.
A program may use at most 64 MiB of HBM per device.

```python
import math
import jax
import jax.numpy as jnp
from jax import lax

CX = 64
NX = 256
NY = 512
NZ = 256


def piecewise_counts(seed_key, depth_cell, row_cell, column_cell, levels):
    coarse = jax.random.randint(seed_key, (NZ // depth_cell + 2, NX // row_cell + 2, NY // column_cell + 2), 0, levels, dtype=jnp.int32)
    spread_out = jnp.repeat(jnp.repeat(jnp.repeat(coarse, depth_cell, 0), row_cell, 1), column_cell, 2)
    start_key = jax.random.fold_in(seed_key, 7)
    depth_start = jax.random.randint(jax.random.fold_in(start_key, 1), (), 0, depth_cell, dtype=jnp.int32)
    row_start = jax.random.randint(jax.random.fold_in(start_key, 2), (), 0, row_cell, dtype=jnp.int32)
    column_start = jax.random.randint(jax.random.fold_in(start_key, 3), (), 0, column_cell, dtype=jnp.int32)
    return lax.dynamic_slice(spread_out, (depth_start, row_start, column_start), (NZ, NX, NY))


def draw_counts(key, part):
    broad_part = piecewise_counts(jax.random.fold_in(key, 11), 32, 32, 32, 2)
    layer_part = piecewise_counts(jax.random.fold_in(key, 12), 1, 8, 8, 4)
    row_part = piecewise_counts(jax.random.fold_in(key, 14), 32, 1, 8, 3)
    jitter = jax.random.randint(jax.random.fold_in(key, 13), (NZ, NX, NY), 0, 2, dtype=jnp.int32)
    values = jnp.clip(broad_part + layer_part + row_part + jitter - 1, 0, 5)
    values = values.at[0, 0, 0].set(0)
    values = values.at[NZ - 1, NX - 1, NY - 1].set(5)
    return values.astype(jnp.int32)


def setup_inputs(seed: int = 0) -> dict:
    key_of = jax.random.split(jax.random.key(seed), 2)
    return {
        "counts": draw_counts(jax.random.fold_in(key_of[1], 71), 0),
    }


gauss_taps = [math.exp(-offset * offset / 8.0) / sum(math.exp(-other * other / 8.0) for other in range(-4, 5)) for offset in range(-4, 5)]
light_z = 0.48
light_x = 0.6
light_y = 0.64


def smooth_valid(values, axis):
    length = values.shape[axis] - 8
    total = gauss_taps[0] * lax.slice_in_dim(values, 0, length, axis=axis)
    for offset in range(1, 9):
        total = total + gauss_taps[offset] * lax.slice_in_dim(values, offset, offset + length, axis=axis)
    return total


def smooth_last(values):
    widths = [(0, 0)] * (values.ndim - 1) + [(4, 4)]
    return smooth_valid(jnp.pad(values, widths), values.ndim - 1)


def render_terms(smooth_ext, depth_total):
    smoothed = smooth_ext[1:-1, 1:-1, :]
    grad_z = 0.5 * (smooth_ext[2:, 1:-1, :] - smooth_ext[:-2, 1:-1, :])
    grad_x = 0.5 * (smooth_ext[1:-1, 2:, :] - smooth_ext[1:-1, :-2, :])
    padded = jnp.pad(smoothed, ((0, 0), (0, 0), (1, 1)))
    grad_y = 0.5 * (padded[:, :, 2:] - padded[:, :, :-2])
    shading = 0.55 + 0.45 * jnp.tanh(3.0 * (light_z * grad_z + light_x * grad_x + light_y * grad_y))
    gradient_sq = grad_z * grad_z + grad_x * grad_x + grad_y * grad_y
    optical = (1.5 / depth_total) * smoothed * smoothed / (1.0 + smoothed * smoothed) * (1.0 + 4.0 * gradient_sq)
    sigma_red = jax.nn.sigmoid(2.0 * (smoothed - 2.5))
    red_light = shading * sigma_red
    green_light = shading * jnp.exp(-(smoothed - 2.5) ** 2)
    blue_light = shading * (1.0 - sigma_red)
    return optical, red_light, green_light, blue_light


def integrate(optical, red_light, green_light, blue_light):
    before = jnp.cumsum(optical, axis=0) - optical
    weight = jnp.exp(-before) * (1.0 - jnp.exp(-optical))
    colors = jnp.stack([jnp.sum(weight * red_light, 0), jnp.sum(weight * green_light, 0), jnp.sum(weight * blue_light, 0)], 0)
    transmit = jnp.exp(-jnp.sum(optical, 0))
    return colors, transmit


def reference(counts):
    density = counts.astype(jnp.float32)
    depth_total, rows_total, columns = density.shape
    padded = jnp.pad(density, ((0, 0), (5, 5), (0, 0)))

    def one_block(block_number):
        offset = (block_number * CX).astype(jnp.int32)
        window_field = lax.dynamic_slice_in_dim(padded, offset, CX + 10, 1)
        window_field = smooth_last(window_field)
        window_field = smooth_valid(window_field, 1)
        window_field = smooth_valid(jnp.pad(window_field, ((4, 4), (0, 0), (0, 0))), 0)
        x_cells = offset - 1 + jnp.arange(CX + 2, dtype=jnp.int32)
        inside = (x_cells >= 0) & (x_cells < rows_total)
        window_field = jnp.where(inside[None, :, None], window_field, jnp.zeros_like(window_field))
        smooth_ext = jnp.pad(window_field, ((1, 1), (0, 0), (0, 0)))
        colors, transmit = integrate(*render_terms(smooth_ext, depth_total))
        return jnp.concatenate([colors, (1.0 - transmit)[None]], 0)

    blocks = lax.map(one_block, jnp.arange(rows_total // CX, dtype=jnp.int32))
    return jnp.transpose(blocks, (1, 0, 2, 3)).reshape(4, rows_total, columns)
```

```python
import functools
import math

import jax
import jax.numpy as jnp
import numpy as np
from jax import lax
from jax.experimental import pallas as pl
from jax.experimental.pallas import tpu as pltpu
from jax.sharding import PartitionSpec as P

gauss_taps = [
    math.exp(-offset * offset / 8.0)
    / sum((math.exp(-other * other / 8.0) for other in range(-4, 5)))
    for offset in range(-4, 5)
]
light_z = 0.48
light_x = 0.6
light_y = 0.64

REACH = 5
PAD = 8


def band(size):
    index = np.arange(size)
    apart = np.abs(index[:, None] - index[None, :])
    taps = np.array(gauss_taps[4:] + [0.0], np.float64)
    return taps[np.minimum(apart, 5)]


def split_terms(matrix):
    high = matrix.astype(jnp.bfloat16)
    low = (matrix - high.astype(np.float64)).astype(jnp.bfloat16)
    return high, low


def column_matrix(columns):
    return np.concatenate(split_terms(band(columns)), 0)


def row_matrix(rows):
    high, low = split_terms(band(rows))
    return np.concatenate([high, high, low], 1)


def smooth_plane(counts, by, lx):
    rows = counts[0].shape[0]
    exact = jnp.concatenate([c.astype(jnp.float32).astype(jnp.bfloat16) for c in counts], 0)
    half = by.shape[0] // 2
    wide = jnp.dot(exact, by[:half], preferred_element_type=jnp.float32) + jnp.dot(
        exact, by[half:], preferred_element_type=jnp.float32
    )
    high = wide.astype(jnp.bfloat16)
    low = (wide - high.astype(jnp.float32)).astype(jnp.bfloat16)
    planes = []
    for n in range(len(counts)):
        part = slice(n * rows, (n + 1) * rows)
        stacked = jnp.concatenate([high[part], low[part], high[part]], 0)
        planes.append(jnp.dot(lx, stacked, preferred_element_type=jnp.float32))
    return planes


def smooth_depth(read, k):
    total = gauss_taps[4] * read(k)
    for offset in range(1, 5):
        total = total + gauss_taps[4 + offset] * (read(k - offset) + read(k + offset))
    return total


def depth_pass(flags, source, target, layers, first):
    tiles = source.shape[1] // 8

    def one_layer(j, _):
        for tile in range(tiles):
            rows = pl.ds(tile * 8, 8)
            value = smooth_depth(lambda k: source[k, rows, :], j + first)
            if tile == 0:
                value = value * flags[0]
            if tile == tiles - 1:
                value = value * flags[1]
            target[j, rows, :] = value
        return 0

    lax.fori_loop(0, layers, one_layer, 0)


def shade_voxels(prev, mid, above, below, following, scale):
    columns = mid.shape[1]
    lane = lax.broadcasted_iota(jnp.int32, mid.shape, 1)
    right = jnp.where(lane == columns - 1, 0.0, pltpu.roll(mid, columns - 1, 1))
    left = jnp.where(lane == 0, 0.0, pltpu.roll(mid, 1, 1))
    dz = following - prev
    dx = below - above
    dy = right - left
    slope = (1.5 * light_z) * dz + (1.5 * light_x) * dx + (1.5 * light_y) * dy
    shading = 0.55 + 0.45 * jnp.tanh(slope)
    gradient_sq4 = dz * dz + dx * dx + dy * dy
    square = mid * mid
    optical = scale * (square / (1.0 + square)) * (1.0 + gradient_sq4)
    centred = mid - 2.5
    red_share = 0.5 + 0.5 * jnp.tanh(centred)
    green_share = jnp.exp(-(centred * centred))
    return optical, shading, red_share, green_share


def render_pass(smoothed, layers, start, carry_in, store, scale):
    tiles = smoothed.shape[1] // 8 - 2

    def one_tile(tile, _):
        base = pl.multiple_of(tile * 8 + 8, 8)
        rows = pl.ds(base, 8)

        def one_layer(j, carry):
            red, green, blue, transmit = carry
            k = j + start
            mid = smoothed[k, rows, :]
            before = smoothed[k, pl.ds(base - 8, 8), :]
            after = smoothed[k, pl.ds(base + 8, 8), :]
            sub = lax.broadcasted_iota(jnp.int32, mid.shape, 0)
            above = pltpu.roll(jnp.where(sub == 7, before, mid), 1, 0)
            below = pltpu.roll(jnp.where(sub == 0, after, mid), 7, 0)
            optical, shading, red_share, green_share = shade_voxels(
                smoothed[k - 1, rows, :], mid, above, below, smoothed[k + 1, rows, :], scale
            )
            remaining = transmit * jnp.exp(-optical)
            lit = (transmit - remaining) * shading
            red_part = lit * red_share
            return (
                red + red_part,
                green + lit * green_share,
                blue + (lit - red_part),
                remaining,
            )

        out = lax.fori_loop(0, layers, one_layer, carry_in(tile))
        store(tile, out)
        return 0

    lax.fori_loop(0, tiles, one_tile, 0)


def interior_kernel(scale, flags, c, xl, xh, by, lx, front, back, image, plane, smoothed):
    layers = c.shape[0]
    group = 4

    def smooth_group(g, _):
        first = g * group
        counts = [
            jnp.concatenate([xl[first + n], c[first + n], xh[first + n]], 0) for n in range(group)
        ]
        for n, value in enumerate(smooth_plane(counts, by, lx[...])):
            plane[first + n] = value
        return 0

    lax.fori_loop(0, layers // group, smooth_group, 0)
    front[...] = plane[: 2 * REACH]
    back[...] = plane[layers - 2 * REACH :]
    depth_pass(flags, plane, smoothed, layers - 8, 4)

    def carry_in(tile):
        zero = jnp.zeros((8, c.shape[2]), jnp.float32)
        return zero, zero, zero, jnp.ones_like(zero)

    def store(tile, out):
        rows = pl.ds(pl.multiple_of(tile * 8, 8), 8)
        for n, value in enumerate(out):
            image[n, rows, :] = value

    render_pass(smoothed, layers - 10, 1, carry_in, store, scale)


def edge_kernel(scale, is_back, flags, own, edge, middle, cl, ch, by, lx, ahead, image, plane, smoothed):
    depth = edge.shape[0]
    if is_back:
        plane[: 2 * REACH] = own[...]
        at = 2 * REACH
    else:
        plane[REACH:] = own[...]
        at = 0
    counts = [
        jnp.concatenate([cl[n], edge[n, :PAD], middle[n], edge[n, PAD:], ch[n]], 0)
        for n in range(depth)
    ]
    for n, value in enumerate(smooth_plane(counts, by, lx[...])):
        plane[at + n] = value
    depth_pass(flags, plane, smoothed, REACH + 2, 4)
    outside = REACH + 1 if is_back else 0
    smoothed[outside] = smoothed[outside] * flags[2]

    def carry_in(tile):
        if not is_back:
            zero = jnp.zeros((8, own.shape[2]), jnp.float32)
            return zero, zero, zero, jnp.ones_like(zero)
        rows = pl.ds(pl.multiple_of(tile * 8, 8), 8)
        through = ahead[3, rows, :]
        colors = tuple(
            ahead[n, rows, :] + through * ahead[4 + n, rows, :] for n in range(3)
        )
        return colors + (through * ahead[7, rows, :],)

    def store(tile, out):
        rows = pl.ds(pl.multiple_of(tile * 8, 8), 8)
        for n, value in enumerate(out):
            image[n, rows, :] = value

    render_pass(smoothed, REACH, 1, carry_in, store, scale)


def whole(count):
    return [pl.BlockSpec(memory_space=pltpu.VMEM)] * count


def smem():
    return pl.BlockSpec(memory_space=pltpu.SMEM)


def call_interior(scale, flags, c, xl, xh, by, lx):
    layers, rows, columns = c.shape
    ext = rows + 2 * PAD
    f32 = jnp.float32
    return pl.pallas_call(
        functools.partial(interior_kernel, scale),
        out_shape=(
            jax.ShapeDtypeStruct((2 * REACH, ext, columns), f32),
            jax.ShapeDtypeStruct((2 * REACH, ext, columns), f32),
            jax.ShapeDtypeStruct((4, rows, columns), f32),
        ),
        in_specs=[smem()] + whole(5),
        out_specs=tuple(whole(3)),
        scratch_shapes=[
            pltpu.VMEM((layers, ext, columns), f32),
            pltpu.VMEM((layers - 8, ext, columns), f32),
        ],
        compiler_params=pltpu.CompilerParams(vmem_limit_bytes=48 * 1024 * 1024),
        cost_estimate=pl.CostEstimate(
            flops=2_000_000_000, transcendentals=0, bytes_accessed=8_000_000
        ),
        name="interior",
    )(flags, c, xl, xh, by, lx)


def call_edge(scale, is_back, flags, own, edge, middle, cl, ch, by, lx, ahead):
    _, ext, columns = own.shape
    f32 = jnp.float32
    return pl.pallas_call(
        functools.partial(edge_kernel, scale, is_back),
        out_shape=jax.ShapeDtypeStruct((4, ext - 2 * PAD, columns), f32),
        in_specs=[smem()] + whole(8),
        out_specs=whole(1)[0],
        scratch_shapes=[
            pltpu.VMEM((3 * REACH, ext, columns), f32),
            pltpu.VMEM((REACH + 2, ext, columns), f32),
        ],
        compiler_params=pltpu.CompilerParams(vmem_limit_bytes=32 * 1024 * 1024),
        cost_estimate=pl.CostEstimate(
            flops=200_000_000, transcendentals=0, bytes_accessed=3_000_000
        ),
        name="back" if is_back else "front",
    )(flags, own, edge, middle, cl, ch, by, lx, ahead)


def shift(value, axis, step):
    count = lax.axis_size(axis)
    pairs = [(i, i + step) for i in range(count) if 0 <= i + step < count]
    return lax.ppermute(value, axis, pairs)


def over(front, back):
    through = front[3:]
    return jnp.concatenate([front[:3] + through * back[:3], through * back[3:]], 0)


def exchange(layers):
    count = lax.axis_size("depth")
    me = lax.axis_index("depth")
    _, rows, columns = layers.shape
    owned = rows // count
    parity, pair = me % 2, me // 2
    pairs = count // 2
    pieces = layers.reshape(4, pairs, 2, owned, columns)
    send = lax.dynamic_index_in_dim(pieces, 1 - parity, 2, keepdims=False)
    keep = lax.dynamic_index_in_dim(pieces, parity, 2, keepdims=False)
    got = lax.ppermute(send, "depth", [(i, i ^ 1) for i in range(count)])
    joined = jnp.where(parity == 0, over(keep, got), over(got, keep))
    parts = []
    for step in range(pairs):
        piece = lax.dynamic_index_in_dim(joined, pair ^ step, 1, keepdims=False)
        if step:
            piece = lax.ppermute(piece, "depth", [(i, i ^ (2 * step)) for i in range(count)])
        parts.append(piece)
    result = jnp.zeros((3, owned, columns), jnp.float32)
    through = jnp.ones((1, owned, columns), jnp.float32)
    for step in range(pairs):
        ahead = jnp.ones((1, owned, columns), jnp.float32)
        for other in range(pairs):
            if other != step:
                nearer = (pair ^ other) < (pair ^ step)
                ahead = ahead * jnp.where(nearer, parts[other][3:], 1.0)
        result = result + ahead * parts[step][:3]
        through = through * parts[step][3:]
    return jnp.concatenate([result, 1.0 - through], 0)


def local(counts):
    slab, rows, columns = counts.shape
    img, depth = lax.axis_index("img"), lax.axis_index("depth")
    imgs, depths = lax.axis_size("img"), lax.axis_size("depth")
    scale = 1.5 / (slab * depths)
    top, bottom = counts[:REACH], counts[slab - REACH :]

    def edges(block):
        return jnp.concatenate([block[:, :PAD], block[:, rows - PAD :]], 1)

    front_edge = shift(edges(bottom), "depth", 1)
    back_edge = shift(edges(top), "depth", -1)
    xl = shift(counts[:, rows - PAD :], "img", 1)
    xh = shift(counts[:, :PAD], "img", -1)
    front_mid = shift(bottom[:, PAD : rows - PAD], "depth", 1)
    back_mid = shift(top[:, PAD : rows - PAD], "depth", -1)
    ends = jnp.concatenate([front_edge, back_edge], 0)
    cl = shift(ends[:, PAD:], "img", 1)
    ch = shift(ends[:, :PAD], "img", -1)
    one = jnp.float32(1.0)
    row_flags = [(img > 0) * one, (img < imgs - 1) * one]
    front_flags = jnp.stack(row_flags + [(depth > 0) * one])
    back_flags = jnp.stack(row_flags + [(depth < depths - 1) * one])
    by = jnp.asarray(column_matrix(columns))
    lx = jnp.asarray(row_matrix(rows + 2 * PAD))
    own_front, own_back, inner = call_interior(scale, front_flags, counts, xl, xh, by, lx)
    ahead = call_edge(
        scale, False, front_flags, own_front, front_edge, front_mid, cl[:REACH], ch[:REACH], by, lx,
        jnp.zeros((8, 8, columns), jnp.float32),
    )
    ahead = jnp.concatenate([ahead, inner], 0)
    layers = call_edge(
        scale, True, back_flags, own_back, back_edge, back_mid, cl[REACH:], ch[REACH:], by, lx, ahead
    )
    return exchange(layers)


def solution(mesh):
    in_specs = (P("depth", "img", None),)
    out_specs = P(None, ("img", "depth"), None)
    return jax.shard_map(local, mesh=mesh, in_specs=in_specs, out_specs=out_specs, check_vma=False)
```

```python
import functools
import math

import jax
import jax.numpy as jnp
import numpy as np
from jax import lax
from jax.experimental import pallas as pl
from jax.experimental.pallas import tpu as pltpu
from jax.sharding import PartitionSpec as P


gauss_taps = [
    math.exp(-offset * offset / 8.0)
    / sum((math.exp(-other * other / 8.0) for other in range(-4, 5)))
    for offset in range(-4, 5)
]
light_z = 0.48
light_x = 0.6
light_y = 0.64

REACH = 5
PAD = 8


def band(size):
    index = np.arange(size)
    apart = np.abs(index[:, None] - index[None, :])
    taps = np.array(gauss_taps[4:] + [0.0], np.float64)
    return taps[np.minimum(apart, 5)]


def split_terms(matrix):
    high = matrix.astype(jnp.bfloat16)
    low = (matrix - high.astype(np.float64)).astype(jnp.bfloat16)
    return high, low


def column_matrix(columns):
    return np.concatenate(split_terms(band(columns)), 0)


def row_matrix(rows):
    high, low = split_terms(band(rows))
    return np.concatenate([high, high, low], 1)


def smooth_plane(counts, by, lx):
    rows = counts[0].shape[0]
    exact = jnp.concatenate([c.astype(jnp.float32).astype(jnp.bfloat16) for c in counts], 0)
    half = by.shape[0] // 2
    wide = jnp.dot(exact, by[:half], preferred_element_type=jnp.float32) + jnp.dot(
        exact, by[half:], preferred_element_type=jnp.float32
    )
    high = wide.astype(jnp.bfloat16)
    low = (wide - high.astype(jnp.float32)).astype(jnp.bfloat16)
    planes = []
    for n in range(len(counts)):
        part = slice(n * rows, (n + 1) * rows)
        stacked = jnp.concatenate([high[part], low[part], high[part]], 0)
        planes.append(jnp.dot(lx, stacked, preferred_element_type=jnp.float32))
    return planes


def smooth_depth(read, k):
    total = gauss_taps[4] * read(k)
    for offset in range(1, 5):
        total = total + gauss_taps[4 + offset] * (read(k - offset) + read(k + offset))
    return total


def smooth_depth_layer(flags, read, k, tiles, write):
    for tile in range(tiles):
        rows = pl.ds(tile * 8, 8)
        value = smooth_depth(lambda j: read(j, rows), k)
        if tile == 0:
            value = value * flags[0]
        if tile == tiles - 1:
            value = value * flags[1]
        write(rows, value)


def shade_voxels(prev, mid, above, below, following, scale):
    columns = mid.shape[1]
    lane = lax.broadcasted_iota(jnp.int32, mid.shape, 1)
    right = jnp.where(lane == columns - 1, 0.0, pltpu.roll(mid, columns - 1, 1))
    left = jnp.where(lane == 0, 0.0, pltpu.roll(mid, 1, 1))
    dz = following - prev
    dx = below - above
    dy = right - left
    slope = (1.5 * light_z) * dz + (1.5 * light_x) * dx + (1.5 * light_y) * dy
    shading = 0.55 + 0.45 * jnp.tanh(slope)
    gradient_sq4 = dz * dz + dx * dx + dy * dy
    square = mid * mid
    optical = scale * (square / (1.0 + square)) * (1.0 + gradient_sq4)
    centred = mid - 2.5
    red_share = 0.5 + 0.5 * jnp.tanh(centred)
    green_share = jnp.exp(-(centred * centred))
    return optical, shading, red_share, green_share


def render_pass(smoothed, layers, carry_in, store, scale):
    tiles = smoothed.shape[1] // 8 - 2

    def one_tile(tile, _):
        base = pl.multiple_of(tile * 8 + 8, 8)
        rows = pl.ds(base, 8)
        red, green, blue, transmit = carry_in(tile)
        for k in range(1, layers + 1):
            mid = smoothed[k, rows, :]
            before = smoothed[k, pl.ds(base - 8, 8), :]
            after = smoothed[k, pl.ds(base + 8, 8), :]
            sub = lax.broadcasted_iota(jnp.int32, mid.shape, 0)
            above = pltpu.roll(jnp.where(sub == 7, before, mid), 1, 0)
            below = pltpu.roll(jnp.where(sub == 0, after, mid), 7, 0)
            optical, shading, red_share, green_share = shade_voxels(
                smoothed[k - 1, rows, :], mid, above, below, smoothed[k + 1, rows, :], scale
            )
            remaining = transmit * jnp.exp(-optical)
            lit = (transmit - remaining) * shading
            red_part = lit * red_share
            red = red + red_part
            green = green + lit * green_share
            blue = blue + (lit - red_part)
            transmit = remaining
        store(tile, (red, green, blue, transmit))
        return 0

    lax.fori_loop(0, tiles, one_tile, 0)


def smooth_kernel(group, c_hbm, xl, xh, by, lx, plane, c, sems):
    groups = c.shape[0] // group

    def fetch(g):
        part = pl.ds(g * group, group)
        return pltpu.make_async_copy(c_hbm.at[part], c.at[part], sems.at[g])

    for g in range(groups):
        fetch(g).start()

    def smooth_group(g, _):
        first = g * group
        fetch(g).wait()
        counts = [
            jnp.concatenate([xl[first + n], c[first + n], xh[first + n]], 0) for n in range(group)
        ]
        for n, value in enumerate(smooth_plane(counts, by, lx[...])):
            plane[first + n] = value
        return 0

    lax.fori_loop(0, groups, smooth_group, 0)


def interior_kernel(scale, flags, plane, image, smoothed):
    layers, ext, columns = plane.shape

    def one_layer(j, _):
        def write(rows, value):
            smoothed[j, rows, :] = value

        smooth_depth_layer(flags, lambda k, rows: plane[k, rows, :], j + 4, ext // 8, write)
        return 0

    lax.fori_loop(0, layers - 8, one_layer, 0)

    def carry_in(tile):
        zero = jnp.zeros((8, columns), jnp.float32)
        return zero, zero, zero, jnp.ones_like(zero)

    def store(tile, out):
        rows = pl.ds(pl.multiple_of(tile * 8, 8), 8)
        for n, value in enumerate(out):
            image[n, rows, :] = value

    render_pass(smoothed, layers - 10, carry_in, store, scale)


def edge_kernel(scale, is_back, flags, own, edge, middle, cl, ch, by, lx, *refs):
    ahead = refs[0]
    image, plane, smoothed = refs[-3:]
    depth = edge.shape[0]
    counts = [
        jnp.concatenate([cl[n], edge[n, :PAD], middle[n], edge[n, PAD:], ch[n]], 0)
        for n in range(depth)
    ]
    for n, value in enumerate(smooth_plane(counts, by, lx[...])):
        plane[n] = value
    held = own.shape[0]

    def read(k, rows):
        if is_back:
            return own[held - 2 * REACH + k, rows, :] if k < 2 * REACH else plane[k - 2 * REACH, rows, :]
        return plane[k, rows, :] if k < REACH else own[k - REACH, rows, :]

    for j in range(REACH + 2):
        outside = j == (REACH + 1 if is_back else 0)

        def write(rows, value, j=j, outside=outside):
            smoothed[j, rows, :] = value * flags[2] if outside else value

        smooth_depth_layer(flags, read, j + 4, own.shape[1] // 8, write)

    def tile_of(ref, tile):
        rows = pl.ds(pl.multiple_of(tile * 8, 8), 8)
        return tuple(ref[n, rows, :] for n in range(4))

    def carry_in(tile):
        if is_back:
            return tile_of(ahead, tile)
        zero = jnp.zeros((8, own.shape[2]), jnp.float32)
        return zero, zero, zero, jnp.ones_like(zero)

    def store(tile, out):
        rows = pl.ds(pl.multiple_of(tile * 8, 8), 8)
        if not is_back:
            inner = tile_of(ahead, tile)
            out = tuple(out[n] + out[3] * inner[n] for n in range(3)) + (out[3] * inner[3],)
        for n, value in enumerate(out):
            image[n, rows, :] = value

    render_pass(smoothed, REACH, carry_in, store, scale)


def whole(count):
    return [pl.BlockSpec(memory_space=pltpu.VMEM)] * count


def smem():
    return pl.BlockSpec(memory_space=pltpu.SMEM)


def call_smooth(c, xl, xh, by, lx):
    layers, rows, columns = c.shape
    ext = rows + 2 * PAD
    group = 4
    return pl.pallas_call(
        functools.partial(smooth_kernel, group),
        out_shape=jax.ShapeDtypeStruct((layers, ext, columns), jnp.float32),
        in_specs=[pl.BlockSpec(memory_space=pltpu.HBM)] + whole(4),
        out_specs=whole(1)[0],
        scratch_shapes=[
            pltpu.VMEM((layers, rows, columns), jnp.int32),
            pltpu.SemaphoreType.DMA((layers // group,)),
        ],
        compiler_params=pltpu.CompilerParams(vmem_limit_bytes=24 * 1024 * 1024),
        cost_estimate=pl.CostEstimate(
            flops=1_000_000_000, transcendentals=0, bytes_accessed=8_000_000
        ),
        name="smooth",
    )(c, xl, xh, by, lx)


def call_interior(scale, flags, plane):
    layers, ext, columns = plane.shape
    return pl.pallas_call(
        functools.partial(interior_kernel, scale),
        out_shape=jax.ShapeDtypeStruct((4, ext - 2 * PAD, columns), jnp.float32),
        in_specs=[smem()] + whole(1),
        out_specs=whole(1)[0],
        scratch_shapes=[pltpu.VMEM((layers - 8, ext, columns), jnp.float32)],
        compiler_params=pltpu.CompilerParams(vmem_limit_bytes=24 * 1024 * 1024),
        cost_estimate=pl.CostEstimate(
            flops=1_000_000_000, transcendentals=0, bytes_accessed=8_000_000
        ),
        name="interior",
    )(flags, plane)


def call_edge(scale, is_back, flags, plane, edge, middle, cl, ch, by, lx, *ahead):
    _, ext, columns = plane.shape
    f32 = jnp.float32
    return pl.pallas_call(
        functools.partial(edge_kernel, scale, is_back),
        out_shape=jax.ShapeDtypeStruct((4, ext - 2 * PAD, columns), f32),
        in_specs=[smem()] + whole(7 + len(ahead)),
        out_specs=whole(1)[0],
        scratch_shapes=[
            pltpu.VMEM((REACH, ext, columns), f32),
            pltpu.VMEM((REACH + 2, ext, columns), f32),
        ],
        compiler_params=pltpu.CompilerParams(vmem_limit_bytes=24 * 1024 * 1024),
        cost_estimate=pl.CostEstimate(
            flops=200_000_000, transcendentals=0, bytes_accessed=3_000_000
        ),
        name="back" if is_back else "front",
    )(flags, plane, edge, middle, cl, ch, by, lx, *ahead)


def shift(value, axis, step):
    count = lax.axis_size(axis)
    pairs = [(i, i + step) for i in range(count) if 0 <= i + step < count]
    return lax.ppermute(value, axis, pairs)


def over(front, back):
    through = front[3:]
    return jnp.concatenate([front[:3] + through * back[:3], through * back[3:]], 0)


def exchange(layers):
    count = lax.axis_size("depth")
    me = lax.axis_index("depth")
    _, rows, columns = layers.shape
    owned = rows // count
    parity, pair = me % 2, me // 2
    pairs = count // 2
    pieces = layers.reshape(4, pairs, 2, owned, columns)
    send = lax.dynamic_index_in_dim(pieces, 1 - parity, 2, keepdims=False)
    keep = lax.dynamic_index_in_dim(pieces, parity, 2, keepdims=False)
    got = lax.ppermute(send, "depth", [(i, i ^ 1) for i in range(count)])
    joined = jnp.where(parity == 0, over(keep, got), over(got, keep))
    parts = []
    for step in range(pairs):
        piece = lax.dynamic_index_in_dim(joined, pair ^ step, 1, keepdims=False)
        if step:
            piece = lax.ppermute(piece, "depth", [(i, i ^ (2 * step)) for i in range(count)])
        parts.append(piece)
    result = jnp.zeros((3, owned, columns), jnp.float32)
    through = jnp.ones((1, owned, columns), jnp.float32)
    for step in range(pairs):
        ahead = jnp.ones((1, owned, columns), jnp.float32)
        for other in range(pairs):
            if other != step:
                nearer = (pair ^ other) < (pair ^ step)
                ahead = ahead * jnp.where(nearer, parts[other][3:], 1.0)
        result = result + ahead * parts[step][:3]
        through = through * parts[step][3:]
    return jnp.concatenate([result, 1.0 - through], 0)


def local(counts):
    slab, rows, columns = counts.shape
    img, depth = lax.axis_index("img"), lax.axis_index("depth")
    imgs, depths = lax.axis_size("img"), lax.axis_size("depth")
    scale = 1.5 / (slab * depths)
    top, bottom = counts[:REACH], counts[slab - REACH :]

    def edges(block):
        return jnp.concatenate([block[:, :PAD], block[:, rows - PAD :]], 1)

    front_edge = shift(edges(bottom), "depth", 1)
    back_edge = shift(edges(top), "depth", -1)
    xl = shift(counts[:, rows - PAD :], "img", 1)
    xh = shift(counts[:, :PAD], "img", -1)
    front_mid = shift(bottom[:, PAD : rows - PAD], "depth", 1)
    back_mid = shift(top[:, PAD : rows - PAD], "depth", -1)
    ends = jnp.concatenate([front_edge, back_edge], 0)
    cl = shift(ends[:, PAD:], "img", 1)
    ch = shift(ends[:, :PAD], "img", -1)
    one = jnp.float32(1.0)
    row_flags = [(img > 0) * one, (img < imgs - 1) * one]
    front_flags = jnp.stack(row_flags + [(depth > 0) * one])
    back_flags = jnp.stack(row_flags + [(depth < depths - 1) * one])
    by = jnp.asarray(column_matrix(columns))
    lx = jnp.asarray(row_matrix(rows + 2 * PAD))
    held = pltpu.with_memory_space_constraint(counts, pltpu.HBM)
    plane = call_smooth(held, xl, xh, by, lx)
    inner = call_interior(scale, front_flags, plane)
    front = call_edge(
        scale, False, front_flags, plane, front_edge, front_mid, cl[:REACH], ch[:REACH], by, lx,
        inner,
    )
    layers = call_edge(
        scale, True, back_flags, plane, back_edge, back_mid, cl[REACH:], ch[REACH:], by, lx,
        front,
    )
    return exchange(layers)


def solution(mesh):
    in_specs = (P("depth", "img", None),)
    out_specs = P(None, ("img", "depth"), None)
    return jax.shard_map(local, mesh=mesh, in_specs=in_specs, out_specs=out_specs, check_vma=False)
```

```python
import functools
import math

import jax
import jax.numpy as jnp
import numpy as np
from jax import lax
from jax.experimental import pallas as pl
from jax.experimental.pallas import tpu as pltpu
from jax.sharding import PartitionSpec as P


gauss_taps = [
    math.exp(-offset * offset / 8.0)
    / sum((math.exp(-other * other / 8.0) for other in range(-4, 5)))
    for offset in range(-4, 5)
]
light_z = 0.48
light_x = 0.6
light_y = 0.64

REACH = 5
PAD = 8


def band(size):
    index = np.arange(size)
    apart = np.abs(index[:, None] - index[None, :])
    taps = np.array(gauss_taps[4:] + [0.0], np.float64)
    return taps[np.minimum(apart, 5)]


def split_terms(matrix):
    high = matrix.astype(jnp.bfloat16)
    low = (matrix - high.astype(np.float64)).astype(jnp.bfloat16)
    return high, low


def column_matrix(columns):
    return np.concatenate(split_terms(band(columns)), 0)


def row_matrices(rows):
    high, low = split_terms(band(rows + 2 * PAD))
    order = np.arange(rows + 2 * PAD)
    swapped = np.concatenate([order[rows + PAD :], order[PAD : rows + PAD], order[:PAD]])
    both = []
    for columns in (order, swapped):
        both.append(np.concatenate([high[:, columns], high[:, columns], low[:, columns]], 1))
    return np.stack(both)


def smooth_plane(counts, by, lx):
    rows = counts[0].shape[0]
    exact = jnp.concatenate([c.astype(jnp.float32).astype(jnp.bfloat16) for c in counts], 0)
    half = by.shape[0] // 2
    wide = jnp.dot(exact, by[:half], preferred_element_type=jnp.float32) + jnp.dot(
        exact, by[half:], preferred_element_type=jnp.float32
    )
    high = wide.astype(jnp.bfloat16)
    low = (wide - high.astype(jnp.float32)).astype(jnp.bfloat16)
    planes = []
    for n in range(len(counts)):
        part = slice(n * rows, (n + 1) * rows)
        stacked = jnp.concatenate([high[part], low[part], high[part]], 0)
        planes.append(jnp.dot(lx, stacked, preferred_element_type=jnp.float32))
    return planes


def smooth_depth(read, k):
    total = gauss_taps[4] * read(k)
    for offset in range(1, 5):
        total = total + gauss_taps[4 + offset] * (read(k - offset) + read(k + offset))
    return total


def smooth_depth_layer(flags, read, k, tiles, write):
    for tile in range(tiles):
        rows = pl.ds(tile * 8, 8)
        value = smooth_depth(lambda j: read(j, rows), k)
        if tile == 0:
            value = value * flags[0]
        if tile == tiles - 1:
            value = value * flags[1]
        write(rows, value)


def shade_voxels(prev, mid, above, below, following, scale):
    columns = mid.shape[1]
    lane = lax.broadcasted_iota(jnp.int32, mid.shape, 1)
    right = jnp.where(lane == columns - 1, 0.0, pltpu.roll(mid, columns - 1, 1))
    left = jnp.where(lane == 0, 0.0, pltpu.roll(mid, 1, 1))
    dz = following - prev
    dx = below - above
    dy = right - left
    slope = (1.5 * light_z) * dz + (1.5 * light_x) * dx + (1.5 * light_y) * dy
    shading = 0.55 + 0.45 * jnp.tanh(slope)
    gradient_sq4 = dz * dz + dx * dx + dy * dy
    square = mid * mid
    optical = scale * (square / (1.0 + square)) * (1.0 + gradient_sq4)
    centred = mid - 2.5
    red_share = 0.5 + 0.5 * jnp.tanh(centred)
    green_share = jnp.exp(-(centred * centred))
    return optical, shading, red_share, green_share


def render_layer(layer, k, base, carry, scale):
    red, green, blue, transmit = carry
    rows = pl.ds(base, 8)
    mid = layer(k, rows)
    before = layer(k, pl.ds(base - 8, 8))
    after = layer(k, pl.ds(base + 8, 8))
    sub = lax.broadcasted_iota(jnp.int32, mid.shape, 0)
    above = pltpu.roll(jnp.where(sub == 7, before, mid), 1, 0)
    below = pltpu.roll(jnp.where(sub == 0, after, mid), 7, 0)
    optical, shading, red_share, green_share = shade_voxels(
        layer(k - 1, rows), mid, above, below, layer(k + 1, rows), scale
    )
    remaining = transmit * jnp.exp(-optical)
    lit = (transmit - remaining) * shading
    red_part = lit * red_share
    return red + red_part, green + lit * green_share, blue + (lit - red_part), remaining


def empty_carry(columns):
    zero = jnp.zeros((8, columns), jnp.float32)
    return zero, zero, zero, jnp.ones_like(zero)


def read_tile(ref, tile):
    rows = pl.ds(pl.multiple_of(tile * 8, 8), 8)
    return tuple(ref[n, rows, :] for n in range(4))


def store_tile(ref, tile, values):
    rows = pl.ds(pl.multiple_of(tile * 8, 8), 8)
    for n, value in enumerate(values):
        ref[n, rows, :] = value


def run_copies(copies):
    for copy in copies:
        copy.start()
    for copy in copies:
        copy.wait()


def pack_edges_kernel(where, c, edge_a, edge_b, sems):
    rows = c.shape[1]
    copies = []
    for n, target in enumerate((edge_a, edge_b)):
        layers = pl.ds(where[n], REACH)
        for half, start in enumerate((0, rows - PAD)):
            source = c.at[layers, pl.ds(start, PAD)]
            part = target.at[:, pl.ds(half * PAD, PAD)]
            copies.append(pltpu.make_async_copy(source, part, sems.at[2 * n + half]))
    run_copies(copies)


def pack_rest_kernel(where, c, side_a, side_b, middle_a, middle_b, sems):
    rows = c.shape[1]
    copies = []
    for n, target in enumerate((side_a, side_b)):
        source = c.at[:, pl.ds(pl.multiple_of(where[2 + n], PAD), PAD)]
        copies.append(pltpu.make_async_copy(source, target, sems.at[n]))
    for n, target in enumerate((middle_a, middle_b)):
        source = c.at[pl.ds(where[n], REACH), pl.ds(PAD, rows - 2 * PAD)]
        copies.append(pltpu.make_async_copy(source, target, sems.at[2 + n]))
    run_copies(copies)


def smooth_kernel(group, order, c_hbm, xa, xb, by, lx, plane, c, sems):
    groups = c.shape[0] // group
    rows_of = order[0]

    def fetch(g):
        part = pl.ds(g * group, group)
        return pltpu.make_async_copy(c_hbm.at[part], c.at[part], sems.at[g])

    for g in range(groups):
        fetch(g).start()

    def smooth_group(g, _):
        first = g * group
        fetch(g).wait()
        counts = [
            jnp.concatenate([xa[first + n], c[first + n], xb[first + n]], 0) for n in range(group)
        ]
        for n, value in enumerate(smooth_plane(counts, by, lx[rows_of])):
            plane[first + n] = value
        return 0

    lax.fori_loop(0, groups, smooth_group, 0)


def interior_kernel(scale, flags, plane, image, smoothed):
    layers, ext, columns = plane.shape

    def one_layer(j, _):
        def write(rows, value):
            smoothed[j, rows, :] = value

        smooth_depth_layer(flags, lambda k, rows: plane[k, rows, :], j + 4, ext // 8, write)
        return 0

    lax.fori_loop(0, layers - 8, one_layer, 0)

    def one_tile(tile, _):
        base = pl.multiple_of(tile * 8 + 8, 8)
        carry = empty_carry(columns)
        for k in range(1, layers - 9):
            carry = render_layer(lambda k, rows: smoothed[k, rows, :], k, base, carry, scale)
        store_tile(image, tile, carry)
        return 0

    lax.fori_loop(0, ext // 8 - 2, one_tile, 0)


def edge_kernel(
    scale, flags, order, plane, smoothed, edge_a, edge_b, mid_a, mid_b, ca, cb, by, lx, inner,
    image, halo, ends,
):
    layers, ext, columns = plane.shape
    rows_of, depth_of = order[0], order[1]
    counts = []
    for n, (edge, middle) in enumerate(((edge_a, mid_a), (edge_b, mid_b))):
        for j in range(REACH):
            at = n * REACH + j
            counts.append(
                jnp.concatenate([ca[at], edge[j, :PAD], middle[j], edge[j, PAD:], cb[at]], 0)
            )
    for at, value in enumerate(smooth_plane(counts, by, lx[rows_of])):
        slot = jnp.where(depth_of == 1, at, (at + REACH) % (2 * REACH))
        halo[slot] = value

    def counted(k, rows):
        if k < 0:
            return halo[k + REACH, rows, :]
        if k >= layers:
            return halo[k - layers + REACH, rows, :]
        return plane[k, rows, :]

    front_layers = range(-1, 4)
    back_layers = range(layers - 4, layers + 1)
    for j, k in enumerate([*front_layers, *back_layers]):

        def write(rows, value, j=j, k=k):
            if k < 0:
                value = value * flags[2]
            if k >= layers:
                value = value * flags[3]
            ends[j, rows, :] = value

        smooth_depth_layer(flags, counted, k, ext // 8, write)

    def layer(k, rows):
        if k < 4:
            return ends[k + 1, rows, :]
        if k >= layers - 4:
            return ends[k - (layers - 4) + REACH, rows, :]
        return smoothed[k - 4, rows, :]

    def one_tile(tile, _):
        base = pl.multiple_of(tile * 8 + 8, 8)
        carry = empty_carry(columns)
        for k in range(REACH):
            carry = render_layer(layer, k, base, carry, scale)
        behind = read_tile(inner, tile)
        carry = tuple(carry[n] + carry[3] * behind[n] for n in range(3)) + (carry[3] * behind[3],)
        for k in range(layers - REACH, layers):
            carry = render_layer(layer, k, base, carry, scale)
        store_tile(image, tile, carry)
        return 0

    lax.fori_loop(0, ext // 8 - 2, one_tile, 0)


def whole(count):
    return [pl.BlockSpec(memory_space=pltpu.VMEM)] * count


def smem():
    return pl.BlockSpec(memory_space=pltpu.SMEM)


def in_hbm():
    return pl.BlockSpec(memory_space=pltpu.HBM)


def params(mib):
    return pltpu.CompilerParams(vmem_limit_bytes=mib * 1024 * 1024)


def cost(flops):
    return pl.CostEstimate(flops=flops, transcendentals=0, bytes_accessed=4_000_000)


def call_pack_edges(where, c):
    _, _, columns = c.shape
    shape = jax.ShapeDtypeStruct((REACH, 2 * PAD, columns), c.dtype)
    return pl.pallas_call(
        pack_edges_kernel,
        out_shape=(shape, shape),
        in_specs=[smem(), in_hbm()],
        out_specs=tuple(whole(2)),
        scratch_shapes=[pltpu.SemaphoreType.DMA((4,))],
        compiler_params=params(8),
        name="pack_edges",
    )(where, c)


def call_pack_rest(where, c):
    layers, rows, columns = c.shape
    side = jax.ShapeDtypeStruct((layers, PAD, columns), c.dtype)
    middle = jax.ShapeDtypeStruct((REACH, rows - 2 * PAD, columns), c.dtype)
    return pl.pallas_call(
        pack_rest_kernel,
        out_shape=(side, side, middle, middle),
        in_specs=[smem(), in_hbm()],
        out_specs=tuple(whole(4)),
        scratch_shapes=[pltpu.SemaphoreType.DMA((4,))],
        compiler_params=params(8),
        name="pack_rest",
    )(where, c)


def call_smooth(order, c, xa, xb, by, lx):
    layers, rows, columns = c.shape
    ext = rows + 2 * PAD
    group = 4
    return pl.pallas_call(
        functools.partial(smooth_kernel, group),
        out_shape=jax.ShapeDtypeStruct((layers, ext, columns), jnp.float32),
        in_specs=[smem(), in_hbm()] + whole(4),
        out_specs=whole(1)[0],
        scratch_shapes=[
            pltpu.VMEM((layers, rows, columns), jnp.int32),
            pltpu.SemaphoreType.DMA((layers // group,)),
        ],
        compiler_params=params(24),
        cost_estimate=cost(1_000_000_000),
        name="smooth",
    )(order, c, xa, xb, by, lx)


def call_interior(scale, flags, plane):
    layers, ext, columns = plane.shape
    return pl.pallas_call(
        functools.partial(interior_kernel, scale),
        out_shape=(
            jax.ShapeDtypeStruct((4, ext - 2 * PAD, columns), jnp.float32),
            jax.ShapeDtypeStruct((layers - 8, ext, columns), jnp.float32),
        ),
        in_specs=[smem()] + whole(1),
        out_specs=tuple(whole(2)),
        compiler_params=params(24),
        cost_estimate=cost(1_000_000_000),
        name="interior",
    )(flags, plane)


def call_edge(scale, flags, order, plane, *operands):
    _, ext, columns = plane.shape
    f32 = jnp.float32
    return pl.pallas_call(
        functools.partial(edge_kernel, scale),
        out_shape=jax.ShapeDtypeStruct((4, ext - 2 * PAD, columns), f32),
        in_specs=[smem(), smem()] + whole(1 + len(operands)),
        out_specs=whole(1)[0],
        scratch_shapes=[
            pltpu.VMEM((2 * REACH, ext, columns), f32),
            pltpu.VMEM((2 * REACH, ext, columns), f32),
        ],
        compiler_params=params(32),
        cost_estimate=cost(300_000_000),
        name="edges",
    )(flags, order, plane, *operands)


def swap(value, axis, first):
    count = lax.axis_size(axis)
    pairs = []
    for low in range(first, count - 1, 2):
        pairs += [(low, low + 1), (low + 1, low)]
    return lax.ppermute(value, axis, pairs)


def over(front, back):
    through = front[3:]
    return jnp.concatenate([front[:3] + through * back[:3], through * back[3:]], 0)


def exchange(layers):
    count = lax.axis_size("depth")
    me = lax.axis_index("depth")
    _, rows, columns = layers.shape
    owned = rows // count
    parity, pair = me % 2, me // 2
    pairs = count // 2
    pieces = layers.reshape(4, pairs, 2, owned, columns)
    send = lax.dynamic_index_in_dim(pieces, 1 - parity, 2, keepdims=False)
    keep = lax.dynamic_index_in_dim(pieces, parity, 2, keepdims=False)
    got = lax.ppermute(send, "depth", [(i, i ^ 1) for i in range(count)])
    joined = jnp.where(parity == 0, over(keep, got), over(got, keep))
    parts = []
    for step in range(pairs):
        piece = lax.dynamic_index_in_dim(joined, pair ^ step, 1, keepdims=False)
        if step:
            piece = lax.ppermute(piece, "depth", [(i, i ^ (2 * step)) for i in range(count)])
        parts.append(piece)
    result = jnp.zeros((3, owned, columns), jnp.float32)
    through = jnp.ones((1, owned, columns), jnp.float32)
    for step in range(pairs):
        ahead = jnp.ones((1, owned, columns), jnp.float32)
        for other in range(pairs):
            if other != step:
                nearer = (pair ^ other) < (pair ^ step)
                ahead = ahead * jnp.where(nearer, parts[other][3:], 1.0)
        result = result + ahead * parts[step][:3]
        through = through * parts[step][3:]
    return jnp.concatenate([result, 1.0 - through], 0)


def local(counts):
    slab, rows, columns = counts.shape
    img, depth = lax.axis_index("img"), lax.axis_index("depth")
    imgs, depths = lax.axis_size("img"), lax.axis_size("depth")
    scale = 1.5 / (slab * depths)
    row_odd, depth_odd = img % 2, depth % 2
    first_a, first_b = (1 - depth_odd) * (slab - REACH), depth_odd * (slab - REACH)
    row_a, row_b = (1 - row_odd) * (rows - PAD), row_odd * (rows - PAD)
    where = jnp.stack([first_a, first_b, row_a, row_b])
    order = jnp.stack([1 - row_odd, depth_odd])
    one = jnp.float32(1.0)
    flags = jnp.stack(
        [(img > 0) * one, (img < imgs - 1) * one, (depth > 0) * one, (depth < depths - 1) * one]
    )
    by = jnp.asarray(column_matrix(columns))
    lx = jnp.asarray(row_matrices(rows))
    held = pltpu.with_memory_space_constraint(counts, pltpu.HBM)
    edge_a, edge_b = call_pack_edges(where, held)
    side_a, side_b, mid_a, mid_b = call_pack_rest(where, held)
    edge_a = swap(edge_a, "depth", 0)
    edge_b = swap(edge_b, "depth", 1)
    xa = swap(side_a, "img", 0)
    xb = swap(side_b, "img", 1)
    mid_a = swap(mid_a, "depth", 0)
    mid_b = swap(mid_b, "depth", 1)
    halves = jnp.concatenate([edge_a, edge_b], 0).reshape(2 * REACH, 2, PAD, columns)
    corner_a = lax.dynamic_index_in_dim(halves, 1 - row_odd, 1, keepdims=False)
    corner_b = lax.dynamic_index_in_dim(halves, row_odd, 1, keepdims=False)
    ca = swap(corner_a, "img", 0)
    cb = swap(corner_b, "img", 1)
    plane = call_smooth(order, held, xa, xb, by, lx)
    inner, smoothed = call_interior(scale, flags, plane)
    layers = call_edge(
        scale, flags, order, plane, smoothed, edge_a, edge_b, mid_a, mid_b, ca, cb, by, lx, inner
    )
    return exchange(layers)


def solution(mesh):
    in_specs = (P("depth", "img", None),)
    out_specs = P(None, ("img", "depth"), None)
    return jax.shard_map(local, mesh=mesh, in_specs=in_specs, out_specs=out_specs, check_vma=False)
```

```python
import functools
import math

import jax
import jax.numpy as jnp
import numpy as np
from jax import lax
from jax.experimental import pallas as pl
from jax.experimental.pallas import tpu as pltpu
from jax.sharding import PartitionSpec as P


gauss_taps = [
    math.exp(-offset * offset / 8.0)
    / sum((math.exp(-other * other / 8.0) for other in range(-4, 5)))
    for offset in range(-4, 5)
]
light_z = 0.48
light_x = 0.6
light_y = 0.64

REACH = 5
PAD = 8


def band(size):
    index = np.arange(size)
    apart = np.abs(index[:, None] - index[None, :])
    taps = np.array(gauss_taps[4:] + [0.0], np.float64)
    return taps[np.minimum(apart, 5)]


def split_terms(matrix):
    high = matrix.astype(jnp.bfloat16)
    low = (matrix - high.astype(np.float64)).astype(jnp.bfloat16)
    return high, low


def column_matrix(columns):
    return np.concatenate(split_terms(band(columns)), 0)


def row_matrices(rows):
    high, low = split_terms(band(rows + 2 * PAD))
    order = np.arange(rows + 2 * PAD)
    swapped = np.concatenate([order[rows + PAD :], order[PAD : rows + PAD], order[:PAD]])
    both = []
    for columns in (order, swapped):
        both.append(np.concatenate([high[:, columns], high[:, columns], low[:, columns]], 1))
    return np.stack(both)


def smooth_plane(counts, by, lx):
    rows = counts[0].shape[0]
    exact = jnp.concatenate([c.astype(jnp.float32).astype(jnp.bfloat16) for c in counts], 0)
    half = by.shape[0] // 2
    wide = jnp.dot(exact, by[:half], preferred_element_type=jnp.float32) + jnp.dot(
        exact, by[half:], preferred_element_type=jnp.float32
    )
    high = wide.astype(jnp.bfloat16)
    low = (wide - high.astype(jnp.float32)).astype(jnp.bfloat16)
    planes = []
    for n in range(len(counts)):
        part = slice(n * rows, (n + 1) * rows)
        stacked = jnp.concatenate([high[part], low[part], high[part]], 0)
        planes.append(jnp.dot(lx, stacked, preferred_element_type=jnp.float32))
    return planes


def smooth_depth(read, k):
    total = gauss_taps[4] * read(k)
    for offset in range(1, 5):
        total = total + gauss_taps[4 + offset] * (read(k - offset) + read(k + offset))
    return total


def smooth_depth_layer(flags, read, k, tiles, write):
    for tile in range(tiles):
        rows = pl.ds(tile * 8, 8)
        value = smooth_depth(lambda j: read(j, rows), k)
        if tile == 0:
            value = value * flags[0]
        if tile == tiles - 1:
            value = value * flags[1]
        write(rows, value)


def shade_voxels(prev, mid, above, below, following, scale):
    columns = mid.shape[1]
    lane = lax.broadcasted_iota(jnp.int32, mid.shape, 1)
    right = jnp.where(lane == columns - 1, 0.0, pltpu.roll(mid, columns - 1, 1))
    left = jnp.where(lane == 0, 0.0, pltpu.roll(mid, 1, 1))
    dz = following - prev
    dx = below - above
    dy = right - left
    slope = (1.5 * light_z) * dz + (1.5 * light_x) * dx + (1.5 * light_y) * dy
    shading = 0.55 + 0.45 * jnp.tanh(slope)
    gradient_sq4 = dz * dz + dx * dx + dy * dy
    square = mid * mid
    optical = scale * (square / (1.0 + square)) * (1.0 + gradient_sq4)
    centred = mid - 2.5
    red_share = 0.5 + 0.5 * jnp.tanh(centred)
    green_share = jnp.exp(-(centred * centred))
    return optical, shading, red_share, green_share


def render_layer(layer, k, base, carry, scale):
    red, green, blue, transmit = carry
    rows = pl.ds(base, 8)
    mid = layer(k, rows)
    before = layer(k, pl.ds(base - 8, 8))
    after = layer(k, pl.ds(base + 8, 8))
    sub = lax.broadcasted_iota(jnp.int32, mid.shape, 0)
    above = pltpu.roll(jnp.where(sub == 7, before, mid), 1, 0)
    below = pltpu.roll(jnp.where(sub == 0, after, mid), 7, 0)
    optical, shading, red_share, green_share = shade_voxels(
        layer(k - 1, rows), mid, above, below, layer(k + 1, rows), scale
    )
    remaining = transmit * jnp.exp(-optical)
    lit = (transmit - remaining) * shading
    red_part = lit * red_share
    return red + red_part, green + lit * green_share, blue + (lit - red_part), remaining


def empty_carry(columns):
    zero = jnp.zeros((8, columns), jnp.float32)
    return zero, zero, zero, jnp.ones_like(zero)


def read_tile(ref, tile):
    rows = pl.ds(pl.multiple_of(tile * 8, 8), 8)
    return tuple(ref[n, rows, :] for n in range(4))


def store_tile(ref, tile, values):
    rows = pl.ds(pl.multiple_of(tile * 8, 8), 8)
    for n, value in enumerate(values):
        ref[n, rows, :] = value


def pack_kernel(where, c, edge_a, side_b, edge_b, side_a, middle_a, middle_b, sems):
    rows = c.shape[1]
    copies = []

    def add(source, target):
        copies.append(pltpu.make_async_copy(source, target, sems.at[len(copies)]))

    sides = (side_a, side_b)
    for n, (edge, middle) in enumerate(((edge_a, middle_a), (edge_b, middle_b))):
        layers = pl.ds(where[n], REACH)
        add(c.at[layers, pl.ds(0, PAD)], edge.at[:, pl.ds(0, PAD)])
        add(c.at[layers, pl.ds(rows - PAD, PAD)], edge.at[:, pl.ds(PAD, PAD)])
        add(c.at[layers, pl.ds(PAD, rows - 2 * PAD)], middle)
        add(c.at[:, pl.ds(pl.multiple_of(where[2 + n], PAD), PAD)], sides[n])
    for copy in copies:
        copy.start()
    for copy in copies:
        copy.wait()


def smooth_kernel(group, order, c_hbm, xa, xb, by, lx, plane, c, sems):
    groups = c.shape[0] // group
    rows_of = order[0]

    def fetch(g):
        part = pl.ds(g * group, group)
        return pltpu.make_async_copy(c_hbm.at[part], c.at[part], sems.at[g])

    for g in range(groups):
        fetch(g).start()

    def smooth_group(g, _):
        first = g * group
        fetch(g).wait()
        counts = [
            jnp.concatenate([xa[first + n], c[first + n], xb[first + n]], 0) for n in range(group)
        ]
        for n, value in enumerate(smooth_plane(counts, by, lx[rows_of])):
            plane[first + n] = value
        return 0

    lax.fori_loop(0, groups, smooth_group, 0)


def interior_kernel(scale, flags, plane, image, smoothed):
    layers, ext, columns = plane.shape

    def one_layer(j, _):
        def write(rows, value):
            smoothed[j, rows, :] = value

        smooth_depth_layer(flags, lambda k, rows: plane[k, rows, :], j + 4, ext // 8, write)
        return 0

    lax.fori_loop(0, layers - 8, one_layer, 0)

    def one_tile(tile, _):
        base = pl.multiple_of(tile * 8 + 8, 8)
        carry = empty_carry(columns)
        for k in range(1, layers - 9):
            carry = render_layer(lambda k, rows: smoothed[k, rows, :], k, base, carry, scale)
        store_tile(image, tile, carry)
        return 0

    lax.fori_loop(0, ext // 8 - 2, one_tile, 0)


def edge_kernel(
    scale, turn, flags, order, plane, smoothed, edge, middle, ca, cb, by, lx, behind,
    image, halo, ends,
):
    layers, ext, columns = plane.shape
    rows_of = order[0]
    is_front = order[1] == 1 - turn
    sign = jnp.where(is_front, 1, -1)
    counts = [
        jnp.concatenate([ca[j], edge[j, :PAD], middle[j], edge[j, PAD:], cb[j]], 0)
        for j in range(REACH)
    ]
    for j, value in enumerate(smooth_plane(counts, by, lx[rows_of])):
        halo[j] = value
    plane_face = jnp.where(is_front, 0, layers - 1)
    halo_face = jnp.where(is_front, REACH, -1)
    ends_face = jnp.where(is_front, 1, REACH)
    smoothed_face = jnp.where(is_front, -4, layers - 5)
    on_grid = jnp.where(is_front, flags[2], flags[3])

    def counted(v, rows):
        if v < 0:
            return halo[halo_face + sign * v, rows, :]
        return plane[plane_face + sign * v, rows, :]

    for v in range(-1, 4):

        def write(rows, value, v=v):
            ends[ends_face + sign * v, rows, :] = value * on_grid if v < 0 else value

        smooth_depth_layer(flags, counted, v, ext // 8, write)
    for v in (4, 5):
        ends[ends_face + sign * v] = smoothed[smoothed_face + sign * v]

    def one_tile(tile, _):
        base = pl.multiple_of(tile * 8 + 8, 8)
        carry = empty_carry(columns)
        for k in range(1, REACH + 1):
            carry = render_layer(lambda k, rows: ends[k, rows, :], k, base, carry, scale)
        other = read_tile(behind, tile)
        front = [jnp.where(is_front, x, y) for x, y in zip(carry, other)]
        back = [jnp.where(is_front, y, x) for x, y in zip(carry, other)]
        colors = [front[n] + front[3] * back[n] for n in range(3)]
        store_tile(image, tile, colors + [front[3] * back[3]])
        return 0

    lax.fori_loop(0, ext // 8 - 2, one_tile, 0)


def whole(count):
    return [pl.BlockSpec(memory_space=pltpu.VMEM)] * count


def smem():
    return pl.BlockSpec(memory_space=pltpu.SMEM)


def in_hbm():
    return pl.BlockSpec(memory_space=pltpu.HBM)


def params(mib):
    return pltpu.CompilerParams(vmem_limit_bytes=mib * 1024 * 1024)


def cost(flops):
    return pl.CostEstimate(flops=flops, transcendentals=0, bytes_accessed=4_000_000)


def call_pack(where, c):
    layers, rows, columns = c.shape
    edge = pltpu.VMEM((REACH, 2 * PAD, columns), c.dtype)
    side = pltpu.VMEM((layers, PAD, columns), c.dtype)
    middle = pltpu.VMEM((REACH, rows - 2 * PAD, columns), c.dtype)
    return pl.pallas_call(
        pack_kernel,
        out_shape=(edge, side, edge, side, middle, middle),
        in_specs=[smem(), in_hbm()],
        out_specs=tuple(whole(6)),
        scratch_shapes=[pltpu.SemaphoreType.DMA((8,))],
        compiler_params=params(8),
        name="pack",
    )(where, c)


def call_smooth(order, c, xa, xb, by, lx):
    layers, rows, columns = c.shape
    ext = rows + 2 * PAD
    group = 4
    return pl.pallas_call(
        functools.partial(smooth_kernel, group),
        out_shape=jax.ShapeDtypeStruct((layers, ext, columns), jnp.float32),
        in_specs=[smem(), in_hbm()] + whole(4),
        out_specs=whole(1)[0],
        scratch_shapes=[
            pltpu.VMEM((layers, rows, columns), jnp.int32),
            pltpu.SemaphoreType.DMA((layers // group,)),
        ],
        compiler_params=params(24),
        cost_estimate=cost(1_000_000_000),
        name="smooth",
    )(order, c, xa, xb, by, lx)


def call_interior(scale, flags, plane):
    layers, ext, columns = plane.shape
    return pl.pallas_call(
        functools.partial(interior_kernel, scale),
        out_shape=(
            jax.ShapeDtypeStruct((4, ext - 2 * PAD, columns), jnp.float32),
            jax.ShapeDtypeStruct((layers - 8, ext, columns), jnp.float32),
        ),
        in_specs=[smem()] + whole(1),
        out_specs=tuple(whole(2)),
        compiler_params=params(24),
        cost_estimate=cost(1_000_000_000),
        name="interior",
    )(flags, plane)


def call_edge(scale, turn, flags, order, plane, *operands):
    _, ext, columns = plane.shape
    f32 = jnp.float32
    return pl.pallas_call(
        functools.partial(edge_kernel, scale, turn),
        out_shape=jax.ShapeDtypeStruct((4, ext - 2 * PAD, columns), f32),
        in_specs=[smem(), smem()] + whole(1 + len(operands)),
        out_specs=whole(1)[0],
        scratch_shapes=[
            pltpu.VMEM((REACH, ext, columns), f32),
            pltpu.VMEM((REACH + 2, ext, columns), f32),
        ],
        compiler_params=params(24),
        cost_estimate=cost(300_000_000),
    )(flags, order, plane, *operands)


def swap(value, axis, first):
    count = lax.axis_size(axis)
    pairs = []
    for low in range(first, count - 1, 2):
        pairs += [(low, low + 1), (low + 1, low)]
    return lax.ppermute(value, axis, pairs)


def over(front, back):
    through = front[3:]
    return jnp.concatenate([front[:3] + through * back[:3], through * back[3:]], 0)


def exchange(layers):
    count = lax.axis_size("depth")
    me = lax.axis_index("depth")
    _, rows, columns = layers.shape
    owned = rows // count
    parity, pair = me % 2, me // 2
    pairs = count // 2
    pieces = layers.reshape(4, pairs, 2, owned, columns)
    send = lax.dynamic_index_in_dim(pieces, 1 - parity, 2, keepdims=False)
    keep = lax.dynamic_index_in_dim(pieces, parity, 2, keepdims=False)
    got = lax.ppermute(send, "depth", [(i, i ^ 1) for i in range(count)])
    joined = jnp.where(parity == 0, over(keep, got), over(got, keep))
    parts = []
    for step in range(pairs):
        piece = lax.dynamic_index_in_dim(joined, pair ^ step, 1, keepdims=False)
        if step:
            piece = lax.ppermute(piece, "depth", [(i, i ^ (2 * step)) for i in range(count)])
        parts.append(piece)
    result = jnp.zeros((3, owned, columns), jnp.float32)
    through = jnp.ones((1, owned, columns), jnp.float32)
    for step in range(pairs):
        ahead = jnp.ones((1, owned, columns), jnp.float32)
        for other in range(pairs):
            if other != step:
                nearer = (pair ^ other) < (pair ^ step)
                ahead = ahead * jnp.where(nearer, parts[other][3:], 1.0)
        result = result + ahead * parts[step][:3]
        through = through * parts[step][3:]
    return jnp.concatenate([result, 1.0 - through], 0)


def local(counts):
    slab, rows, columns = counts.shape
    img, depth = lax.axis_index("img"), lax.axis_index("depth")
    imgs, depths = lax.axis_size("img"), lax.axis_size("depth")
    scale = 1.5 / (slab * depths)
    row_odd, depth_odd = img % 2, depth % 2
    first_a, first_b = (1 - depth_odd) * (slab - REACH), depth_odd * (slab - REACH)
    row_a, row_b = (1 - row_odd) * (rows - PAD), row_odd * (rows - PAD)
    where = jnp.stack([first_a, first_b, row_a, row_b])
    order = jnp.stack([1 - row_odd, depth_odd])
    one = jnp.float32(1.0)
    flags = jnp.stack(
        [(img > 0) * one, (img < imgs - 1) * one, (depth > 0) * one, (depth < depths - 1) * one]
    )
    by = jnp.asarray(column_matrix(columns))
    lx = jnp.asarray(row_matrices(rows))
    held = pltpu.with_memory_space_constraint(counts, pltpu.HBM)
    edge_a, side_b, edge_b, side_a, mid_a, mid_b = call_pack(where, held)
    edge_a = swap(edge_a, "depth", 0)
    edge_b = swap(edge_b, "depth", 1)
    xa = swap(side_a, "img", 0)
    xb = swap(side_b, "img", 1)
    mid_a = swap(mid_a, "depth", 0)
    mid_b = swap(mid_b, "depth", 1)
    halves = jnp.concatenate([edge_a, edge_b], 0).reshape(2 * REACH, 2, PAD, columns)
    corner_a = lax.dynamic_index_in_dim(halves, 1 - row_odd, 1, keepdims=False)
    corner_b = lax.dynamic_index_in_dim(halves, row_odd, 1, keepdims=False)
    ca = swap(corner_a, "img", 0)
    cb = swap(corner_b, "img", 1)
    plane = call_smooth(order, held, xa, xb, by, lx)
    inner, smoothed = call_interior(scale, flags, plane)
    common = (flags, order, plane, smoothed)
    layers = call_edge(
        scale, 0, *common, edge_a, mid_a, ca[:REACH], cb[:REACH], by, lx, inner
    )
    layers = call_edge(
        scale, 1, *common, edge_b, mid_b, ca[REACH:], cb[REACH:], by, lx, layers
    )
    return exchange(layers)


def solution(mesh):
    in_specs = (P("depth", "img", None),)
    out_specs = P(None, ("img", "depth"), None)
    return jax.shard_map(local, mesh=mesh, in_specs=in_specs, out_specs=out_specs, check_vma=False)
```

```python
import functools
import math

import jax
import jax.numpy as jnp
import numpy as np
from jax import lax
from jax.experimental import pallas as pl
from jax.experimental.pallas import tpu as pltpu
from jax.sharding import PartitionSpec as P


gauss_taps = [
    math.exp(-offset * offset / 8.0)
    / sum((math.exp(-other * other / 8.0) for other in range(-4, 5)))
    for offset in range(-4, 5)
]
light_z = 0.48
light_x = 0.6
light_y = 0.64


REACH = 5
PAD = 8


def band(size):
    index = np.arange(size)
    apart = np.abs(index[:, None] - index[None, :])
    taps = np.array(gauss_taps[4:] + [0.0], np.float64)
    return taps[np.minimum(apart, 5)]


def split_terms(matrix):
    high = matrix.astype(jnp.bfloat16)
    low = (matrix - high.astype(np.float64)).astype(jnp.bfloat16)
    return high, low


def column_matrix(columns):
    return np.concatenate(split_terms(band(columns)), 0)


def row_matrices(rows):
    high, low = split_terms(band(rows + 2 * PAD))
    order = np.arange(rows + 2 * PAD)
    swapped = np.concatenate([order[rows + PAD :], order[PAD : rows + PAD], order[:PAD]])
    both = []
    for columns in (order, swapped):
        both.append(np.concatenate([high[:, columns], high[:, columns], low[:, columns]], 1))
    return np.stack(both)


def smooth_plane(counts, by, lx):
    rows = counts[0].shape[0]
    exact = jnp.concatenate([c.astype(jnp.float32).astype(jnp.bfloat16) for c in counts], 0)
    half = by.shape[0] // 2
    wide = jnp.dot(exact, by[:half], preferred_element_type=jnp.float32) + jnp.dot(
        exact, by[half:], preferred_element_type=jnp.float32
    )
    high = wide.astype(jnp.bfloat16)
    low = (wide - high.astype(jnp.float32)).astype(jnp.bfloat16)
    planes = []
    for n in range(len(counts)):
        part = slice(n * rows, (n + 1) * rows)
        stacked = jnp.concatenate([high[part], low[part], high[part]], 0)
        planes.append(jnp.dot(lx, stacked, preferred_element_type=jnp.float32))
    return planes


def smooth_depth(read, k):
    total = gauss_taps[4] * read(k)
    for offset in range(1, 5):
        total = total + gauss_taps[4 + offset] * (read(k - offset) + read(k + offset))
    return total


def smooth_depth_layer(flags, read, k, tiles, write):
    for tile in range(tiles):
        rows = pl.ds(tile * 8, 8)
        value = smooth_depth(lambda j: read(j, rows), k)
        if tile == 0:
            value = value * flags[0]
        if tile == tiles - 1:
            value = value * flags[1]
        write(rows, value)


def shade_voxels(prev, mid, above, below, following, scale):
    columns = mid.shape[1]
    lane = lax.broadcasted_iota(jnp.int32, mid.shape, 1)
    right = jnp.where(lane == columns - 1, 0.0, pltpu.roll(mid, columns - 1, 1))
    left = jnp.where(lane == 0, 0.0, pltpu.roll(mid, 1, 1))
    dz = following - prev
    dx = below - above
    dy = right - left
    slope = (1.5 * light_z) * dz + (1.5 * light_x) * dx + (1.5 * light_y) * dy
    shading = 0.55 + 0.45 * jnp.tanh(slope)
    gradient_sq4 = dz * dz + dx * dx + dy * dy
    square = mid * mid
    optical = scale * (square / (1.0 + square)) * (1.0 + gradient_sq4)
    centred = mid - 2.5
    red_share = 0.5 + 0.5 * jnp.tanh(centred)
    green_share = jnp.exp(-(centred * centred))
    return optical, shading, red_share, green_share


def render_layer(layer, k, base, carry, scale):
    red, green, blue, transmit = carry
    rows = pl.ds(base, 8)
    mid = layer(k, rows)
    before = layer(k, pl.ds(base - 8, 8))
    after = layer(k, pl.ds(base + 8, 8))
    sub = lax.broadcasted_iota(jnp.int32, mid.shape, 0)
    above = pltpu.roll(jnp.where(sub == 7, before, mid), 1, 0)
    below = pltpu.roll(jnp.where(sub == 0, after, mid), 7, 0)
    optical, shading, red_share, green_share = shade_voxels(
        layer(k - 1, rows), mid, above, below, layer(k + 1, rows), scale
    )
    remaining = transmit * jnp.exp(-optical)
    lit = (transmit - remaining) * shading
    red_part = lit * red_share
    return red + red_part, green + lit * green_share, blue + (lit - red_part), remaining


def empty_carry(columns):
    zero = jnp.zeros((8, columns), jnp.float32)
    return zero, zero, zero, jnp.ones_like(zero)


def read_tile(ref, tile):
    rows = pl.ds(pl.multiple_of(tile * 8, 8), 8)
    return tuple(ref[n, rows, :] for n in range(4))


def store_tile(ref, tile, values):
    rows = pl.ds(pl.multiple_of(tile * 8, 8), 8)
    for n, value in enumerate(values):
        ref[n, rows, :] = value


def pack_kernel(where, c, edge_a, side_b, edge_b, side_a, sems):
    rows = c.shape[1]
    copies = []

    def add(source, target):
        copies.append(pltpu.make_async_copy(source, target, sems.at[len(copies)]))

    for n, (edge, side) in enumerate(((edge_a, side_a), (edge_b, side_b))):
        layers = pl.ds(where[n], REACH)
        add(c.at[layers, pl.ds(0, PAD)], edge.at[:, pl.ds(0, PAD)])
        add(c.at[layers, pl.ds(rows - PAD, PAD)], edge.at[:, pl.ds(PAD, PAD)])
        add(c.at[:, pl.ds(pl.multiple_of(where[2 + n], PAD), PAD)], side)
    for copy in copies:
        copy.start()
    for copy in copies:
        copy.wait()


def smooth_kernel(group, order, c_hbm, xa, xb, by, lx, plane, c, sems):
    groups = c.shape[0] // group
    rows_of = order[0]

    def fetch(g):
        part = pl.ds(g * group, group)
        return pltpu.make_async_copy(c_hbm.at[part], c.at[part], sems.at[g])

    for g in range(groups):
        fetch(g).start()

    def smooth_group(g, _):
        first = g * group
        fetch(g).wait()
        counts = [
            jnp.concatenate([xa[first + n], c[first + n], xb[first + n]], 0) for n in range(group)
        ]
        for n, value in enumerate(smooth_plane(counts, by, lx[rows_of])):
            plane[first + n] = value
        return 0

    lax.fori_loop(0, groups, smooth_group, 0)


def interior_kernel(scale, flags, plane, image, smoothed):
    layers, ext, columns = plane.shape

    def one_layer(j, _):
        def write(rows, value):
            smoothed[j, rows, :] = value

        smooth_depth_layer(flags, lambda k, rows: plane[k, rows, :], j + 4, ext // 8, write)
        return 0

    lax.fori_loop(0, layers - 8, one_layer, 0)

    def one_tile(tile, _):
        base = pl.multiple_of(tile * 8 + 8, 8)
        carry = empty_carry(columns)
        for k in range(1, layers - 9):
            carry = render_layer(lambda k, rows: smoothed[k, rows, :], k, base, carry, scale)
        store_tile(image, tile, carry)
        return 0

    lax.fori_loop(0, ext // 8 - 2, one_tile, 0)


def edge_smooth(turn, flags, order, plane, smoothed, edge, middle, ca, cb, by, lx, ends, halo):
    layers, ext, _ = plane.shape
    rows_of = order[0]
    is_front = order[1] == 1 - turn
    sign = jnp.where(is_front, 1, -1)
    counts = [
        jnp.concatenate([ca[j], edge[j, :PAD], middle[j], edge[j, PAD:], cb[j]], 0)
        for j in range(REACH)
    ]
    for j, value in enumerate(smooth_plane(counts, by, lx[rows_of])):
        halo[j] = value
    plane_face = jnp.where(is_front, 0, layers - 1)
    halo_face = jnp.where(is_front, REACH, -1)
    ends_face = jnp.where(is_front, 1, REACH)
    smoothed_face = jnp.where(is_front, -4, layers - 5)
    on_grid = jnp.where(is_front, flags[2], flags[3])

    def counted(v, rows):
        if v < 0:
            return halo[halo_face + sign * v, rows, :]
        return plane[plane_face + sign * v, rows, :]

    for v in range(-1, 4):

        def write(rows, value, v=v):
            ends[ends_face + sign * v, rows, :] = value * on_grid if v < 0 else value

        smooth_depth_layer(flags, counted, v, ext // 8, write)
    for v in (4, 5):
        ends[ends_face + sign * v] = smoothed[smoothed_face + sign * v]


def edge_render(scale, is_front, ends, behind, image, tiles, tile_of):
    columns = ends.shape[2]

    def one_tile(place, _):
        tile = tile_of(place)
        base = pl.multiple_of(tile * 8 + 8, 8)
        carry = empty_carry(columns)
        for k in range(1, REACH + 1):
            carry = render_layer(lambda k, rows: ends[k, rows, :], k, base, carry, scale)
        other = read_tile(behind, tile)
        front = [jnp.where(is_front, x, y) for x, y in zip(carry, other)]
        back = [jnp.where(is_front, y, x) for x, y in zip(carry, other)]
        colors = [front[n] + front[3] * back[n] for n in range(3)]
        store_tile(image, place, colors + [front[3] * back[3]])
        return 0

    lax.fori_loop(0, tiles, one_tile, 0)


def half_tiles(owner_tiles, wanted):
    def tile_of(place):
        return (place // owner_tiles * 2 + wanted) * owner_tiles + place % owner_tiles

    return tile_of


def first_edge_kernel(scale, flags, order, plane, smoothed, edge, middle, ca, cb, by, lx, behind,
                      image, ends, halo):
    edge_smooth(0, flags, order, plane, smoothed, edge, middle, ca, cb, by, lx, ends, halo)
    tiles = plane.shape[1] // 8 - 2
    edge_render(scale, order[1] == 1, ends, behind, image, tiles, lambda place: place)


def last_edge_kernel(scale, owner_tiles, flags, order, plane, smoothed, edge, middle, ca, cb, by,
                     lx, behind, image, ends, halo):
    edge_smooth(1, flags, order, plane, smoothed, edge, middle, ca, cb, by, lx, ends, halo)
    tiles = plane.shape[1] // 8 - 2
    tile_of = lambda place: place
    if owner_tiles:
        tiles, tile_of = tiles // 2, half_tiles(owner_tiles, 1 - order[1])
    edge_render(scale, order[1] == 0, ends, behind, image, tiles, tile_of)


def kept_edge_kernel(scale, owner_tiles, order, ends, behind, image):
    tiles = ends.shape[1] // 8 - 2
    tile_of = half_tiles(owner_tiles, order[1])
    edge_render(scale, order[1] == 0, ends, behind, image, tiles // 2, tile_of)


def whole(count):
    return [pl.BlockSpec(memory_space=pltpu.VMEM)] * count


def smem():
    return pl.BlockSpec(memory_space=pltpu.SMEM)


def in_hbm():
    return pl.BlockSpec(memory_space=pltpu.HBM)


def params(mib):
    return pltpu.CompilerParams(vmem_limit_bytes=mib * 1024 * 1024)


def cost(flops):
    return pl.CostEstimate(flops=flops, transcendentals=0, bytes_accessed=4_000_000)


def call_pack(where, c):
    layers, _, columns = c.shape
    edge = pltpu.VMEM((REACH, 2 * PAD, columns), c.dtype)
    side = pltpu.VMEM((layers, PAD, columns), c.dtype)
    return pl.pallas_call(
        pack_kernel,
        out_shape=(edge, side, edge, side),
        in_specs=[smem(), in_hbm()],
        out_specs=tuple(whole(4)),
        scratch_shapes=[pltpu.SemaphoreType.DMA((6,))],
        compiler_params=params(8),
        name="pack",
    )(where, c)


def call_smooth(order, c, xa, xb, by, lx):
    layers, rows, columns = c.shape
    ext = rows + 2 * PAD
    group = 8
    return pl.pallas_call(
        functools.partial(smooth_kernel, group),
        out_shape=jax.ShapeDtypeStruct((layers, ext, columns), jnp.float32),
        in_specs=[smem(), in_hbm()] + whole(4),
        out_specs=whole(1)[0],
        scratch_shapes=[
            pltpu.VMEM((layers, rows, columns), jnp.int32),
            pltpu.SemaphoreType.DMA((layers // group,)),
        ],
        compiler_params=params(24),
        cost_estimate=cost(1_000_000_000),
        name="smooth",
    )(order, c, xa, xb, by, lx)


def call_interior(scale, flags, plane):
    layers, ext, columns = plane.shape
    return pl.pallas_call(
        functools.partial(interior_kernel, scale),
        out_shape=(
            jax.ShapeDtypeStruct((4, ext - 2 * PAD, columns), jnp.float32),
            jax.ShapeDtypeStruct((layers - 8, ext, columns), jnp.float32),
        ),
        in_specs=[smem()] + whole(1),
        out_specs=tuple(whole(2)),
        compiler_params=params(24),
        cost_estimate=cost(1_000_000_000),
        name="interior",
    )(flags, plane)


def call_first_edge(scale, flags, order, plane, *operands):
    _, ext, columns = plane.shape
    f32 = jnp.float32
    return pl.pallas_call(
        functools.partial(first_edge_kernel, scale),
        out_shape=jax.ShapeDtypeStruct((4, ext - 2 * PAD, columns), f32),
        in_specs=[smem(), smem()] + whole(1 + len(operands)),
        out_specs=whole(1)[0],
        scratch_shapes=[
            pltpu.VMEM((REACH + 2, ext, columns), f32),
            pltpu.VMEM((REACH, ext, columns), f32),
        ],
        compiler_params=params(24),
        cost_estimate=cost(300_000_000),
        name="first_edge",
    )(flags, order, plane, *operands)


def call_last_edge(scale, owner_tiles, flags, order, plane, *operands):
    _, ext, columns = plane.shape
    f32 = jnp.float32
    rows = (ext - 2 * PAD) // (2 if owner_tiles else 1)
    return pl.pallas_call(
        functools.partial(last_edge_kernel, scale, owner_tiles),
        out_shape=(
            jax.ShapeDtypeStruct((4, rows, columns), f32),
            jax.ShapeDtypeStruct((REACH + 2, ext, columns), f32),
        ),
        in_specs=[smem(), smem()] + whole(1 + len(operands)),
        out_specs=tuple(whole(2)),
        scratch_shapes=[pltpu.VMEM((REACH, ext, columns), f32)],
        compiler_params=params(24),
        cost_estimate=cost(300_000_000),
        name="last_edge",
    )(flags, order, plane, *operands)


def call_kept_edge(scale, owner_tiles, order, ends, behind):
    _, ext, columns = ends.shape
    return pl.pallas_call(
        functools.partial(kept_edge_kernel, scale, owner_tiles),
        out_shape=jax.ShapeDtypeStruct((4, (ext - 2 * PAD) // 2, columns), jnp.float32),
        in_specs=[smem()] + whole(2),
        out_specs=whole(1)[0],
        compiler_params=params(24),
        cost_estimate=cost(200_000_000),
        name="kept_edge",
    )(order, ends, behind)


def swap(value, axis, first):
    count = lax.axis_size(axis)
    pairs = []
    for low in range(first, count - 1, 2):
        pairs += [(low, low + 1), (low + 1, low)]
    return lax.ppermute(value, axis, pairs)


def over(front, back):
    through = front[3:]
    return jnp.concatenate([front[:3] + through * back[:3], through * back[3:]], 0)


def halves_of(layers):
    count = lax.axis_size("depth")
    parity = lax.axis_index("depth") % 2
    _, rows, columns = layers.shape
    pieces = layers.reshape(4, count // 2, 2, rows // count, columns)
    send = lax.dynamic_index_in_dim(pieces, 1 - parity, 2, keepdims=False)
    keep = lax.dynamic_index_in_dim(pieces, parity, 2, keepdims=False)
    return send, keep


def exchange(send, keep):
    count = lax.axis_size("depth")
    me = lax.axis_index("depth")
    parity, pair = me % 2, me // 2
    pairs = count // 2
    send, keep = (value.reshape(4, pairs, -1, value.shape[-1]) for value in (send, keep))
    owned, columns = send.shape[2:]
    got = swap(send, "depth", 0)
    joined = jnp.where(parity == 0, over(keep, got), over(got, keep))
    parts = []
    for step in range(pairs):
        piece = lax.dynamic_index_in_dim(joined, pair ^ step, 1, keepdims=False)
        if step:
            piece = lax.ppermute(piece, "depth", [(i, i ^ (2 * step)) for i in range(count)])
        parts.append(piece)
    result = jnp.zeros((3, owned, columns), jnp.float32)
    through = jnp.ones((1, owned, columns), jnp.float32)
    for step in range(pairs):
        ahead = jnp.ones((1, owned, columns), jnp.float32)
        for other in range(pairs):
            if other != step:
                nearer = (pair ^ other) < (pair ^ step)
                ahead = ahead * jnp.where(nearer, parts[other][3:], 1.0)
        result = result + ahead * parts[step][:3]
        through = through * parts[step][3:]
    return jnp.concatenate([result, 1.0 - through], 0)


def local(counts):
    slab, rows, columns = counts.shape
    img, depth = lax.axis_index("img"), lax.axis_index("depth")
    imgs, depths = lax.axis_size("img"), lax.axis_size("depth")
    scale = 1.5 / (slab * depths)
    row_odd, depth_odd = img % 2, depth % 2
    first_a, first_b = (1 - depth_odd) * (slab - REACH), depth_odd * (slab - REACH)
    row_a, row_b = (1 - row_odd) * (rows - PAD), row_odd * (rows - PAD)
    where = jnp.stack([first_a, first_b, row_a, row_b])
    order = jnp.stack([1 - row_odd, depth_odd])
    one = jnp.float32(1.0)
    flags = jnp.stack(
        [(img > 0) * one, (img < imgs - 1) * one, (depth > 0) * one, (depth < depths - 1) * one]
    )
    by = jnp.asarray(column_matrix(columns))
    lx = jnp.asarray(row_matrices(rows))
    held = pltpu.with_memory_space_constraint(counts, pltpu.HBM)
    mid_a = lax.dynamic_slice(counts, (first_a, PAD, 0), (REACH, rows - 2 * PAD, columns))
    edge_a, side_b, edge_b, side_a = call_pack(where, held)
    later, edge_a = lax.optimization_barrier((counts, edge_a))
    mid_b = lax.dynamic_slice(later, (first_b, PAD, 0), (REACH, rows - 2 * PAD, columns))
    edge_a = swap(edge_a, "depth", 0)
    edge_b = swap(edge_b, "depth", 1)
    xa = swap(side_a, "img", 0)
    xb = swap(side_b, "img", 1)
    mid_a = swap(mid_a, "depth", 0)
    mid_b = swap(mid_b, "depth", 1)
    halves = jnp.concatenate([edge_a, edge_b], 0).reshape(2 * REACH, 2, PAD, columns)
    corner_a = lax.dynamic_index_in_dim(halves, 1 - row_odd, 1, keepdims=False)
    corner_b = lax.dynamic_index_in_dim(halves, row_odd, 1, keepdims=False)
    ca = swap(corner_a, "img", 0)
    cb = swap(corner_b, "img", 1)
    plane = call_smooth(order, held, xa, xb, by, lx)
    inner, smoothed = call_interior(scale, flags, plane)
    owned = rows // depths
    owner_tiles = owned // 8 if owned % 8 == 0 else 0
    common = (flags, order, plane, smoothed)
    layers = call_first_edge(
        scale, *common, edge_a, mid_a, ca[:REACH], cb[:REACH], by, lx, inner
    )
    send, ends = call_last_edge(
        scale, owner_tiles, *common, edge_b, mid_b, ca[REACH:], cb[REACH:], by, lx, layers
    )
    if owner_tiles:
        keep = call_kept_edge(scale, owner_tiles, order, ends, layers)
    else:
        send, keep = halves_of(send)
    return exchange(send, keep)


def solution(mesh):
    in_specs = (P("depth", "img", None),)
    out_specs = P(None, ("img", "depth"), None)
    return jax.shard_map(local, mesh=mesh, in_specs=in_specs, out_specs=out_specs, check_vma=False)
```

```python
import functools
import math

import jax
import jax.numpy as jnp
import numpy as np
from jax import lax
from jax.experimental import pallas as pl
from jax.experimental.pallas import tpu as pltpu
from jax.sharding import PartitionSpec as P


gauss_taps = [
    math.exp(-offset * offset / 8.0)
    / sum((math.exp(-other * other / 8.0) for other in range(-4, 5)))
    for offset in range(-4, 5)
]
light_z = 0.48
light_x = 0.6
light_y = 0.64


REACH = 5
PAD = 8


def band(size):
    index = np.arange(size)
    apart = np.abs(index[:, None] - index[None, :])
    taps = np.array(gauss_taps[4:] + [0.0], np.float64)
    return taps[np.minimum(apart, 5)]


def split_terms(matrix):
    high = matrix.astype(jnp.bfloat16)
    low = (matrix - high.astype(np.float64)).astype(jnp.bfloat16)
    return high, low


def column_matrix(columns):
    return np.concatenate(split_terms(band(columns)), 0)


def row_matrices(rows):
    high, low = split_terms(band(rows + 2 * PAD))
    order = np.arange(rows + 2 * PAD)
    swapped = np.concatenate([order[rows + PAD :], order[PAD : rows + PAD], order[:PAD]])
    both = []
    for columns in (order, swapped):
        both.append(np.concatenate([high[:, columns], high[:, columns], low[:, columns]], 1))
    return np.stack(both)


def smooth_plane(counts, by, lx):
    rows = counts[0].shape[0]
    exact = jnp.concatenate([c.astype(jnp.float32).astype(jnp.bfloat16) for c in counts], 0)
    half = by.shape[0] // 2
    wide = jnp.dot(exact, by[:half], preferred_element_type=jnp.float32) + jnp.dot(
        exact, by[half:], preferred_element_type=jnp.float32
    )
    high = wide.astype(jnp.bfloat16)
    low = (wide - high.astype(jnp.float32)).astype(jnp.bfloat16)
    planes = []
    for n in range(len(counts)):
        part = slice(n * rows, (n + 1) * rows)
        stacked = jnp.concatenate([high[part], low[part], high[part]], 0)
        planes.append(jnp.dot(lx, stacked, preferred_element_type=jnp.float32))
    return planes


def smooth_depth(read, k):
    total = gauss_taps[4] * read(k)
    for offset in range(1, 5):
        total = total + gauss_taps[4 + offset] * (read(k - offset) + read(k + offset))
    return total


def smooth_depth_layer(flags, read, k, tiles, write):
    for tile in range(tiles):
        rows = pl.ds(tile * 8, 8)
        value = smooth_depth(lambda j: read(j, rows), k)
        if tile == 0:
            value = value * flags[0]
        if tile == tiles - 1:
            value = value * flags[1]
        write(rows, value)


def shade_voxels(prev, mid, above, below, following, scale):
    columns = mid.shape[1]
    lane = lax.broadcasted_iota(jnp.int32, mid.shape, 1)
    right = jnp.where(lane == columns - 1, 0.0, pltpu.roll(mid, columns - 1, 1))
    left = jnp.where(lane == 0, 0.0, pltpu.roll(mid, 1, 1))
    dz = following - prev
    dx = below - above
    dy = right - left
    slope = (1.5 * light_z) * dz + (1.5 * light_x) * dx + (1.5 * light_y) * dy
    shading = 0.55 + 0.45 * jnp.tanh(slope)
    gradient_sq4 = dz * dz + dx * dx + dy * dy
    square = mid * mid
    optical = scale * (square / (1.0 + square)) * (1.0 + gradient_sq4)
    centred = mid - 2.5
    red_share = 0.5 + 0.5 * jnp.tanh(centred)
    green_share = jnp.exp(-(centred * centred))
    return optical, shading, red_share, green_share


def render_layer(layer, k, base, carry, scale):
    red, green, blue, transmit = carry
    rows = pl.ds(base, 8)
    mid = layer(k, rows)
    before = layer(k, pl.ds(base - 8, 8))
    after = layer(k, pl.ds(base + 8, 8))
    sub = lax.broadcasted_iota(jnp.int32, mid.shape, 0)
    above = pltpu.roll(jnp.where(sub == 7, before, mid), 1, 0)
    below = pltpu.roll(jnp.where(sub == 0, after, mid), 7, 0)
    optical, shading, red_share, green_share = shade_voxels(
        layer(k - 1, rows), mid, above, below, layer(k + 1, rows), scale
    )
    remaining = transmit * jnp.exp(-optical)
    lit = (transmit - remaining) * shading
    red_part = lit * red_share
    return red + red_part, green + lit * green_share, blue + (lit - red_part), remaining


def empty_carry(columns):
    zero = jnp.zeros((8, columns), jnp.float32)
    return zero, zero, zero, jnp.ones_like(zero)


def read_tile(ref, tile):
    rows = pl.ds(pl.multiple_of(tile * 8, 8), 8)
    return tuple(ref[n, rows, :] for n in range(4))


def store_tile(ref, tile, values):
    rows = pl.ds(pl.multiple_of(tile * 8, 8), 8)
    for n, value in enumerate(values):
        ref[n, rows, :] = value


def pack_kernel(where, c, edge_a, side_b, edge_b, side_a, middle_a, middle_b, sems):
    rows = c.shape[1]
    copies = []

    def add(source, target):
        copies.append(pltpu.make_async_copy(source, target, sems.at[len(copies)]))

    blocks = ((edge_a, side_a, middle_a), (edge_b, side_b, middle_b))
    for n, (edge, side, middle) in enumerate(blocks):
        layers = pl.ds(where[n], REACH)
        add(c.at[layers, pl.ds(0, PAD)], edge.at[:, pl.ds(0, PAD)])
        add(c.at[layers, pl.ds(rows - PAD, PAD)], edge.at[:, pl.ds(PAD, PAD)])
        add(c.at[:, pl.ds(pl.multiple_of(where[2 + n], PAD), PAD)], side)
        add(c.at[layers, pl.ds(PAD, rows - 2 * PAD)], middle)
    for copy in copies:
        copy.start()
    for copy in copies:
        copy.wait()


def smooth_kernel(group, order, c_hbm, xa, xb, by, lx, plane, c, sems):
    groups = c.shape[0] // group
    rows_of = order[0]

    def fetch(g):
        part = pl.ds(g * group, group)
        return pltpu.make_async_copy(c_hbm.at[part], c.at[part], sems.at[g])

    for g in range(groups):
        fetch(g).start()

    def smooth_group(g, _):
        first = g * group
        fetch(g).wait()
        counts = [
            jnp.concatenate([xa[first + n], c[first + n], xb[first + n]], 0) for n in range(group)
        ]
        for n, value in enumerate(smooth_plane(counts, by, lx[rows_of])):
            plane[first + n] = value
        return 0

    lax.fori_loop(0, groups, smooth_group, 0)


def interior_kernel(scale, flags, plane, image, smoothed):
    layers, ext, columns = plane.shape

    def one_layer(j, _):
        def write(rows, value):
            smoothed[j, rows, :] = value

        smooth_depth_layer(flags, lambda k, rows: plane[k, rows, :], j + 4, ext // 8, write)
        return 0

    lax.fori_loop(0, layers - 8, one_layer, 0)

    def one_tile(tile, _):
        base = pl.multiple_of(tile * 8 + 8, 8)
        carry = empty_carry(columns)
        for k in range(1, layers - 9):
            carry = render_layer(lambda k, rows: smoothed[k, rows, :], k, base, carry, scale)
        store_tile(image, tile, carry)
        return 0

    lax.fori_loop(0, ext // 8 - 2, one_tile, 0)


def edge_smooth(turn, flags, order, plane, smoothed, edge, middle, ca, cb, by, lx, ends, halo):
    layers, ext, _ = plane.shape
    rows_of = order[0]
    is_front = order[1] == 1 - turn
    sign = jnp.where(is_front, 1, -1)
    counts = [
        jnp.concatenate([ca[j], edge[j, :PAD], middle[j], edge[j, PAD:], cb[j]], 0)
        for j in range(REACH)
    ]
    for j, value in enumerate(smooth_plane(counts, by, lx[rows_of])):
        halo[j] = value
    plane_face = jnp.where(is_front, 0, layers - 1)
    halo_face = jnp.where(is_front, REACH, -1)
    ends_face = jnp.where(is_front, 1, REACH)
    smoothed_face = jnp.where(is_front, -4, layers - 5)
    on_grid = jnp.where(is_front, flags[2], flags[3])

    def counted(v, rows):
        if v < 0:
            return halo[halo_face + sign * v, rows, :]
        return plane[plane_face + sign * v, rows, :]

    for v in range(-1, 4):

        def write(rows, value, v=v):
            ends[ends_face + sign * v, rows, :] = value * on_grid if v < 0 else value

        smooth_depth_layer(flags, counted, v, ext // 8, write)
    for v in (4, 5):
        ends[ends_face + sign * v] = smoothed[smoothed_face + sign * v]


def edge_render(scale, is_front, ends, behind, image, tiles, tile_of):
    columns = ends.shape[2]

    def one_tile(place, _):
        tile = tile_of(place)
        base = pl.multiple_of(tile * 8 + 8, 8)
        carry = empty_carry(columns)
        for k in range(1, REACH + 1):
            carry = render_layer(lambda k, rows: ends[k, rows, :], k, base, carry, scale)
        other = read_tile(behind, tile)
        front = [jnp.where(is_front, x, y) for x, y in zip(carry, other)]
        back = [jnp.where(is_front, y, x) for x, y in zip(carry, other)]
        colors = [front[n] + front[3] * back[n] for n in range(3)]
        store_tile(image, place, colors + [front[3] * back[3]])
        return 0

    lax.fori_loop(0, tiles, one_tile, 0)


def half_tiles(owner_tiles, wanted):
    def tile_of(place):
        return (place // owner_tiles * 2 + wanted) * owner_tiles + place % owner_tiles

    return tile_of


def first_edge_kernel(scale, flags, order, plane, smoothed, edge, middle, ca, cb, by, lx, behind,
                      image, ends, halo):
    edge_smooth(0, flags, order, plane, smoothed, edge, middle, ca, cb, by, lx, ends, halo)
    tiles = plane.shape[1] // 8 - 2
    edge_render(scale, order[1] == 1, ends, behind, image, tiles, lambda place: place)


def last_edge_kernel(scale, owner_tiles, flags, order, plane, smoothed, edge, middle, ca, cb, by,
                     lx, behind, image, ends, halo):
    edge_smooth(1, flags, order, plane, smoothed, edge, middle, ca, cb, by, lx, ends, halo)
    tiles = plane.shape[1] // 8 - 2
    tile_of = lambda place: place
    if owner_tiles:
        tiles, tile_of = tiles // 2, half_tiles(owner_tiles, 1 - order[1])
    edge_render(scale, order[1] == 0, ends, behind, image, tiles, tile_of)


def kept_edge_kernel(scale, owner_tiles, order, ends, behind, image):
    tiles = ends.shape[1] // 8 - 2
    tile_of = half_tiles(owner_tiles, order[1])
    edge_render(scale, order[1] == 0, ends, behind, image, tiles // 2, tile_of)


def whole(count):
    return [pl.BlockSpec(memory_space=pltpu.VMEM)] * count


def smem():
    return pl.BlockSpec(memory_space=pltpu.SMEM)


def in_hbm():
    return pl.BlockSpec(memory_space=pltpu.HBM)


def params(mib):
    return pltpu.CompilerParams(vmem_limit_bytes=mib * 1024 * 1024)


def cost(flops):
    return pl.CostEstimate(flops=flops, transcendentals=0, bytes_accessed=4_000_000)


def call_pack(where, c):
    layers, rows, columns = c.shape
    edge = pltpu.VMEM((REACH, 2 * PAD, columns), c.dtype)
    side = pltpu.VMEM((layers, PAD, columns), c.dtype)
    middle = pltpu.VMEM((REACH, rows - 2 * PAD, columns), c.dtype)
    return pl.pallas_call(
        pack_kernel,
        out_shape=(edge, side, edge, side, middle, middle),
        in_specs=[smem(), in_hbm()],
        out_specs=tuple(whole(6)),
        scratch_shapes=[pltpu.SemaphoreType.DMA((8,))],
        compiler_params=params(8),
        name="pack",
    )(where, c)


def call_smooth(order, c, xa, xb, by, lx):
    layers, rows, columns = c.shape
    ext = rows + 2 * PAD
    group = 8
    return pl.pallas_call(
        functools.partial(smooth_kernel, group),
        out_shape=jax.ShapeDtypeStruct((layers, ext, columns), jnp.float32),
        in_specs=[smem(), in_hbm()] + whole(4),
        out_specs=whole(1)[0],
        scratch_shapes=[
            pltpu.VMEM((layers, rows, columns), jnp.int32),
            pltpu.SemaphoreType.DMA((layers // group,)),
        ],
        compiler_params=params(24),
        cost_estimate=cost(1_000_000_000),
        name="smooth",
    )(order, c, xa, xb, by, lx)


def call_interior(scale, flags, plane):
    layers, ext, columns = plane.shape
    return pl.pallas_call(
        functools.partial(interior_kernel, scale),
        out_shape=(
            jax.ShapeDtypeStruct((4, ext - 2 * PAD, columns), jnp.float32),
            jax.ShapeDtypeStruct((layers - 8, ext, columns), jnp.float32),
        ),
        in_specs=[smem()] + whole(1),
        out_specs=tuple(whole(2)),
        compiler_params=params(24),
        cost_estimate=cost(1_000_000_000),
        name="interior",
    )(flags, plane)


def call_first_edge(scale, flags, order, plane, *operands):
    _, ext, columns = plane.shape
    f32 = jnp.float32
    return pl.pallas_call(
        functools.partial(first_edge_kernel, scale),
        out_shape=jax.ShapeDtypeStruct((4, ext - 2 * PAD, columns), f32),
        in_specs=[smem(), smem()] + whole(1 + len(operands)),
        out_specs=whole(1)[0],
        scratch_shapes=[
            pltpu.VMEM((REACH + 2, ext, columns), f32),
            pltpu.VMEM((REACH, ext, columns), f32),
        ],
        compiler_params=params(24),
        cost_estimate=cost(300_000_000),
        name="first_edge",
    )(flags, order, plane, *operands)


def call_last_edge(scale, owner_tiles, flags, order, plane, *operands):
    _, ext, columns = plane.shape
    f32 = jnp.float32
    rows = (ext - 2 * PAD) // (2 if owner_tiles else 1)
    return pl.pallas_call(
        functools.partial(last_edge_kernel, scale, owner_tiles),
        out_shape=(
            jax.ShapeDtypeStruct((4, rows, columns), f32),
            jax.ShapeDtypeStruct((REACH + 2, ext, columns), f32),
        ),
        in_specs=[smem(), smem()] + whole(1 + len(operands)),
        out_specs=tuple(whole(2)),
        scratch_shapes=[pltpu.VMEM((REACH, ext, columns), f32)],
        compiler_params=params(24),
        cost_estimate=cost(300_000_000),
        name="last_edge",
    )(flags, order, plane, *operands)


def call_kept_edge(scale, owner_tiles, order, ends, behind):
    _, ext, columns = ends.shape
    return pl.pallas_call(
        functools.partial(kept_edge_kernel, scale, owner_tiles),
        out_shape=jax.ShapeDtypeStruct((4, (ext - 2 * PAD) // 2, columns), jnp.float32),
        in_specs=[smem()] + whole(2),
        out_specs=whole(1)[0],
        compiler_params=params(24),
        cost_estimate=cost(200_000_000),
        name="kept_edge",
    )(order, ends, behind)


def swap(value, axis, first):
    count = lax.axis_size(axis)
    pairs = []
    for low in range(first, count - 1, 2):
        pairs += [(low, low + 1), (low + 1, low)]
    return lax.ppermute(value, axis, pairs)


def over(front, back):
    through = front[3:]
    return jnp.concatenate([front[:3] + through * back[:3], through * back[3:]], 0)


def halves_of(layers):
    count = lax.axis_size("depth")
    parity = lax.axis_index("depth") % 2
    _, rows, columns = layers.shape
    pieces = layers.reshape(4, count // 2, 2, rows // count, columns)
    send = lax.dynamic_index_in_dim(pieces, 1 - parity, 2, keepdims=False)
    keep = lax.dynamic_index_in_dim(pieces, parity, 2, keepdims=False)
    return send, keep


def exchange(send, keep):
    count = lax.axis_size("depth")
    me = lax.axis_index("depth")
    parity, pair = me % 2, me // 2
    pairs = count // 2
    send, keep = (value.reshape(4, pairs, -1, value.shape[-1]) for value in (send, keep))
    owned, columns = send.shape[2:]
    got = swap(send, "depth", 0)
    joined = jnp.where(parity == 0, over(keep, got), over(got, keep))
    parts = []
    for step in range(pairs):
        piece = lax.dynamic_index_in_dim(joined, pair ^ step, 1, keepdims=False)
        if step:
            piece = lax.ppermute(piece, "depth", [(i, i ^ (2 * step)) for i in range(count)])
        parts.append(piece)
    result = jnp.zeros((3, owned, columns), jnp.float32)
    through = jnp.ones((1, owned, columns), jnp.float32)
    for step in range(pairs):
        ahead = jnp.ones((1, owned, columns), jnp.float32)
        for other in range(pairs):
            if other != step:
                nearer = (pair ^ other) < (pair ^ step)
                ahead = ahead * jnp.where(nearer, parts[other][3:], 1.0)
        result = result + ahead * parts[step][:3]
        through = through * parts[step][3:]
    return jnp.concatenate([result, 1.0 - through], 0)


def local(counts):
    slab, rows, columns = counts.shape
    img, depth = lax.axis_index("img"), lax.axis_index("depth")
    imgs, depths = lax.axis_size("img"), lax.axis_size("depth")
    scale = 1.5 / (slab * depths)
    row_odd, depth_odd = img % 2, depth % 2
    first_a, first_b = (1 - depth_odd) * (slab - REACH), depth_odd * (slab - REACH)
    row_a, row_b = (1 - row_odd) * (rows - PAD), row_odd * (rows - PAD)
    where = jnp.stack([first_a, first_b, row_a, row_b])
    order = jnp.stack([1 - row_odd, depth_odd])
    one = jnp.float32(1.0)
    flags = jnp.stack(
        [(img > 0) * one, (img < imgs - 1) * one, (depth > 0) * one, (depth < depths - 1) * one]
    )
    by = jnp.asarray(column_matrix(columns))
    lx = jnp.asarray(row_matrices(rows))
    held = pltpu.with_memory_space_constraint(counts, pltpu.HBM)
    edge_a, side_b, edge_b, side_a, mid_a, mid_b = call_pack(where, held)
    edge_a = swap(edge_a, "depth", 0)
    edge_b = swap(edge_b, "depth", 1)
    xa = swap(side_a, "img", 0)
    xb = swap(side_b, "img", 1)
    mid_a = swap(mid_a, "depth", 0)
    mid_b = swap(mid_b, "depth", 1)
    halves = jnp.concatenate([edge_a, edge_b], 0).reshape(2 * REACH, 2, PAD, columns)
    corner_a = lax.dynamic_index_in_dim(halves, 1 - row_odd, 1, keepdims=False)
    corner_b = lax.dynamic_index_in_dim(halves, row_odd, 1, keepdims=False)
    ca = swap(corner_a, "img", 0)
    cb = swap(corner_b, "img", 1)
    plane = call_smooth(order, held, xa, xb, by, lx)
    inner, smoothed = call_interior(scale, flags, plane)
    owned = rows // depths
    owner_tiles = owned // 8 if owned % 8 == 0 else 0
    common = (flags, order, plane, smoothed)
    layers = call_first_edge(
        scale, *common, edge_a, mid_a, ca[:REACH], cb[:REACH], by, lx, inner
    )
    send, ends = call_last_edge(
        scale, owner_tiles, *common, edge_b, mid_b, ca[REACH:], cb[REACH:], by, lx, layers
    )
    if owner_tiles:
        keep = call_kept_edge(scale, owner_tiles, order, ends, layers)
    else:
        send, keep = halves_of(send)
    return exchange(send, keep)


def solution(mesh):
    in_specs = (P("depth", "img", None),)
    out_specs = P(None, ("img", "depth"), None)
    return jax.shard_map(local, mesh=mesh, in_specs=in_specs, out_specs=out_specs, check_vma=False)
```

```python
import functools
import math

import jax
import jax.numpy as jnp
import numpy as np
from jax import lax
from jax.experimental import pallas as pl
from jax.experimental.pallas import tpu as pltpu
from jax.sharding import PartitionSpec as P


gauss_taps = [
    math.exp(-offset * offset / 8.0)
    / sum((math.exp(-other * other / 8.0) for other in range(-4, 5)))
    for offset in range(-4, 5)
]
light_z = 0.48
light_x = 0.6
light_y = 0.64


REACH = 5
PAD = 8


def band(size):
    index = np.arange(size)
    apart = np.abs(index[:, None] - index[None, :])
    taps = np.array(gauss_taps[4:] + [0.0], np.float64)
    return taps[np.minimum(apart, 5)]


def split_terms(matrix):
    high = matrix.astype(jnp.bfloat16)
    low = (matrix - high.astype(np.float64)).astype(jnp.bfloat16)
    return high, low


def column_matrix(columns):
    return np.concatenate(split_terms(band(columns)), 0)


def row_matrices(rows):
    high, low = split_terms(band(rows + 2 * PAD))
    order = np.arange(rows + 2 * PAD)
    swapped = np.concatenate([order[rows + PAD :], order[PAD : rows + PAD], order[:PAD]])
    both = []
    for columns in (order, swapped):
        both.append(np.concatenate([high[:, columns], high[:, columns], low[:, columns]], 1))
    return np.stack(both)


def smooth_plane(counts, by, lx):
    rows = counts[0].shape[0]
    exact = jnp.concatenate([c.astype(jnp.float32).astype(jnp.bfloat16) for c in counts], 0)
    half = by.shape[0] // 2
    wide = jnp.dot(exact, by[:half], preferred_element_type=jnp.float32) + jnp.dot(
        exact, by[half:], preferred_element_type=jnp.float32
    )
    high = wide.astype(jnp.bfloat16)
    low = (wide - high.astype(jnp.float32)).astype(jnp.bfloat16)
    planes = []
    for n in range(len(counts)):
        part = slice(n * rows, (n + 1) * rows)
        stacked = jnp.concatenate([high[part], low[part], high[part]], 0)
        planes.append(jnp.dot(lx, stacked, preferred_element_type=jnp.float32))
    return planes


def smooth_depth(read, k):
    total = gauss_taps[4] * read(k)
    for offset in range(1, 5):
        total = total + gauss_taps[4 + offset] * (read(k - offset) + read(k + offset))
    return total


def smooth_depth_layer(flags, read, k, tiles, write):
    for tile in range(tiles):
        rows = pl.ds(tile * 8, 8)
        value = smooth_depth(lambda j: read(j, rows), k)
        if tile == 0:
            value = value * flags[0]
        if tile == tiles - 1:
            value = value * flags[1]
        write(rows, value)


def shade_voxels(prev, mid, above, below, following, scale):
    columns = mid.shape[1]
    lane = lax.broadcasted_iota(jnp.int32, mid.shape, 1)
    right = jnp.where(lane == columns - 1, 0.0, pltpu.roll(mid, columns - 1, 1))
    left = jnp.where(lane == 0, 0.0, pltpu.roll(mid, 1, 1))
    dz = following - prev
    dx = below - above
    dy = right - left
    slope = (1.5 * light_z) * dz + (1.5 * light_x) * dx + (1.5 * light_y) * dy
    shading = 0.55 + 0.45 * jnp.tanh(slope)
    gradient_sq4 = dz * dz + dx * dx + dy * dy
    square = mid * mid
    optical = scale * (square / (1.0 + square)) * (1.0 + gradient_sq4)
    centred = mid - 2.5
    red_share = 0.5 + 0.5 * jnp.tanh(centred)
    green_share = jnp.exp(-(centred * centred))
    return optical, shading, red_share, green_share


def render_layer(layer, k, base, carry, scale):
    red, green, blue, transmit = carry
    rows = pl.ds(base, 8)
    mid = layer(k, rows)
    before = layer(k, pl.ds(base - 8, 8))
    after = layer(k, pl.ds(base + 8, 8))
    sub = lax.broadcasted_iota(jnp.int32, mid.shape, 0)
    above = pltpu.roll(jnp.where(sub == 7, before, mid), 1, 0)
    below = pltpu.roll(jnp.where(sub == 0, after, mid), 7, 0)
    optical, shading, red_share, green_share = shade_voxels(
        layer(k - 1, rows), mid, above, below, layer(k + 1, rows), scale
    )
    remaining = transmit * jnp.exp(-optical)
    lit = (transmit - remaining) * shading
    red_part = lit * red_share
    return red + red_part, green + lit * green_share, blue + (lit - red_part), remaining


def empty_carry(columns):
    zero = jnp.zeros((8, columns), jnp.float32)
    return zero, zero, zero, jnp.ones_like(zero)


def read_tile(ref, tile):
    rows = pl.ds(pl.multiple_of(tile * 8, 8), 8)
    return tuple(ref[n, rows, :] for n in range(4))


def store_tile(ref, tile, values):
    rows = pl.ds(pl.multiple_of(tile * 8, 8), 8)
    for n, value in enumerate(values):
        ref[n, rows, :] = value


def pack_kernel(where, c, edge_a, side_b, edge_b, side_a, middle_a, middle_b, sems):
    rows = c.shape[1]
    copies = []

    def add(source, target):
        copies.append(pltpu.make_async_copy(source, target, sems.at[len(copies)]))

    blocks = ((edge_a, side_a, middle_a), (edge_b, side_b, middle_b))
    for n, (edge, side, middle) in enumerate(blocks):
        layers = pl.ds(where[n], REACH)
        add(c.at[layers, pl.ds(0, PAD)], edge.at[:, pl.ds(0, PAD)])
        add(c.at[layers, pl.ds(rows - PAD, PAD)], edge.at[:, pl.ds(PAD, PAD)])
        add(c.at[:, pl.ds(pl.multiple_of(where[2 + n], PAD), PAD)], side)
        add(c.at[layers, pl.ds(PAD, rows - 2 * PAD)], middle)
    for copy in copies:
        copy.start()
    for copy in copies:
        copy.wait()


def smooth_kernel(group, order, c_hbm, xa, xb, by, lx, plane, c, sems):
    groups = c.shape[0] // group
    rows_of = order[0]

    def fetch(g):
        part = pl.ds(g * group, group)
        return pltpu.make_async_copy(c_hbm.at[part], c.at[part], sems.at[g])

    for g in range(groups):
        fetch(g).start()

    def smooth_group(g, _):
        first = g * group
        fetch(g).wait()
        counts = [
            jnp.concatenate([xa[first + n], c[first + n], xb[first + n]], 0) for n in range(group)
        ]
        for n, value in enumerate(smooth_plane(counts, by, lx[rows_of])):
            plane[first + n] = value
        return 0

    lax.fori_loop(0, groups, smooth_group, 0)


def interior_kernel(scale, flags, plane, image, smoothed):
    layers, ext, columns = plane.shape

    def one_layer(j, _):
        def write(rows, value):
            smoothed[j, rows, :] = value

        smooth_depth_layer(flags, lambda k, rows: plane[k, rows, :], j + 4, ext // 8, write)
        return 0

    lax.fori_loop(0, layers - 8, one_layer, 0)

    def one_tile(tile, _):
        base = pl.multiple_of(tile * 8 + 8, 8)
        carry = empty_carry(columns)
        for k in range(1, layers - 9):
            carry = render_layer(lambda k, rows: smoothed[k, rows, :], k, base, carry, scale)
        store_tile(image, tile, carry)
        return 0

    lax.fori_loop(0, ext // 8 - 2, one_tile, 0)


def edge_smooth(turn, flags, order, plane, smoothed, edge, middle, ca, cb, by, lx, ends, halo):
    layers, ext, _ = plane.shape
    rows_of = order[0]
    is_front = order[1] == 1 - turn
    sign = jnp.where(is_front, 1, -1)
    counts = [
        jnp.concatenate([ca[j], edge[j, :PAD], middle[j], edge[j, PAD:], cb[j]], 0)
        for j in range(REACH)
    ]
    for j, value in enumerate(smooth_plane(counts, by, lx[rows_of])):
        halo[j] = value
    plane_face = jnp.where(is_front, 0, layers - 1)
    halo_face = jnp.where(is_front, REACH, -1)
    ends_face = jnp.where(is_front, 1, REACH)
    smoothed_face = jnp.where(is_front, -4, layers - 5)
    on_grid = jnp.where(is_front, flags[2], flags[3])

    def counted(v, rows):
        if v < 0:
            return halo[halo_face + sign * v, rows, :]
        return plane[plane_face + sign * v, rows, :]

    for v in range(-1, 4):

        def write(rows, value, v=v):
            ends[ends_face + sign * v, rows, :] = value * on_grid if v < 0 else value

        smooth_depth_layer(flags, counted, v, ext // 8, write)
    for v in (4, 5):
        ends[ends_face + sign * v] = smoothed[smoothed_face + sign * v]


def edge_render(scale, is_front, ends, behind, image, tiles, tile_of):
    columns = ends.shape[2]

    def one_tile(place, _):
        tile = tile_of(place)
        base = pl.multiple_of(tile * 8 + 8, 8)
        carry = empty_carry(columns)
        for k in range(1, REACH + 1):
            carry = render_layer(lambda k, rows: ends[k, rows, :], k, base, carry, scale)
        other = read_tile(behind, tile)
        front = [jnp.where(is_front, x, y) for x, y in zip(carry, other)]
        back = [jnp.where(is_front, y, x) for x, y in zip(carry, other)]
        colors = [front[n] + front[3] * back[n] for n in range(3)]
        store_tile(image, place, colors + [front[3] * back[3]])
        return 0

    lax.fori_loop(0, tiles, one_tile, 0)


def half_tiles(owner_tiles, wanted):
    def tile_of(place):
        return (place // owner_tiles * 2 + wanted) * owner_tiles + place % owner_tiles

    return tile_of


def first_edge_kernel(scale, flags, order, plane, smoothed, edge, middle, ca, cb, by, lx, behind,
                      image, ends, halo):
    edge_smooth(1, flags, order, plane, smoothed, edge, middle, ca, cb, by, lx, ends, halo)
    tiles = plane.shape[1] // 8 - 2
    edge_render(scale, order[1] == 0, ends, behind, image, tiles, lambda place: place)


def last_edge_kernel(scale, owner_tiles, flags, order, plane, smoothed, edge, middle, ca, cb, by,
                     lx, behind, image, ends, halo):
    edge_smooth(0, flags, order, plane, smoothed, edge, middle, ca, cb, by, lx, ends, halo)
    tiles = plane.shape[1] // 8 - 2
    tile_of = lambda place: place
    if owner_tiles:
        tiles, tile_of = tiles // 2, half_tiles(owner_tiles, 1 - order[1])
    edge_render(scale, order[1] == 1, ends, behind, image, tiles, tile_of)


def kept_edge_kernel(scale, owner_tiles, order, ends, behind, image):
    tiles = ends.shape[1] // 8 - 2
    tile_of = half_tiles(owner_tiles, order[1])
    edge_render(scale, order[1] == 1, ends, behind, image, tiles // 2, tile_of)


def whole(count):
    return [pl.BlockSpec(memory_space=pltpu.VMEM)] * count


def smem():
    return pl.BlockSpec(memory_space=pltpu.SMEM)


def in_hbm():
    return pl.BlockSpec(memory_space=pltpu.HBM)


def params(mib):
    return pltpu.CompilerParams(vmem_limit_bytes=mib * 1024 * 1024)


def cost(flops):
    return pl.CostEstimate(flops=flops, transcendentals=0, bytes_accessed=4_000_000)


def call_pack(where, c):
    layers, rows, columns = c.shape
    edge = pltpu.VMEM((REACH, 2 * PAD, columns), c.dtype)
    side = pltpu.VMEM((layers, PAD, columns), c.dtype)
    middle = pltpu.VMEM((REACH, rows - 2 * PAD, columns), c.dtype)
    return pl.pallas_call(
        pack_kernel,
        out_shape=(edge, side, edge, side, middle, middle),
        in_specs=[smem(), in_hbm()],
        out_specs=tuple(whole(6)),
        scratch_shapes=[pltpu.SemaphoreType.DMA((8,))],
        compiler_params=params(8),
        name="pack",
    )(where, c)


def call_smooth(order, c, xa, xb, by, lx):
    layers, rows, columns = c.shape
    ext = rows + 2 * PAD
    group = 8
    return pl.pallas_call(
        functools.partial(smooth_kernel, group),
        out_shape=jax.ShapeDtypeStruct((layers, ext, columns), jnp.float32),
        in_specs=[smem(), in_hbm()] + whole(4),
        out_specs=whole(1)[0],
        scratch_shapes=[
            pltpu.VMEM((layers, rows, columns), jnp.int32),
            pltpu.SemaphoreType.DMA((layers // group,)),
        ],
        compiler_params=params(24),
        cost_estimate=cost(1_000_000_000),
        name="smooth",
    )(order, c, xa, xb, by, lx)


def call_interior(scale, flags, plane):
    layers, ext, columns = plane.shape
    return pl.pallas_call(
        functools.partial(interior_kernel, scale),
        out_shape=(
            jax.ShapeDtypeStruct((4, ext - 2 * PAD, columns), jnp.float32),
            jax.ShapeDtypeStruct((layers - 8, ext, columns), jnp.float32),
        ),
        in_specs=[smem()] + whole(1),
        out_specs=tuple(whole(2)),
        compiler_params=params(24),
        cost_estimate=cost(1_000_000_000),
        name="interior",
    )(flags, plane)


def call_first_edge(scale, flags, order, plane, *operands):
    _, ext, columns = plane.shape
    f32 = jnp.float32
    return pl.pallas_call(
        functools.partial(first_edge_kernel, scale),
        out_shape=jax.ShapeDtypeStruct((4, ext - 2 * PAD, columns), f32),
        in_specs=[smem(), smem()] + whole(1 + len(operands)),
        out_specs=whole(1)[0],
        scratch_shapes=[
            pltpu.VMEM((REACH + 2, ext, columns), f32),
            pltpu.VMEM((REACH, ext, columns), f32),
        ],
        compiler_params=params(24),
        cost_estimate=cost(300_000_000),
        name="first_edge",
    )(flags, order, plane, *operands)


def call_last_edge(scale, owner_tiles, flags, order, plane, *operands):
    _, ext, columns = plane.shape
    f32 = jnp.float32
    rows = (ext - 2 * PAD) // (2 if owner_tiles else 1)
    return pl.pallas_call(
        functools.partial(last_edge_kernel, scale, owner_tiles),
        out_shape=(
            jax.ShapeDtypeStruct((4, rows, columns), f32),
            jax.ShapeDtypeStruct((REACH + 2, ext, columns), f32),
        ),
        in_specs=[smem(), smem()] + whole(1 + len(operands)),
        out_specs=tuple(whole(2)),
        scratch_shapes=[pltpu.VMEM((REACH, ext, columns), f32)],
        compiler_params=params(24),
        cost_estimate=cost(300_000_000),
        name="last_edge",
    )(flags, order, plane, *operands)


def call_kept_edge(scale, owner_tiles, order, ends, behind):
    _, ext, columns = ends.shape
    return pl.pallas_call(
        functools.partial(kept_edge_kernel, scale, owner_tiles),
        out_shape=jax.ShapeDtypeStruct((4, (ext - 2 * PAD) // 2, columns), jnp.float32),
        in_specs=[smem()] + whole(2),
        out_specs=whole(1)[0],
        compiler_params=params(24),
        cost_estimate=cost(200_000_000),
        name="kept_edge",
    )(order, ends, behind)


def swap(value, axis, first):
    count = lax.axis_size(axis)
    pairs = []
    for low in range(first, count - 1, 2):
        pairs += [(low, low + 1), (low + 1, low)]
    return lax.ppermute(value, axis, pairs)


def over(front, back):
    through = front[3:]
    return jnp.concatenate([front[:3] + through * back[:3], through * back[3:]], 0)


def halves_of(layers):
    count = lax.axis_size("depth")
    parity = lax.axis_index("depth") % 2
    _, rows, columns = layers.shape
    pieces = layers.reshape(4, count // 2, 2, rows // count, columns)
    send = lax.dynamic_index_in_dim(pieces, 1 - parity, 2, keepdims=False)
    keep = lax.dynamic_index_in_dim(pieces, parity, 2, keepdims=False)
    return send, keep


def exchange(send, keep):
    count = lax.axis_size("depth")
    me = lax.axis_index("depth")
    parity, pair = me % 2, me // 2
    pairs = count // 2
    send, keep = (value.reshape(4, pairs, -1, value.shape[-1]) for value in (send, keep))
    owned, columns = send.shape[2:]
    got = swap(send, "depth", 0)
    joined = jnp.where(parity == 0, over(keep, got), over(got, keep))
    parts = []
    for step in range(pairs):
        piece = lax.dynamic_index_in_dim(joined, pair ^ step, 1, keepdims=False)
        if step:
            piece = lax.ppermute(piece, "depth", [(i, i ^ (2 * step)) for i in range(count)])
        parts.append(piece)
    result = jnp.zeros((3, owned, columns), jnp.float32)
    through = jnp.ones((1, owned, columns), jnp.float32)
    for step in range(pairs):
        ahead = jnp.ones((1, owned, columns), jnp.float32)
        for other in range(pairs):
            if other != step:
                nearer = (pair ^ other) < (pair ^ step)
                ahead = ahead * jnp.where(nearer, parts[other][3:], 1.0)
        result = result + ahead * parts[step][:3]
        through = through * parts[step][3:]
    return jnp.concatenate([result, 1.0 - through], 0)


def local(counts):
    slab, rows, columns = counts.shape
    img, depth = lax.axis_index("img"), lax.axis_index("depth")
    imgs, depths = lax.axis_size("img"), lax.axis_size("depth")
    scale = 1.5 / (slab * depths)
    row_odd, depth_odd = img % 2, depth % 2
    first_a, first_b = (1 - depth_odd) * (slab - REACH), depth_odd * (slab - REACH)
    row_a, row_b = (1 - row_odd) * (rows - PAD), row_odd * (rows - PAD)
    where = jnp.stack([first_a, first_b, row_a, row_b])
    order = jnp.stack([1 - row_odd, depth_odd])
    one = jnp.float32(1.0)
    flags = jnp.stack(
        [(img > 0) * one, (img < imgs - 1) * one, (depth > 0) * one, (depth < depths - 1) * one]
    )
    by = jnp.asarray(column_matrix(columns))
    lx = jnp.asarray(row_matrices(rows))
    held = pltpu.with_memory_space_constraint(counts, pltpu.HBM)
    edge_a, side_b, edge_b, side_a, mid_a, mid_b = call_pack(where, held)
    edge_a = swap(edge_a, "depth", 0)
    edge_b = swap(edge_b, "depth", 1)
    xa = swap(side_a, "img", 0)
    xb = swap(side_b, "img", 1)
    mid_a = swap(mid_a, "depth", 0)
    mid_b = swap(mid_b, "depth", 1)
    halves = jnp.concatenate([edge_a, edge_b], 0).reshape(2 * REACH, 2, PAD, columns)
    corner_a = lax.dynamic_index_in_dim(halves, 1 - row_odd, 1, keepdims=False)
    corner_b = lax.dynamic_index_in_dim(halves, row_odd, 1, keepdims=False)
    ca = swap(corner_a, "img", 0)
    cb = swap(corner_b, "img", 1)
    plane = call_smooth(order, held, xa, xb, by, lx)
    inner, smoothed = call_interior(scale, flags, plane)
    owned = rows // depths
    owner_tiles = owned // 8 if owned % 8 == 0 else 0
    common = (flags, order, plane, smoothed)
    layers = call_first_edge(
        scale, *common, edge_b, mid_b, ca[REACH:], cb[REACH:], by, lx, inner
    )
    send, ends = call_last_edge(
        scale, owner_tiles, *common, edge_a, mid_a, ca[:REACH], cb[:REACH], by, lx, layers
    )
    if owner_tiles:
        keep = call_kept_edge(scale, owner_tiles, order, ends, layers)
    else:
        send, keep = halves_of(send)
    return exchange(send, keep)


def solution(mesh):
    in_specs = (P("depth", "img", None),)
    out_specs = P(None, ("img", "depth"), None)
    return jax.shard_map(local, mesh=mesh, in_specs=in_specs, out_specs=out_specs, check_vma=False)
```

```python
import functools
import math

import jax
import jax.numpy as jnp
import numpy as np
from jax import lax
from jax.experimental import pallas as pl
from jax.experimental.pallas import tpu as pltpu
from jax.sharding import PartitionSpec as P


gauss_taps = [
    math.exp(-offset * offset / 8.0)
    / sum((math.exp(-other * other / 8.0) for other in range(-4, 5)))
    for offset in range(-4, 5)
]
light_z = 0.48
light_x = 0.6
light_y = 0.64


REACH = 5
BLOCK = 256
PAD = 8


def band(size):
    index = np.arange(size)
    apart = np.abs(index[:, None] - index[None, :])
    taps = np.array(gauss_taps[4:] + [0.0], np.float64)
    return taps[np.minimum(apart, 5)]


def split_terms(matrix):
    high = matrix.astype(jnp.bfloat16)
    low = (matrix - high.astype(np.float64)).astype(jnp.bfloat16)
    return high, low


def column_matrices():
    full = band(2 * BLOCK)
    inside = full[:BLOCK, :BLOCK]
    half = BLOCK // 2
    across = full[half : 3 * half, half : 3 * half].copy()
    across[:half, :half] = 0.0
    across[half:, half:] = 0.0
    return np.concatenate([*split_terms(inside), *split_terms(across)], 0)


def row_matrices(rows):
    high, low = split_terms(band(rows + 2 * PAD))
    order = np.arange(rows + 2 * PAD)
    swapped = np.concatenate([order[rows + PAD :], order[PAD : rows + PAD], order[:PAD]])
    both = []
    for columns in (order, swapped):
        both.append(np.concatenate([high[:, columns], high[:, columns], low[:, columns]], 1))
    return np.stack(both)


def two_terms(value, high, low):
    return jnp.dot(value, high, preferred_element_type=jnp.float32) + jnp.dot(
        value, low, preferred_element_type=jnp.float32
    )


def smooth_columns(exact, by):
    rows, columns = exact.shape
    half = BLOCK // 2
    starts = range(0, columns, BLOCK)
    stacked = jnp.concatenate([exact[:, at : at + BLOCK] for at in starts], 0)
    inside = two_terms(stacked, by[:BLOCK], by[BLOCK : 2 * BLOCK])
    parts = []
    for n in range(len(starts)):
        block = inside[n * rows : (n + 1) * rows]
        parts += [block[:, :half], block[:, half:]]
    for n, at in enumerate(starts[1:]):
        window = exact[:, at - half : at + half]
        across = two_terms(window, by[2 * BLOCK : 3 * BLOCK], by[3 * BLOCK :])
        parts[2 * n + 1] = parts[2 * n + 1] + across[:, :half]
        parts[2 * n + 2] = parts[2 * n + 2] + across[:, half:]
    return jnp.concatenate(parts, 1)


def smooth_plane(counts, by, lx):
    rows = counts[0].shape[0]
    exact = jnp.concatenate([c.astype(jnp.float32).astype(jnp.bfloat16) for c in counts], 0)
    wide = smooth_columns(exact, by)
    high = wide.astype(jnp.bfloat16)
    low = (wide - high.astype(jnp.float32)).astype(jnp.bfloat16)
    planes = []
    for n in range(len(counts)):
        part = slice(n * rows, (n + 1) * rows)
        stacked = jnp.concatenate([high[part], low[part], high[part]], 0)
        planes.append(jnp.dot(lx, stacked, preferred_element_type=jnp.float32))
    return planes


def smooth_depth(read, k):
    total = gauss_taps[4] * read(k)
    for offset in range(1, 5):
        total = total + gauss_taps[4 + offset] * (read(k - offset) + read(k + offset))
    return total


def smooth_depth_layer(flags, read, k, tiles, write):
    for tile in range(tiles):
        rows = pl.ds(tile * 8, 8)
        value = smooth_depth(lambda j: read(j, rows), k)
        if tile == 0:
            value = value * flags[0]
        if tile == tiles - 1:
            value = value * flags[1]
        write(rows, value)


def beside(mid, step):
    lanes = 128
    lane = lax.broadcasted_iota(jnp.int32, (mid.shape[0], lanes), 1)
    parts = [mid[:, at : at + lanes] for at in range(0, mid.shape[1], lanes)]
    turned = [pltpu.roll(part, lanes - 1 if step == 1 else 1, 1) for part in parts]
    zero = jnp.zeros_like(parts[0])
    if step == 1:
        return jnp.concatenate(
            [jnp.where(lane == lanes - 1, y, x) for x, y in zip(turned, turned[1:] + [zero])], 1
        )
    return jnp.concatenate(
        [jnp.where(lane == 0, y, x) for x, y in zip(turned, [zero] + turned[:-1])], 1
    )


def render_layer(layer, k, base, carry, scale):
    total, tilted, green, transmit = carry
    rows = pl.ds(base, 8)
    mid = layer(k, rows)
    before = layer(k, pl.ds(base - 8, 8))
    after = layer(k, pl.ds(base + 8, 8))
    sub = lax.broadcasted_iota(jnp.int32, mid.shape, 0)
    above = pltpu.roll(jnp.where(sub == 7, before, mid), 1, 0)
    below = pltpu.roll(jnp.where(sub == 0, after, mid), 7, 0)
    dz = layer(k + 1, rows) - layer(k - 1, rows)
    dx = below - above
    dy = beside(mid, 1) - beside(mid, -1)
    slope = (1.5 * light_z) * dz + (1.5 * light_x) * dx + (1.5 * light_y) * dy
    shading = jnp.tanh(slope) + (0.55 / 0.45)
    gradient_sq4 = dz * dz + dx * dx + dy * dy
    square = mid * mid
    optical = (square / (1.0 + square)) * (1.0 + gradient_sq4)
    centred = mid - 2.5
    log2e = math.log2(math.e)
    remaining = transmit * jnp.exp2(optical * (-scale * log2e))
    lit = (transmit - remaining) * shading
    return (
        total + lit,
        tilted + lit * jnp.tanh(centred),
        green + lit * jnp.exp2((centred * -log2e) * centred),
        remaining,
    )


def empty_carry(columns):
    zero = jnp.zeros((8, columns), jnp.float32)
    return zero, zero, zero, jnp.ones_like(zero)


def read_tile(ref, tile):
    rows = pl.ds(pl.multiple_of(tile * 8, 8), 8)
    return tuple(ref[n, rows, :] for n in range(4))


def store_tile(ref, tile, values):
    rows = pl.ds(pl.multiple_of(tile * 8, 8), 8)
    for n, value in enumerate(values):
        ref[n, rows, :] = value


def run_copies(copies):
    for copy in copies:
        copy.start()
    for copy in copies:
        copy.wait()


def run_copies(pairs, sems):
    copies = [pltpu.make_async_copy(*pair, sems.at[n]) for n, pair in enumerate(pairs)]
    for copy in copies:
        copy.start()
    for copy in copies:
        copy.wait()


def pack_block_kernel(where, c, block, sems):
    half = block.shape[1] // 2
    layers = pl.ds(where[1], REACH)
    parts = [pl.ds(n * half, half) for n in range(2)]
    run_copies([(c.at[layers, part], block.at[:, part]) for part in parts], sems)


def pack_rest_kernel(where, c, side_b, edge, middle, side_a, sems):
    rows = c.shape[1]
    layers = pl.ds(where[0], REACH)
    pairs = [
        (c.at[:, pl.ds(pl.multiple_of(where[2 + n], PAD), PAD)], side)
        for n, side in enumerate((side_a, side_b))
    ]
    pairs.append((c.at[layers, pl.ds(0, PAD)], edge.at[:, pl.ds(0, PAD)]))
    pairs.append((c.at[layers, pl.ds(rows - PAD, PAD)], edge.at[:, pl.ds(PAD, PAD)]))
    pairs.append((c.at[layers, pl.ds(PAD, rows - 2 * PAD)], middle))
    run_copies(pairs, sems)


def smooth_kernel(group, order, c_hbm, xa, xb, by, lx, plane, c, sems):
    groups = c.shape[0] // group
    rows_of = order[0]

    def fetch(g):
        part = pl.ds(g * group, group)
        return pltpu.make_async_copy(c_hbm.at[part], c.at[part], sems.at[g])

    for g in range(groups):
        fetch(g).start()

    def smooth_group(g, _):
        first = g * group
        fetch(g).wait()
        counts = [
            jnp.concatenate([xa[first + n], c[first + n], xb[first + n]], 0) for n in range(group)
        ]
        for n, value in enumerate(smooth_plane(counts, by, lx[rows_of])):
            plane[first + n] = value
        return 0

    lax.fori_loop(0, groups, smooth_group, 0)


def interior_kernel(scale, flags, plane, image, smoothed):
    layers, ext, columns = plane.shape

    def one_layer(j, _):
        def write(rows, value):
            smoothed[j, rows, :] = value

        smooth_depth_layer(flags, lambda k, rows: plane[k, rows, :], j + 4, ext // 8, write)
        return 0

    lax.fori_loop(0, layers - 8, one_layer, 0)

    def one_tile(tile, _):
        base = pl.multiple_of(tile * 8 + 8, 8)
        carry = empty_carry(columns)
        for k in range(1, layers - 9):
            carry = render_layer(lambda k, rows: smoothed[k, rows, :], k, base, carry, scale)
        store_tile(image, tile, carry)
        return 0

    lax.fori_loop(0, ext // 8 - 2, one_tile, 0)


def edge_smooth(turn, flags, order, plane, smoothed, tile, ca, cb, by, lx, ends, halo):
    layers, ext, _ = plane.shape
    rows_of = order[0]
    is_front = order[1] == 1 - turn
    sign = jnp.where(is_front, 1, -1)
    counts = [jnp.concatenate([ca[j], tile(j), cb[j]], 0) for j in range(REACH)]
    for j, value in enumerate(smooth_plane(counts, by, lx[rows_of])):
        halo[j] = value
    plane_face = jnp.where(is_front, 0, layers - 1)
    halo_face = jnp.where(is_front, REACH, -1)
    ends_face = jnp.where(is_front, 1, REACH)
    smoothed_face = jnp.where(is_front, -4, layers - 5)
    on_grid = jnp.where(is_front, flags[2], flags[3])

    def counted(v, rows):
        if v < 0:
            return halo[halo_face + sign * v, rows, :]
        return plane[plane_face + sign * v, rows, :]

    for v in range(-1, 4):

        def write(rows, value, v=v):
            ends[ends_face + sign * v, rows, :] = value * on_grid if v < 0 else value

        smooth_depth_layer(flags, counted, v, ext // 8, write)
    for v in (4, 5):
        ends[ends_face + sign * v] = smoothed[smoothed_face + sign * v]


def edge_render(scale, is_front, ends, behind, image, tiles, tile_of):
    columns = ends.shape[2]

    def one_tile(place, _):
        tile = tile_of(place)
        base = pl.multiple_of(tile * 8 + 8, 8)
        carry = empty_carry(columns)
        for k in range(1, REACH + 1):
            carry = render_layer(lambda k, rows: ends[k, rows, :], k, base, carry, scale)
        other = read_tile(behind, tile)
        front = [jnp.where(is_front, x, y) for x, y in zip(carry, other)]
        back = [jnp.where(is_front, y, x) for x, y in zip(carry, other)]
        colors = [front[n] + front[3] * back[n] for n in range(3)]
        store_tile(image, place, colors + [front[3] * back[3]])
        return 0

    lax.fori_loop(0, tiles, one_tile, 0)


def half_tiles(owner_tiles, wanted):
    def tile_of(place):
        return (place // owner_tiles * 2 + wanted) * owner_tiles + place % owner_tiles

    return tile_of


def first_edge_kernel(scale, flags, order, plane, smoothed, block, ca, cb, by, lx, behind, image,
                      ends, halo):
    tile = lambda j: block[j]
    edge_smooth(1, flags, order, plane, smoothed, tile, ca, cb, by, lx, ends, halo)
    tiles = plane.shape[1] // 8 - 2
    edge_render(scale, order[1] == 0, ends, behind, image, tiles, lambda place: place)


def last_edge_kernel(scale, owner_tiles, flags, order, plane, smoothed, middle_any, edge, ca, cb,
                     by, lx, behind, image, ends, halo, middle, sem):
    run_copies([(middle_any, middle)], sem)
    tile = lambda j: jnp.concatenate([edge[j, :PAD], middle[j], edge[j, PAD:]], 0)
    edge_smooth(0, flags, order, plane, smoothed, tile, ca, cb, by, lx, ends, halo)
    tiles = plane.shape[1] // 8 - 2
    tile_of = lambda place: place
    if owner_tiles:
        tiles, tile_of = tiles // 2, half_tiles(owner_tiles, 1 - order[1])
    edge_render(scale, order[1] == 1, ends, behind, image, tiles, tile_of)


def kept_edge_kernel(scale, owner_tiles, order, ends, behind, image):
    tiles = ends.shape[1] // 8 - 2
    tile_of = half_tiles(owner_tiles, order[1])
    edge_render(scale, order[1] == 1, ends, behind, image, tiles // 2, tile_of)


def whole(count):
    return [pl.BlockSpec(memory_space=pltpu.VMEM)] * count


def smem():
    return pl.BlockSpec(memory_space=pltpu.SMEM)


def in_hbm():
    return pl.BlockSpec(memory_space=pltpu.HBM)


def params(mib):
    return pltpu.CompilerParams(vmem_limit_bytes=mib * 1024 * 1024)


def cost(flops):
    return pl.CostEstimate(flops=flops, transcendentals=0, bytes_accessed=4_000_000)


def call_pack_block(where, c):
    _, rows, columns = c.shape
    return pl.pallas_call(
        pack_block_kernel,
        out_shape=jax.ShapeDtypeStruct((REACH, rows, columns), c.dtype),
        in_specs=[smem(), in_hbm()],
        out_specs=whole(1)[0],
        scratch_shapes=[pltpu.SemaphoreType.DMA((2,))],
        compiler_params=params(8),
        name="pack_block",
    )(where, c)


def call_pack_rest(where, c):
    layers, rows, columns = c.shape
    edge = jax.ShapeDtypeStruct((REACH, 2 * PAD, columns), c.dtype)
    side = jax.ShapeDtypeStruct((layers, PAD, columns), c.dtype)
    middle = jax.ShapeDtypeStruct((REACH, rows - 2 * PAD, columns), c.dtype)
    return pl.pallas_call(
        pack_rest_kernel,
        out_shape=(side, edge, middle, side),
        in_specs=[smem(), in_hbm()],
        out_specs=tuple(whole(4)),
        scratch_shapes=[pltpu.SemaphoreType.DMA((5,))],
        compiler_params=params(8),
        name="pack_rest",
    )(where, c)


def call_smooth(order, c, xa, xb, by, lx):
    layers, rows, columns = c.shape
    ext = rows + 2 * PAD
    group = 8
    return pl.pallas_call(
        functools.partial(smooth_kernel, group),
        out_shape=jax.ShapeDtypeStruct((layers, ext, columns), jnp.float32),
        in_specs=[smem(), in_hbm()] + whole(4),
        out_specs=whole(1)[0],
        scratch_shapes=[
            pltpu.VMEM((layers, rows, columns), jnp.int32),
            pltpu.SemaphoreType.DMA((layers // group,)),
        ],
        compiler_params=params(24),
        cost_estimate=cost(1_000_000_000),
        name="smooth",
    )(order, c, xa, xb, by, lx)


def call_interior(scale, flags, plane):
    layers, ext, columns = plane.shape
    return pl.pallas_call(
        functools.partial(interior_kernel, scale),
        out_shape=(
            jax.ShapeDtypeStruct((4, ext - 2 * PAD, columns), jnp.float32),
            jax.ShapeDtypeStruct((layers - 8, ext, columns), jnp.float32),
        ),
        in_specs=[smem()] + whole(1),
        out_specs=tuple(whole(2)),
        compiler_params=params(24),
        cost_estimate=cost(1_000_000_000),
        name="interior",
    )(flags, plane)


def call_first_edge(scale, flags, order, plane, *operands):
    _, ext, columns = plane.shape
    f32 = jnp.float32
    return pl.pallas_call(
        functools.partial(first_edge_kernel, scale),
        out_shape=jax.ShapeDtypeStruct((4, ext - 2 * PAD, columns), f32),
        in_specs=[smem(), smem()] + whole(1 + len(operands)),
        out_specs=whole(1)[0],
        scratch_shapes=[
            pltpu.VMEM((REACH + 2, ext, columns), f32),
            pltpu.VMEM((REACH, ext, columns), f32),
        ],
        compiler_params=params(24),
        cost_estimate=cost(300_000_000),
        name="first_edge",
    )(flags, order, plane, *operands)


def call_last_edge(scale, owner_tiles, flags, order, plane, *operands):
    _, ext, columns = plane.shape
    f32 = jnp.float32
    rows = (ext - 2 * PAD) // (2 if owner_tiles else 1)
    return pl.pallas_call(
        functools.partial(last_edge_kernel, scale, owner_tiles),
        out_shape=(
            jax.ShapeDtypeStruct((4, rows, columns), f32),
            jax.ShapeDtypeStruct((REACH + 2, ext, columns), f32),
        ),
        in_specs=[smem(), smem()]
        + whole(2)
        + [in_hbm()]
        + whole(len(operands) - 2),
        out_specs=tuple(whole(2)),
        scratch_shapes=[
            pltpu.VMEM((REACH, ext, columns), f32),
            pltpu.VMEM(operands[1].shape, operands[1].dtype),
            pltpu.SemaphoreType.DMA((1,)),
        ],
        compiler_params=params(24),
        cost_estimate=cost(300_000_000),
        name="last_edge",
    )(flags, order, plane, *operands)


def call_kept_edge(scale, owner_tiles, order, ends, behind):
    _, ext, columns = ends.shape
    return pl.pallas_call(
        functools.partial(kept_edge_kernel, scale, owner_tiles),
        out_shape=jax.ShapeDtypeStruct((4, (ext - 2 * PAD) // 2, columns), jnp.float32),
        in_specs=[smem()] + whole(2),
        out_specs=whole(1)[0],
        compiler_params=params(24),
        cost_estimate=cost(200_000_000),
        name="kept_edge",
    )(order, ends, behind)


def swap(value, axis, first):
    count = lax.axis_size(axis)
    pairs = []
    for low in range(first, count - 1, 2):
        pairs += [(low, low + 1), (low + 1, low)]
    return lax.ppermute(value, axis, pairs)


def over(front, back):
    through = front[3:]
    return jnp.concatenate([front[:3] + through * back[:3], through * back[3:]], 0)


def halves_of(layers):
    count = lax.axis_size("depth")
    parity = lax.axis_index("depth") % 2
    _, rows, columns = layers.shape
    pieces = layers.reshape(4, count // 2, 2, rows // count, columns)
    send = lax.dynamic_index_in_dim(pieces, 1 - parity, 2, keepdims=False)
    keep = lax.dynamic_index_in_dim(pieces, parity, 2, keepdims=False)
    return send, keep


def exchange(send, keep):
    count = lax.axis_size("depth")
    me = lax.axis_index("depth")
    parity, pair = me % 2, me // 2
    pairs = count // 2
    send, keep = (value.reshape(4, pairs, -1, value.shape[-1]) for value in (send, keep))
    owned, columns = send.shape[2:]
    got = swap(send, "depth", 0)
    joined = jnp.where(parity == 0, over(keep, got), over(got, keep))
    parts = []
    for step in range(pairs):
        piece = lax.dynamic_index_in_dim(joined, pair ^ step, 1, keepdims=False)
        if step:
            piece = lax.ppermute(piece, "depth", [(i, i ^ (2 * step)) for i in range(count)])
        parts.append(piece)
    result = jnp.zeros((3, owned, columns), jnp.float32)
    through = jnp.ones((1, owned, columns), jnp.float32)
    for step in range(pairs):
        ahead = jnp.ones((1, owned, columns), jnp.float32)
        for other in range(pairs):
            if other != step:
                nearer = (pair ^ other) < (pair ^ step)
                ahead = ahead * jnp.where(nearer, parts[other][3:], 1.0)
        result = result + ahead * parts[step][:3]
        through = through * parts[step][3:]
    total, tilted, green = 0.225 * result[:1], 0.225 * result[1:2], 0.45 * result[2:]
    return jnp.concatenate([total + tilted, green, total - tilted, 1.0 - through], 0)


def local(counts):
    slab, rows, _ = counts.shape
    img, depth = lax.axis_index("img"), lax.axis_index("depth")
    imgs, depths = lax.axis_size("img"), lax.axis_size("depth")
    scale = 1.5 / (slab * depths)
    row_odd, depth_odd = img % 2, depth % 2
    first_a, first_b = (1 - depth_odd) * (slab - REACH), depth_odd * (slab - REACH)
    row_a, row_b = (1 - row_odd) * (rows - PAD), row_odd * (rows - PAD)
    where = jnp.stack([first_a, first_b, row_a, row_b])
    order = jnp.stack([1 - row_odd, depth_odd])
    one = jnp.float32(1.0)
    flags = jnp.stack(
        [(img > 0) * one, (img < imgs - 1) * one, (depth > 0) * one, (depth < depths - 1) * one]
    )
    by = jnp.asarray(column_matrices())
    lx = jnp.asarray(row_matrices(rows))
    held = pltpu.with_memory_space_constraint(counts, pltpu.HBM)
    block_b = call_pack_block(where, held)
    side_b, edge_a, mid_a, side_a = call_pack_rest(where, held)
    block_b = swap(block_b, "depth", 1)
    xb = swap(side_b, "img", 1)
    edge_a = swap(edge_a, "depth", 0)
    mid_a = swap(mid_a, "depth", 0)
    xa = swap(side_a, "img", 0)

    def corner(far):
        of_a = lax.dynamic_slice_in_dim(edge_a, far * PAD, PAD, 1)
        of_b = lax.dynamic_slice_in_dim(block_b, far * (rows - PAD), PAD, 1)
        return jnp.concatenate([of_a, of_b], 0)

    ca = swap(corner(1 - row_odd), "img", 0)
    cb = swap(corner(row_odd), "img", 1)
    plane = call_smooth(order, held, xa, xb, by, lx)
    inner, smoothed = call_interior(scale, flags, plane)
    owned = rows // depths
    owner_tiles = owned // 8 if owned % 8 == 0 else 0
    common = (flags, order, plane, smoothed)
    layers = call_first_edge(
        scale, *common, block_b, ca[REACH:], cb[REACH:], by, lx, inner
    )
    send, ends = call_last_edge(
        scale, owner_tiles, *common, pltpu.with_memory_space_constraint(mid_a, pltpu.HBM), edge_a,
        ca[:REACH], cb[:REACH], by, lx, layers
    )
    if owner_tiles:
        keep = call_kept_edge(scale, owner_tiles, order, ends, layers)
    else:
        send, keep = halves_of(send)
    return exchange(send, keep)


def solution(mesh):
    in_specs = (P("depth", "img", None),)
    out_specs = P(None, ("img", "depth"), None)
    return jax.shard_map(local, mesh=mesh, in_specs=in_specs, out_specs=out_specs, check_vma=False)
```

```python
import functools
import math

import jax
import jax.numpy as jnp
import numpy as np
from jax import lax
from jax.experimental import pallas as pl
from jax.experimental.pallas import tpu as pltpu
from jax.sharding import PartitionSpec as P


gauss_taps = [
    math.exp(-offset * offset / 8.0)
    / sum((math.exp(-other * other / 8.0) for other in range(-4, 5)))
    for offset in range(-4, 5)
]
light_z = 0.48
light_x = 0.6
light_y = 0.64


REACH = 5
SIDE_GROUP = 4
PAD = 8


def band(size):
    index = np.arange(size)
    apart = np.abs(index[:, None] - index[None, :])
    taps = np.array(gauss_taps[4:] + [0.0], np.float64)
    return taps[np.minimum(apart, 5)]


def split_terms(matrix):
    high = matrix.astype(jnp.bfloat16)
    low = (matrix - high.astype(np.float64)).astype(jnp.bfloat16)
    return high, low


def column_matrices(columns):
    return np.concatenate(split_terms(band(columns)), 0)


def row_terms(matrix):
    high, low = split_terms(matrix)
    return np.concatenate([high, high, low], 1)


def row_orders(rows):
    full = band(rows + 2 * PAD)
    order = np.arange(rows + 2 * PAD)
    swapped = np.concatenate([order[rows + PAD :], order[PAD : rows + PAD], order[:PAD]])
    return [full[:, order], full[:, swapped]]


def row_matrices(rows):
    return np.stack([row_terms(matrix) for matrix in row_orders(rows)])


def own_matrix(rows):
    return row_terms(band(rows + 2 * PAD)[:, PAD : rows + PAD])


def side_matrices(rows):
    both = []
    for matrix in row_orders(rows):
        sides = np.concatenate([matrix[:, :PAD], matrix[:, rows + PAD :]], 1)
        touched = np.concatenate([sides[: 2 * PAD], sides[rows:]], 0)
        both.append(row_terms(np.kron(np.eye(SIDE_GROUP), touched)))
    return np.stack(both)


def two_terms(value, high, low):
    return jnp.dot(value, high, preferred_element_type=jnp.float32) + jnp.dot(
        value, low, preferred_element_type=jnp.float32
    )


def smooth_columns(exact, by):
    half = by.shape[0] // 2
    return two_terms(exact, by[:half], by[half:])


def column_terms(counts, by):
    exact = jnp.concatenate([c.astype(jnp.float32).astype(jnp.bfloat16) for c in counts], 0)
    wide = smooth_columns(exact, by)
    high = wide.astype(jnp.bfloat16)
    return high, (wide - high.astype(jnp.float32)).astype(jnp.bfloat16)


def row_product(matrix, high, low):
    stacked = jnp.concatenate([high, low, high], 0)
    return jnp.dot(matrix, stacked, preferred_element_type=jnp.float32)


def smooth_plane(counts, by, lx):
    rows = counts[0].shape[0]
    high, low = column_terms(counts, by)
    parts = [slice(n * rows, (n + 1) * rows) for n in range(len(counts))]
    return [row_product(lx, high[part], low[part]) for part in parts]


def smooth_depth(read, k):
    total = gauss_taps[4] * read(k)
    for offset in range(1, 5):
        total = total + gauss_taps[4 + offset] * (read(k - offset) + read(k + offset))
    return total


def smooth_depth_layer(flags, read, k, tiles, write):
    for tile in range(tiles):
        rows = pl.ds(tile * 8, 8)
        value = smooth_depth(lambda j: read(j, rows), k)
        if tile == 0:
            value = value * flags[0]
        if tile == tiles - 1:
            value = value * flags[1]
        write(rows, value)


def beside(mid, step):
    lanes = 128
    lane = lax.broadcasted_iota(jnp.int32, (mid.shape[0], lanes), 1)
    parts = [mid[:, at : at + lanes] for at in range(0, mid.shape[1], lanes)]
    turned = [pltpu.roll(part, lanes - 1 if step == 1 else 1, 1) for part in parts]
    zero = jnp.zeros_like(parts[0])
    if step == 1:
        return jnp.concatenate(
            [jnp.where(lane == lanes - 1, y, x) for x, y in zip(turned, turned[1:] + [zero])], 1
        )
    return jnp.concatenate(
        [jnp.where(lane == 0, y, x) for x, y in zip(turned, [zero] + turned[:-1])], 1
    )


def render_layer(layer, k, base, carry, scale):
    total, tilted, green, transmit = carry
    rows = pl.ds(base, 8)
    mid = layer(k, rows)
    before = layer(k, pl.ds(base - 8, 8))
    after = layer(k, pl.ds(base + 8, 8))
    sub = lax.broadcasted_iota(jnp.int32, mid.shape, 0)
    above = pltpu.roll(jnp.where(sub == 7, before, mid), 1, 0)
    below = pltpu.roll(jnp.where(sub == 0, after, mid), 7, 0)
    dz = layer(k + 1, rows) - layer(k - 1, rows)
    dx = below - above
    dy = beside(mid, 1) - beside(mid, -1)
    slope = (1.5 * light_z) * dz + (1.5 * light_x) * dx + (1.5 * light_y) * dy
    shading = jnp.tanh(slope) + (0.55 / 0.45)
    gradient_sq4 = dz * dz + dx * dx + dy * dy
    square = mid * mid
    optical = (square / (1.0 + square)) * (1.0 + gradient_sq4)
    centred = mid - 2.5
    log2e = math.log2(math.e)
    remaining = transmit * jnp.exp2(optical * (-scale * log2e))
    lit = (transmit - remaining) * shading
    return (
        total + lit,
        tilted + lit * jnp.tanh(centred),
        green + lit * jnp.exp2((centred * -log2e) * centred),
        remaining,
    )


def empty_carry(columns):
    zero = jnp.zeros((8, columns), jnp.float32)
    return zero, zero, zero, jnp.ones_like(zero)


def read_tile(ref, tile):
    rows = pl.ds(pl.multiple_of(tile * 8, 8), 8)
    return tuple(ref[n, rows, :] for n in range(4))


def store_tile(ref, tile, values):
    rows = pl.ds(pl.multiple_of(tile * 8, 8), 8)
    for n, value in enumerate(values):
        ref[n, rows, :] = value


def run_copies(copies):
    for copy in copies:
        copy.start()
    for copy in copies:
        copy.wait()


def run_copies(pairs, sems):
    copies = [pltpu.make_async_copy(*pair, sems.at[n]) for n, pair in enumerate(pairs)]
    for copy in copies:
        copy.start()
    for copy in copies:
        copy.wait()


def pack_block_kernel(where, c, block, sems):
    half = block.shape[1] // 2
    layers = pl.ds(where[1], REACH)
    parts = [pl.ds(n * half, half) for n in range(2)]
    run_copies([(c.at[layers, part], block.at[:, part]) for part in parts], sems)


def pack_rest_kernel(where, c, side_b, edge, middle, side_a, sems):
    rows = c.shape[1]
    layers = pl.ds(where[0], REACH)
    pairs = [
        (c.at[:, pl.ds(pl.multiple_of(where[2 + n], PAD), PAD)], side)
        for n, side in enumerate((side_a, side_b))
    ]
    pairs.append((c.at[layers, pl.ds(0, PAD)], edge.at[:, pl.ds(0, PAD)]))
    pairs.append((c.at[layers, pl.ds(rows - PAD, PAD)], edge.at[:, pl.ds(PAD, PAD)]))
    pairs.append((c.at[layers, pl.ds(PAD, rows - 2 * PAD)], middle))
    run_copies(pairs, sems)


def smooth_kernel(group, c_hbm, by, lx, plane, c, sems):
    groups = c.shape[0] // group

    def fetch(g):
        part = pl.ds(g * group, group)
        return pltpu.make_async_copy(c_hbm.at[part], c.at[part], sems.at[g])

    for g in range(groups):
        fetch(g).start()

    def smooth_group(g, _):
        first = g * group
        fetch(g).wait()
        counts = [c[first + n] for n in range(group)]
        for n, value in enumerate(smooth_plane(counts, by, lx[...])):
            plane[first + n] = value
        return 0

    lax.fori_loop(0, groups, smooth_group, 0)


def depth_kernel(flags, order, partial, xa, xb, by, lx, plane, smoothed):
    layers, ext, _ = plane.shape
    group = 2 * SIDE_GROUP
    edge = 2 * PAD
    sides = lx[order[0]]

    def add_sides(g, _):
        first = g * group
        counts = [jnp.concatenate([xa[first + n], xb[first + n]], 0) for n in range(group)]
        high, low = column_terms(counts, by)
        for half in range(2):
            part = slice(half * SIDE_GROUP * edge, (half + 1) * SIDE_GROUP * edge)
            added = row_product(sides, high[part], low[part])
            for n in range(SIDE_GROUP):
                k = first + half * SIDE_GROUP + n
                at = n * 2 * edge
                plane[k, :edge, :] = partial[k, :edge, :] + added[at : at + edge]
                plane[k, ext - edge :, :] = (
                    partial[k, ext - edge :, :] + added[at + edge : at + 2 * edge]
                )
        return 0

    lax.fori_loop(0, layers // group, add_sides, 0)

    def one_layer(j, _):
        def write(rows, value):
            smoothed[j, rows, :] = value

        smooth_depth_layer(flags, lambda k, rows: plane[k, rows, :], j + 4, ext // 8, write)
        return 0

    lax.fori_loop(0, layers - 8, one_layer, 0)


def interior_kernel(scale, smoothed, image):
    held, ext, columns = smoothed.shape

    def one_tile(tile, _):
        base = pl.multiple_of(tile * 8 + 8, 8)
        carry = empty_carry(columns)
        for k in range(1, held - 1):
            carry = render_layer(lambda k, rows: smoothed[k, rows, :], k, base, carry, scale)
        store_tile(image, tile, carry)
        return 0

    lax.fori_loop(0, ext // 8 - 2, one_tile, 0)


def edge_smooth(turn, flags, order, plane, smoothed, tile, ca, cb, by, lx, ends, halo):
    layers, ext, _ = plane.shape
    rows_of = order[0]
    is_front = order[1] == 1 - turn
    sign = jnp.where(is_front, 1, -1)
    counts = [jnp.concatenate([ca[j], tile(j), cb[j]], 0) for j in range(REACH)]
    for j, value in enumerate(smooth_plane(counts, by, lx[rows_of])):
        halo[j] = value
    plane_face = jnp.where(is_front, 0, layers - 1)
    halo_face = jnp.where(is_front, REACH, -1)
    ends_face = jnp.where(is_front, 1, REACH)
    smoothed_face = jnp.where(is_front, -4, layers - 5)
    on_grid = jnp.where(is_front, flags[2], flags[3])

    def counted(v, rows):
        if v < 0:
            return halo[halo_face + sign * v, rows, :]
        return plane[plane_face + sign * v, rows, :]

    for v in range(-1, 4):

        def write(rows, value, v=v):
            ends[ends_face + sign * v, rows, :] = value * on_grid if v < 0 else value

        smooth_depth_layer(flags, counted, v, ext // 8, write)
    for v in (4, 5):
        ends[ends_face + sign * v] = smoothed[smoothed_face + sign * v]


def edge_render(scale, is_front, ends, behind, image, tiles, tile_of):
    columns = ends.shape[2]

    def one_tile(place, _):
        tile = tile_of(place)
        base = pl.multiple_of(tile * 8 + 8, 8)
        carry = empty_carry(columns)
        for k in range(1, REACH + 1):
            carry = render_layer(lambda k, rows: ends[k, rows, :], k, base, carry, scale)
        other = read_tile(behind, tile)
        front = [jnp.where(is_front, x, y) for x, y in zip(carry, other)]
        back = [jnp.where(is_front, y, x) for x, y in zip(carry, other)]
        colors = [front[n] + front[3] * back[n] for n in range(3)]
        store_tile(image, place, colors + [front[3] * back[3]])
        return 0

    lax.fori_loop(0, tiles, one_tile, 0)


def half_tiles(owner_tiles, wanted):
    def tile_of(place):
        return (place // owner_tiles * 2 + wanted) * owner_tiles + place % owner_tiles

    return tile_of


def first_edge_kernel(scale, flags, order, plane, smoothed, block, ca, cb, by, lx, behind, image,
                      ends, halo):
    tile = lambda j: block[j]
    edge_smooth(1, flags, order, plane, smoothed, tile, ca, cb, by, lx, ends, halo)
    tiles = plane.shape[1] // 8 - 2
    edge_render(scale, order[1] == 0, ends, behind, image, tiles, lambda place: place)


def last_edge_kernel(scale, owner_tiles, flags, order, plane, smoothed, middle_any, edge, ca, cb,
                     by, lx, behind, image, ends, halo, middle, sem):
    run_copies([(middle_any, middle)], sem)
    tile = lambda j: jnp.concatenate([edge[j, :PAD], middle[j], edge[j, PAD:]], 0)
    edge_smooth(0, flags, order, plane, smoothed, tile, ca, cb, by, lx, ends, halo)
    tiles = plane.shape[1] // 8 - 2
    tile_of = lambda place: place
    if owner_tiles:
        tiles, tile_of = tiles // 2, half_tiles(owner_tiles, 1 - order[1])
    edge_render(scale, order[1] == 1, ends, behind, image, tiles, tile_of)


def kept_edge_kernel(scale, owner_tiles, order, ends, behind, image):
    tiles = ends.shape[1] // 8 - 2
    tile_of = half_tiles(owner_tiles, order[1])
    edge_render(scale, order[1] == 1, ends, behind, image, tiles // 2, tile_of)


def whole(count):
    return [pl.BlockSpec(memory_space=pltpu.VMEM)] * count


def smem():
    return pl.BlockSpec(memory_space=pltpu.SMEM)


def in_hbm():
    return pl.BlockSpec(memory_space=pltpu.HBM)


def params(mib):
    return pltpu.CompilerParams(vmem_limit_bytes=mib * 1024 * 1024)


def cost(flops):
    return pl.CostEstimate(flops=flops, transcendentals=0, bytes_accessed=4_000_000)


def call_pack_block(where, c):
    _, rows, columns = c.shape
    return pl.pallas_call(
        pack_block_kernel,
        out_shape=jax.ShapeDtypeStruct((REACH, rows, columns), c.dtype),
        in_specs=[smem(), in_hbm()],
        out_specs=whole(1)[0],
        scratch_shapes=[pltpu.SemaphoreType.DMA((2,))],
        compiler_params=params(8),
        name="pack_block",
    )(where, c)


def call_pack_rest(where, c):
    layers, rows, columns = c.shape
    edge = jax.ShapeDtypeStruct((REACH, 2 * PAD, columns), c.dtype)
    side = jax.ShapeDtypeStruct((layers, PAD, columns), c.dtype)
    middle = jax.ShapeDtypeStruct((REACH, rows - 2 * PAD, columns), c.dtype)
    return pl.pallas_call(
        pack_rest_kernel,
        out_shape=(side, edge, middle, side),
        in_specs=[smem(), in_hbm()],
        out_specs=tuple(whole(4)),
        scratch_shapes=[pltpu.SemaphoreType.DMA((5,))],
        compiler_params=params(8),
        name="pack_rest",
    )(where, c)


def call_smooth(c, by, lx):
    layers, rows, columns = c.shape
    ext = rows + 2 * PAD
    group = 8
    return pl.pallas_call(
        functools.partial(smooth_kernel, group),
        out_shape=jax.ShapeDtypeStruct((layers, ext, columns), jnp.float32),
        in_specs=[in_hbm()] + whole(2),
        out_specs=whole(1)[0],
        scratch_shapes=[
            pltpu.VMEM((layers, rows, columns), jnp.int32),
            pltpu.SemaphoreType.DMA((layers // group,)),
        ],
        compiler_params=params(16),
        cost_estimate=cost(1_000_000_000),
        name="smooth",
    )(c, by, lx)


def call_depth(flags, order, partial, *operands):
    layers, ext, columns = partial.shape
    return pl.pallas_call(
        depth_kernel,
        out_shape=(
            jax.ShapeDtypeStruct(partial.shape, jnp.float32),
            jax.ShapeDtypeStruct((layers - 8, ext, columns), jnp.float32),
        ),
        in_specs=[smem(), smem()] + whole(1 + len(operands)),
        out_specs=tuple(whole(2)),
        input_output_aliases={2: 0},
        compiler_params=params(12),
        cost_estimate=cost(500_000_000),
        name="depth",
    )(flags, order, partial, *operands)


def call_interior(scale, smoothed):
    _, ext, columns = smoothed.shape
    return pl.pallas_call(
        functools.partial(interior_kernel, scale),
        out_shape=jax.ShapeDtypeStruct((4, ext - 2 * PAD, columns), jnp.float32),
        in_specs=whole(1),
        out_specs=whole(1)[0],
        compiler_params=params(12),
        cost_estimate=cost(1_000_000_000),
        name="interior",
    )(smoothed)


def call_first_edge(scale, flags, order, plane, *operands):
    _, ext, columns = plane.shape
    f32 = jnp.float32
    return pl.pallas_call(
        functools.partial(first_edge_kernel, scale),
        out_shape=jax.ShapeDtypeStruct((4, ext - 2 * PAD, columns), f32),
        in_specs=[smem(), smem()] + whole(1 + len(operands)),
        out_specs=whole(1)[0],
        scratch_shapes=[
            pltpu.VMEM((REACH + 2, ext, columns), f32),
            pltpu.VMEM((REACH, ext, columns), f32),
        ],
        compiler_params=params(24),
        cost_estimate=cost(300_000_000),
        name="first_edge",
    )(flags, order, plane, *operands)


def call_last_edge(scale, owner_tiles, flags, order, plane, *operands):
    _, ext, columns = plane.shape
    f32 = jnp.float32
    rows = (ext - 2 * PAD) // (2 if owner_tiles else 1)
    return pl.pallas_call(
        functools.partial(last_edge_kernel, scale, owner_tiles),
        out_shape=(
            jax.ShapeDtypeStruct((4, rows, columns), f32),
            jax.ShapeDtypeStruct((REACH + 2, ext, columns), f32),
        ),
        in_specs=[smem(), smem()]
        + whole(2)
        + [in_hbm()]
        + whole(len(operands) - 2),
        out_specs=tuple(whole(2)),
        scratch_shapes=[
            pltpu.VMEM((REACH, ext, columns), f32),
            pltpu.VMEM(operands[1].shape, operands[1].dtype),
            pltpu.SemaphoreType.DMA((1,)),
        ],
        compiler_params=params(24),
        cost_estimate=cost(300_000_000),
        name="last_edge",
    )(flags, order, plane, *operands)


def call_kept_edge(scale, owner_tiles, order, ends, behind):
    _, ext, columns = ends.shape
    return pl.pallas_call(
        functools.partial(kept_edge_kernel, scale, owner_tiles),
        out_shape=jax.ShapeDtypeStruct((4, (ext - 2 * PAD) // 2, columns), jnp.float32),
        in_specs=[smem()] + whole(2),
        out_specs=whole(1)[0],
        compiler_params=params(24),
        cost_estimate=cost(200_000_000),
        name="kept_edge",
    )(order, ends, behind)


def swap(value, axis, first):
    count = lax.axis_size(axis)
    pairs = []
    for low in range(first, count - 1, 2):
        pairs += [(low, low + 1), (low + 1, low)]
    return lax.ppermute(value, axis, pairs)


def over(front, back):
    through = front[3:]
    return jnp.concatenate([front[:3] + through * back[:3], through * back[3:]], 0)


def halves_of(layers):
    count = lax.axis_size("depth")
    parity = lax.axis_index("depth") % 2
    _, rows, columns = layers.shape
    pieces = layers.reshape(4, count // 2, 2, rows // count, columns)
    send = lax.dynamic_index_in_dim(pieces, 1 - parity, 2, keepdims=False)
    keep = lax.dynamic_index_in_dim(pieces, parity, 2, keepdims=False)
    return send, keep


def exchange(send, keep):
    count = lax.axis_size("depth")
    me = lax.axis_index("depth")
    parity, pair = me % 2, me // 2
    pairs = count // 2
    send, keep = (value.reshape(4, pairs, -1, value.shape[-1]) for value in (send, keep))
    owned, columns = send.shape[2:]
    got = swap(send, "depth", 0)
    joined = jnp.where(parity == 0, over(keep, got), over(got, keep))
    parts = []
    for step in range(pairs):
        piece = lax.dynamic_index_in_dim(joined, pair ^ step, 1, keepdims=False)
        if step:
            piece = lax.ppermute(piece, "depth", [(i, i ^ (2 * step)) for i in range(count)])
        parts.append(piece)
    result = jnp.zeros((3, owned, columns), jnp.float32)
    through = jnp.ones((1, owned, columns), jnp.float32)
    for step in range(pairs):
        ahead = jnp.ones((1, owned, columns), jnp.float32)
        for other in range(pairs):
            if other != step:
                nearer = (pair ^ other) < (pair ^ step)
                ahead = ahead * jnp.where(nearer, parts[other][3:], 1.0)
        result = result + ahead * parts[step][:3]
        through = through * parts[step][3:]
    total, tilted, green = 0.225 * result[:1], 0.225 * result[1:2], 0.45 * result[2:]
    return jnp.concatenate([total + tilted, green, total - tilted, 1.0 - through], 0)


def local(counts):
    slab, rows, columns = counts.shape
    img, depth = lax.axis_index("img"), lax.axis_index("depth")
    imgs, depths = lax.axis_size("img"), lax.axis_size("depth")
    scale = 1.5 / (slab * depths)
    row_odd, depth_odd = img % 2, depth % 2
    first_a, first_b = (1 - depth_odd) * (slab - REACH), depth_odd * (slab - REACH)
    row_a, row_b = (1 - row_odd) * (rows - PAD), row_odd * (rows - PAD)
    where = jnp.stack([first_a, first_b, row_a, row_b])
    order = jnp.stack([1 - row_odd, depth_odd])
    one = jnp.float32(1.0)
    flags = jnp.stack(
        [(img > 0) * one, (img < imgs - 1) * one, (depth > 0) * one, (depth < depths - 1) * one]
    )
    by = jnp.asarray(column_matrices(columns))
    lx = jnp.asarray(row_matrices(rows))
    held = pltpu.with_memory_space_constraint(counts, pltpu.HBM)
    block_b = call_pack_block(where, held)
    side_b, edge_a, mid_a, side_a = call_pack_rest(where, held)
    block_b = swap(block_b, "depth", 1)
    xb = swap(side_b, "img", 1)
    edge_a = swap(edge_a, "depth", 0)
    mid_a = swap(mid_a, "depth", 0)
    xa = swap(side_a, "img", 0)

    def corner(far):
        of_a = lax.dynamic_slice_in_dim(edge_a, far * PAD, PAD, 1)
        of_b = lax.dynamic_slice_in_dim(block_b, far * (rows - PAD), PAD, 1)
        return jnp.concatenate([of_a, of_b], 0)

    ca = swap(corner(1 - row_odd), "img", 0)
    cb = swap(corner(row_odd), "img", 1)
    partial = call_smooth(held, by, jnp.asarray(own_matrix(rows)))
    plane, smoothed = call_depth(
        flags, order, partial, xa, xb, by, jnp.asarray(side_matrices(rows))
    )
    inner = call_interior(scale, smoothed)
    owned = rows // depths
    owner_tiles = owned // 8 if owned % 8 == 0 else 0
    common = (flags, order, plane, smoothed)
    layers = call_first_edge(
        scale, *common, block_b, ca[REACH:], cb[REACH:], by, lx, inner
    )
    send, ends = call_last_edge(
        scale, owner_tiles, *common, pltpu.with_memory_space_constraint(mid_a, pltpu.HBM), edge_a,
        ca[:REACH], cb[:REACH], by, lx, layers
    )
    if owner_tiles:
        keep = call_kept_edge(scale, owner_tiles, order, ends, layers)
    else:
        send, keep = halves_of(send)
    return exchange(send, keep)


def solution(mesh):
    in_specs = (P("depth", "img", None),)
    out_specs = P(None, ("img", "depth"), None)
    return jax.shard_map(local, mesh=mesh, in_specs=in_specs, out_specs=out_specs, check_vma=False)
```

```python
import functools
import math

import jax
import jax.numpy as jnp
import numpy as np
from jax import lax
from jax.experimental import pallas as pl
from jax.experimental.pallas import tpu as pltpu
from jax.sharding import PartitionSpec as P


gauss_taps = [
    math.exp(-offset * offset / 8.0)
    / sum((math.exp(-other * other / 8.0) for other in range(-4, 5)))
    for offset in range(-4, 5)
]
light_z = 0.48
light_x = 0.6
light_y = 0.64


REACH = 5
SIDE_GROUP = 4
PAD = 8


def band(size):
    index = np.arange(size)
    apart = np.abs(index[:, None] - index[None, :])
    taps = np.array(gauss_taps[4:] + [0.0], np.float64)
    return taps[np.minimum(apart, 5)]


def split_terms(matrix):
    high = matrix.astype(jnp.bfloat16)
    low = (matrix - high.astype(np.float64)).astype(jnp.bfloat16)
    return high, low


def column_matrices(columns):
    return np.concatenate(split_terms(band(columns)), 0)


def row_terms(matrix):
    high, low = split_terms(matrix)
    return np.concatenate([high, high, low], 1)


def row_orders(rows):
    full = band(rows + 2 * PAD)
    order = np.arange(rows + 2 * PAD)
    swapped = np.concatenate([order[rows + PAD :], order[PAD : rows + PAD], order[:PAD]])
    return [full[:, order], full[:, swapped]]


def row_matrices(rows):
    return np.stack([row_terms(matrix) for matrix in row_orders(rows)])


def own_matrix(rows):
    return row_terms(band(rows + 2 * PAD)[:, PAD : rows + PAD])


def side_matrices(rows):
    both = []
    for matrix in row_orders(rows):
        sides = np.concatenate([matrix[:, :PAD], matrix[:, rows + PAD :]], 1)
        touched = np.concatenate([sides[: 2 * PAD], sides[rows:]], 0)
        both.append(row_terms(np.kron(np.eye(SIDE_GROUP), touched)))
    return np.stack(both)


def two_terms(value, high, low):
    return jnp.dot(value, high, preferred_element_type=jnp.float32) + jnp.dot(
        value, low, preferred_element_type=jnp.float32
    )


def smooth_columns(exact, by):
    half = by.shape[0] // 2
    return two_terms(exact, by[:half], by[half:])


def column_terms(counts, by):
    exact = jnp.concatenate([c.astype(jnp.float32).astype(jnp.bfloat16) for c in counts], 0)
    wide = smooth_columns(exact, by)
    high = wide.astype(jnp.bfloat16)
    return high, (wide - high.astype(jnp.float32)).astype(jnp.bfloat16)


def row_product(matrix, high, low):
    stacked = jnp.concatenate([high, low, high], 0)
    return jnp.dot(matrix, stacked, preferred_element_type=jnp.float32)


def smooth_plane(counts, by, lx):
    rows = counts[0].shape[0]
    high, low = column_terms(counts, by)
    parts = [slice(n * rows, (n + 1) * rows) for n in range(len(counts))]
    return [row_product(lx, high[part], low[part]) for part in parts]


def smooth_depth(read, k):
    total = gauss_taps[4] * read(k)
    for offset in range(1, 5):
        total = total + gauss_taps[4 + offset] * (read(k - offset) + read(k + offset))
    return total


def smooth_depth_layer(flags, read, k, tiles, write):
    for tile in range(tiles):
        rows = pl.ds(tile * 8, 8)
        value = smooth_depth(lambda j: read(j, rows), k)
        if tile == 0:
            value = value * flags[0]
        if tile == tiles - 1:
            value = value * flags[1]
        write(rows, value)


def beside(mid, step):
    lanes = 128
    lane = lax.broadcasted_iota(jnp.int32, (mid.shape[0], lanes), 1)
    parts = [mid[:, at : at + lanes] for at in range(0, mid.shape[1], lanes)]
    turned = [pltpu.roll(part, lanes - 1 if step == 1 else 1, 1) for part in parts]
    zero = jnp.zeros_like(parts[0])
    if step == 1:
        return jnp.concatenate(
            [jnp.where(lane == lanes - 1, y, x) for x, y in zip(turned, turned[1:] + [zero])], 1
        )
    return jnp.concatenate(
        [jnp.where(lane == 0, y, x) for x, y in zip(turned, [zero] + turned[:-1])], 1
    )


def render_layer(layer, k, base, carry, scale):
    total, tilted, green, transmit = carry
    rows = pl.ds(base, 8)
    mid = layer(k, rows)
    before = layer(k, pl.ds(base - 8, 8))
    after = layer(k, pl.ds(base + 8, 8))
    sub = lax.broadcasted_iota(jnp.int32, mid.shape, 0)
    above = pltpu.roll(jnp.where(sub == 7, before, mid), 1, 0)
    below = pltpu.roll(jnp.where(sub == 0, after, mid), 7, 0)
    dz = layer(k + 1, rows) - layer(k - 1, rows)
    dx = below - above
    dy = beside(mid, 1) - beside(mid, -1)
    slope = (1.5 * light_z) * dz + (1.5 * light_x) * dx + (1.5 * light_y) * dy
    shading = jnp.tanh(slope) + (0.55 / 0.45)
    gradient_sq4 = dz * dz + dx * dx + dy * dy
    square = mid * mid
    optical = (square / (1.0 + square)) * (1.0 + gradient_sq4)
    centred = mid - 2.5
    log2e = math.log2(math.e)
    remaining = transmit * jnp.exp2(optical * (-scale * log2e))
    lit = (transmit - remaining) * shading
    return (
        total + lit,
        tilted + lit * jnp.tanh(centred),
        green + lit * jnp.exp2((centred * -log2e) * centred),
        remaining,
    )


def empty_carry(columns):
    zero = jnp.zeros((8, columns), jnp.float32)
    return zero, zero, zero, jnp.ones_like(zero)


def read_tile(ref, tile):
    rows = pl.ds(pl.multiple_of(tile * 8, 8), 8)
    return tuple(ref[n, rows, :] for n in range(4))


def store_tile(ref, tile, values):
    rows = pl.ds(pl.multiple_of(tile * 8, 8), 8)
    for n, value in enumerate(values):
        ref[n, rows, :] = value


def run_copies(copies):
    for copy in copies:
        copy.start()
    for copy in copies:
        copy.wait()


def run_copies(pairs, sems):
    copies = [pltpu.make_async_copy(*pair, sems.at[n]) for n, pair in enumerate(pairs)]
    for copy in copies:
        copy.start()
    for copy in copies:
        copy.wait()


def pack_block_kernel(where, c, block, sems):
    half = block.shape[1] // 2
    layers = pl.ds(where[1], REACH)
    parts = [pl.ds(n * half, half) for n in range(2)]
    run_copies([(c.at[layers, part], block.at[:, part]) for part in parts], sems)


def pack_rest_kernel(where, c, side_b, edge, middle, side_a, sems):
    rows = c.shape[1]
    layers = pl.ds(where[0], REACH)
    pairs = [
        (c.at[:, pl.ds(pl.multiple_of(where[2 + n], PAD), PAD)], side)
        for n, side in enumerate((side_a, side_b))
    ]
    pairs.append((c.at[layers, pl.ds(0, PAD)], edge.at[:, pl.ds(0, PAD)]))
    pairs.append((c.at[layers, pl.ds(rows - PAD, PAD)], edge.at[:, pl.ds(PAD, PAD)]))
    pairs.append((c.at[layers, pl.ds(PAD, rows - 2 * PAD)], middle))
    run_copies(pairs, sems)


def smooth_kernel(group, c_hbm, by, lx, plane, c, sems):
    groups = c.shape[0] // group

    def fetch(g):
        part = pl.ds(g * group, group)
        return pltpu.make_async_copy(c_hbm.at[part], c.at[part], sems.at[g])

    for g in range(groups):
        fetch(g).start()

    def smooth_group(g, _):
        first = g * group
        fetch(g).wait()
        counts = [c[first + n] for n in range(group)]
        for n, value in enumerate(smooth_plane(counts, by, lx[...])):
            plane[first + n] = value
        return 0

    lax.fori_loop(0, groups, smooth_group, 0)


def depth_kernel(flags, order, partial, xa, xb, by, lx, plane, smoothed):
    layers, ext, _ = plane.shape
    group = 2 * SIDE_GROUP
    edge = 2 * PAD
    sides = lx[order[0]]

    def add_sides(g, _):
        first = g * group
        counts = [jnp.concatenate([xa[first + n], xb[first + n]], 0) for n in range(group)]
        high, low = column_terms(counts, by)
        for half in range(2):
            part = slice(half * SIDE_GROUP * edge, (half + 1) * SIDE_GROUP * edge)
            added = row_product(sides, high[part], low[part])
            for n in range(SIDE_GROUP):
                k = first + half * SIDE_GROUP + n
                at = n * 2 * edge
                plane[k, :edge, :] = partial[k, :edge, :] + added[at : at + edge]
                plane[k, ext - edge :, :] = (
                    partial[k, ext - edge :, :] + added[at + edge : at + 2 * edge]
                )
        return 0

    lax.fori_loop(0, layers // group, add_sides, 0)

    def one_layer(j, _):
        def write(rows, value):
            smoothed[j, rows, :] = value

        smooth_depth_layer(flags, lambda k, rows: plane[k, rows, :], j + 4, ext // 8, write)
        return 0

    lax.fori_loop(0, layers - 8, one_layer, 0)


def interior_kernel(scale, smoothed, image):
    held, ext, columns = smoothed.shape

    def one_tile(tile, _):
        base = pl.multiple_of(tile * 8 + 8, 8)
        carry = empty_carry(columns)
        for k in range(1, held - 1):
            carry = render_layer(lambda k, rows: smoothed[k, rows, :], k, base, carry, scale)
        store_tile(image, tile, carry)
        return 0

    lax.fori_loop(0, ext // 8 - 2, one_tile, 0)


def edge_smooth(turn, flags, order, plane, smoothed, tile, ca, cb, by, lx, ends, halo):
    layers, ext, _ = plane.shape
    rows_of = order[0]
    is_front = order[1] == 1 - turn
    sign = jnp.where(is_front, 1, -1)
    counts = [jnp.concatenate([ca[j], tile(j), cb[j]], 0) for j in range(REACH)]
    for j, value in enumerate(smooth_plane(counts, by, lx[rows_of])):
        halo[j] = value
    plane_face = jnp.where(is_front, 0, layers - 1)
    halo_face = jnp.where(is_front, REACH, -1)
    ends_face = jnp.where(is_front, 1, REACH)
    smoothed_face = jnp.where(is_front, -4, layers - 5)
    on_grid = jnp.where(is_front, flags[2], flags[3])

    def counted(v, rows):
        if v < 0:
            return halo[halo_face + sign * v, rows, :]
        return plane[plane_face + sign * v, rows, :]

    for v in range(-1, 4):

        def write(rows, value, v=v):
            ends[ends_face + sign * v, rows, :] = value * on_grid if v < 0 else value

        smooth_depth_layer(flags, counted, v, ext // 8, write)
    for v in (4, 5):
        ends[ends_face + sign * v] = smoothed[smoothed_face + sign * v]


def edge_render(scale, is_front, ends, behind, image, tiles, tile_of, first=0):
    columns = ends.shape[2]

    def one_tile(place, _):
        tile = tile_of(place + first)
        base = pl.multiple_of(tile * 8 + 8, 8)
        carry = empty_carry(columns)
        for k in range(1, REACH + 1):
            carry = render_layer(lambda k, rows: ends[k, rows, :], k, base, carry, scale)
        other = read_tile(behind, tile)
        front = [jnp.where(is_front, x, y) for x, y in zip(carry, other)]
        back = [jnp.where(is_front, y, x) for x, y in zip(carry, other)]
        colors = [front[n] + front[3] * back[n] for n in range(3)]
        colors.append(front[3] * back[3])
        if len(image.shape) == 3:
            store_tile(image, place, colors)
        else:
            owner_tiles = image.shape[2] // 8
            store_tile(image.at[place // owner_tiles], place % owner_tiles, colors)
        return 0

    lax.fori_loop(0, tiles, one_tile, 0)


def half_tiles(order, pairs, owner_tiles, wanted):
    def tile_of(place):
        pair = order[2] ^ (pairs - 1 - place // owner_tiles)
        return (2 * pair + wanted) * owner_tiles + place % owner_tiles

    return tile_of


def first_edge_kernel(scale, flags, order, plane, smoothed, block, ca, cb, by, lx, behind, image,
                      ends, halo):
    tile = lambda j: block[j]
    edge_smooth(1, flags, order, plane, smoothed, tile, ca, cb, by, lx, ends, halo)
    tiles = plane.shape[1] // 8 - 2
    edge_render(scale, order[1] == 0, ends, behind, image, tiles, lambda place: place)


def render_halves(scale, is_front, ends, behind, images, tile_of):
    for n, image in enumerate(images):
        places, _, owned, _ = image.shape
        tiles = places * (owned // 8)
        edge_render(scale, is_front, ends, behind, image, tiles, tile_of, n * tiles)


def last_edge_kernel(scale, split, flags, order, plane, smoothed, middle_any, edge, ca, cb,
                     by, lx, behind, *refs):
    images, (ends, halo, middle, sem) = refs[:-4], refs[-4:]
    run_copies([(middle_any, middle)], sem)
    tile = lambda j: jnp.concatenate([edge[j, :PAD], middle[j], edge[j, PAD:]], 0)
    edge_smooth(0, flags, order, plane, smoothed, tile, ca, cb, by, lx, ends, halo)
    if split:
        tile_of = half_tiles(order, *split, 1 - order[1])
        render_halves(scale, order[1] == 1, ends, behind, images, tile_of)
    else:
        tiles = plane.shape[1] // 8 - 2
        edge_render(scale, order[1] == 1, ends, behind, images[0], tiles, lambda place: place)


def kept_edge_kernel(scale, split, order, ends, behind, *images):
    tile_of = half_tiles(order, *split, order[1])
    render_halves(scale, order[1] == 1, ends, behind, images, tile_of)


def whole(count):
    return [pl.BlockSpec(memory_space=pltpu.VMEM)] * count


def smem():
    return pl.BlockSpec(memory_space=pltpu.SMEM)


def in_hbm():
    return pl.BlockSpec(memory_space=pltpu.HBM)


def params(mib):
    return pltpu.CompilerParams(vmem_limit_bytes=mib * 1024 * 1024)


def cost(flops):
    return pl.CostEstimate(flops=flops, transcendentals=0, bytes_accessed=4_000_000)


def call_pack_block(where, c):
    _, rows, columns = c.shape
    return pl.pallas_call(
        pack_block_kernel,
        out_shape=jax.ShapeDtypeStruct((REACH, rows, columns), c.dtype),
        in_specs=[smem(), in_hbm()],
        out_specs=whole(1)[0],
        scratch_shapes=[pltpu.SemaphoreType.DMA((2,))],
        compiler_params=params(8),
        name="pack_block",
    )(where, c)


def call_pack_rest(where, c):
    layers, rows, columns = c.shape
    edge = jax.ShapeDtypeStruct((REACH, 2 * PAD, columns), c.dtype)
    side = jax.ShapeDtypeStruct((layers, PAD, columns), c.dtype)
    middle = jax.ShapeDtypeStruct((REACH, rows - 2 * PAD, columns), c.dtype)
    return pl.pallas_call(
        pack_rest_kernel,
        out_shape=(side, edge, middle, side),
        in_specs=[smem(), in_hbm()],
        out_specs=tuple(whole(4)),
        scratch_shapes=[pltpu.SemaphoreType.DMA((5,))],
        compiler_params=params(8),
        name="pack_rest",
    )(where, c)


def call_smooth(c, by, lx):
    layers, rows, columns = c.shape
    ext = rows + 2 * PAD
    group = 8
    return pl.pallas_call(
        functools.partial(smooth_kernel, group),
        out_shape=jax.ShapeDtypeStruct((layers, ext, columns), jnp.float32),
        in_specs=[in_hbm()] + whole(2),
        out_specs=whole(1)[0],
        scratch_shapes=[
            pltpu.VMEM((layers, rows, columns), jnp.int32),
            pltpu.SemaphoreType.DMA((layers // group,)),
        ],
        compiler_params=params(16),
        cost_estimate=cost(1_000_000_000),
        name="smooth",
    )(c, by, lx)


def call_depth(flags, order, partial, *operands):
    layers, ext, columns = partial.shape
    return pl.pallas_call(
        depth_kernel,
        out_shape=(
            jax.ShapeDtypeStruct(partial.shape, jnp.float32),
            jax.ShapeDtypeStruct((layers - 8, ext, columns), jnp.float32),
        ),
        in_specs=[smem(), smem()] + whole(1 + len(operands)),
        out_specs=tuple(whole(2)),
        input_output_aliases={2: 0},
        compiler_params=params(12),
        cost_estimate=cost(500_000_000),
        name="depth",
    )(flags, order, partial, *operands)


def call_interior(scale, smoothed):
    _, ext, columns = smoothed.shape
    return pl.pallas_call(
        functools.partial(interior_kernel, scale),
        out_shape=jax.ShapeDtypeStruct((4, ext - 2 * PAD, columns), jnp.float32),
        in_specs=whole(1),
        out_specs=whole(1)[0],
        compiler_params=params(12),
        cost_estimate=cost(1_000_000_000),
        name="interior",
    )(smoothed)


def call_first_edge(scale, flags, order, plane, *operands):
    _, ext, columns = plane.shape
    f32 = jnp.float32
    return pl.pallas_call(
        functools.partial(first_edge_kernel, scale),
        out_shape=jax.ShapeDtypeStruct((4, ext - 2 * PAD, columns), f32),
        in_specs=[smem(), smem()] + whole(1 + len(operands)),
        out_specs=whole(1)[0],
        scratch_shapes=[
            pltpu.VMEM((REACH + 2, ext, columns), f32),
            pltpu.VMEM((REACH, ext, columns), f32),
        ],
        compiler_params=params(24),
        cost_estimate=cost(300_000_000),
        name="first_edge",
    )(flags, order, plane, *operands)


def half_shape(split, columns):
    pairs, owner_tiles = split
    return pairs // 2, 4, owner_tiles * 8, columns


def call_last_edge(scale, split, flags, order, plane, *operands):
    _, ext, columns = plane.shape
    f32 = jnp.float32
    rows = ext - 2 * PAD
    images = 2 * [half_shape(split, columns)] if split else [(4, rows, columns)]
    shapes = [*images, (REACH + 2, ext, columns)]
    return pl.pallas_call(
        functools.partial(last_edge_kernel, scale, split),
        out_shape=tuple(jax.ShapeDtypeStruct(shape, f32) for shape in shapes),
        in_specs=[smem(), smem()] + whole(2) + [in_hbm()] + whole(len(operands) - 2),
        out_specs=tuple(whole(len(shapes))),
        scratch_shapes=[
            pltpu.VMEM((REACH, ext, columns), f32),
            pltpu.VMEM(operands[1].shape, operands[1].dtype),
            pltpu.SemaphoreType.DMA((1,)),
        ],
        compiler_params=params(12),
        cost_estimate=cost(300_000_000),
        name="last_edge",
    )(flags, order, plane, *operands)


def call_kept_edge(scale, split, order, ends, behind):
    image = jax.ShapeDtypeStruct(half_shape(split, ends.shape[2]), jnp.float32)
    return pl.pallas_call(
        functools.partial(kept_edge_kernel, scale, split),
        out_shape=(image, image),
        in_specs=[smem()] + whole(2),
        out_specs=tuple(whole(2)),
        compiler_params=params(12),
        cost_estimate=cost(200_000_000),
        name="kept_edge",
    )(order, ends, behind)


def swap(value, axis, first):
    count = lax.axis_size(axis)
    pairs = []
    for low in range(first, count - 1, 2):
        pairs += [(low, low + 1), (low + 1, low)]
    return lax.ppermute(value, axis, pairs)


def over(front, back):
    through = front[:, 3:]
    return jnp.concatenate([front[:, :3] + through * back[:, :3], through * back[:, 3:]], 1)


def halves_of(layers):
    count = lax.axis_size("depth")
    me = lax.axis_index("depth")
    parity, pair, pairs = me % 2, me // 2, count // 2
    _, rows, columns = layers.shape
    pieces = layers.reshape(4, pairs, 2, rows // count, columns)
    ordered = jnp.concatenate(
        [lax.dynamic_slice_in_dim(pieces, pair ^ step, 1, 1) for step in reversed(range(pairs))], 1
    )
    both = []
    for wanted in (1 - parity, parity):
        chosen = lax.dynamic_index_in_dim(ordered, wanted, 2, keepdims=False)
        chosen = jnp.moveaxis(chosen, 1, 0)
        both.append((chosen[: pairs // 2], chosen[pairs // 2 :]))
    return both


def exchange(sends, keeps):
    count = lax.axis_size("depth")
    me = lax.axis_index("depth")
    parity, pair = me % 2, me // 2
    pairs = count // 2
    parts = [None] * pairs
    for half, (send, keep) in enumerate(zip(sends, keeps)):
        owned, columns = send.shape[2:]
        got = swap(send, "depth", 0)
        joined = jnp.where(parity == 0, over(keep, got), over(got, keep))
        for place in range(pairs // 2):
            step = pairs - 1 - half * (pairs // 2) - place
            piece = joined[place]
            if step:
                piece = lax.ppermute(piece, "depth", [(i, i ^ (2 * step)) for i in range(count)])
            parts[step] = piece
    result = jnp.zeros((3, owned, columns), jnp.float32)
    through = jnp.ones((1, owned, columns), jnp.float32)
    for step in range(pairs):
        ahead = jnp.ones((1, owned, columns), jnp.float32)
        for other in range(pairs):
            if other != step:
                nearer = (pair ^ other) < (pair ^ step)
                ahead = ahead * jnp.where(nearer, parts[other][3:], 1.0)
        result = result + ahead * parts[step][:3]
        through = through * parts[step][3:]
    total, tilted, green = 0.225 * result[:1], 0.225 * result[1:2], 0.45 * result[2:]
    return jnp.concatenate([total + tilted, green, total - tilted, 1.0 - through], 0)


def local(counts):
    slab, rows, columns = counts.shape
    img, depth = lax.axis_index("img"), lax.axis_index("depth")
    imgs, depths = lax.axis_size("img"), lax.axis_size("depth")
    scale = 1.5 / (slab * depths)
    row_odd, depth_odd = img % 2, depth % 2
    first_a, first_b = (1 - depth_odd) * (slab - REACH), depth_odd * (slab - REACH)
    row_a, row_b = (1 - row_odd) * (rows - PAD), row_odd * (rows - PAD)
    where = jnp.stack([first_a, first_b, row_a, row_b])
    order = jnp.stack([1 - row_odd, depth_odd, depth // 2])
    one = jnp.float32(1.0)
    flags = jnp.stack(
        [(img > 0) * one, (img < imgs - 1) * one, (depth > 0) * one, (depth < depths - 1) * one]
    )
    by = jnp.asarray(column_matrices(columns))
    lx = jnp.asarray(row_matrices(rows))
    held = pltpu.with_memory_space_constraint(counts, pltpu.HBM)
    block_b = call_pack_block(where, held)
    side_b, edge_a, mid_a, side_a = call_pack_rest(where, held)
    block_b = swap(block_b, "depth", 1)
    xb = swap(side_b, "img", 1)
    edge_a = swap(edge_a, "depth", 0)
    mid_a = swap(mid_a, "depth", 0)
    xa = swap(side_a, "img", 0)

    def corner(far):
        of_a = lax.dynamic_slice_in_dim(edge_a, far * PAD, PAD, 1)
        of_b = lax.dynamic_slice_in_dim(block_b, far * (rows - PAD), PAD, 1)
        return jnp.concatenate([of_a, of_b], 0)

    ca = swap(corner(1 - row_odd), "img", 0)
    cb = swap(corner(row_odd), "img", 1)
    partial = call_smooth(held, by, jnp.asarray(own_matrix(rows)))
    plane, smoothed = call_depth(
        flags, order, partial, xa, xb, by, jnp.asarray(side_matrices(rows))
    )
    inner = call_interior(scale, smoothed)
    owned = rows // depths
    split = (depths // 2, owned // 8) if owned % 8 == 0 else None
    common = (flags, order, plane, smoothed)
    layers = call_first_edge(
        scale, *common, block_b, ca[REACH:], cb[REACH:], by, lx, inner
    )
    mid_a = pltpu.with_memory_space_constraint(mid_a, pltpu.HBM)
    *sends, ends = call_last_edge(
        scale, split, *common, mid_a, edge_a, ca[:REACH], cb[:REACH], by, lx, layers
    )
    if split:
        keeps = call_kept_edge(scale, split, order, ends, layers)
    else:
        sends, keeps = halves_of(sends[0])
    return exchange(sends, keeps)


def solution(mesh):
    in_specs = (P("depth", "img", None),)
    out_specs = P(None, ("img", "depth"), None)
    return jax.shard_map(local, mesh=mesh, in_specs=in_specs, out_specs=out_specs, check_vma=False)
```

```python
import functools
import math

import jax
import jax.numpy as jnp
import numpy as np
from jax import lax
from jax.experimental import pallas as pl
from jax.experimental.pallas import tpu as pltpu
from jax.sharding import PartitionSpec as P


gauss_taps = [
    math.exp(-offset * offset / 8.0)
    / sum((math.exp(-other * other / 8.0) for other in range(-4, 5)))
    for offset in range(-4, 5)
]
light_z = 0.48
light_x = 0.6
light_y = 0.64


REACH = 5
SIDE_GROUP = 4
PAD = 8


def band(size):
    index = np.arange(size)
    apart = np.abs(index[:, None] - index[None, :])
    taps = np.array(gauss_taps[4:] + [0.0], np.float64)
    return taps[np.minimum(apart, 5)]


def split_terms(matrix):
    high = matrix.astype(jnp.bfloat16)
    low = (matrix - high.astype(np.float64)).astype(jnp.bfloat16)
    return high, low


def column_matrices(columns):
    return np.concatenate(split_terms(band(columns)), 0)


def row_terms(matrix):
    high, low = split_terms(matrix)
    return np.concatenate([high, high, low], 1)


def row_orders(rows):
    full = band(rows + 2 * PAD)
    order = np.arange(rows + 2 * PAD)
    swapped = np.concatenate([order[rows + PAD :], order[PAD : rows + PAD], order[:PAD]])
    return [full[:, order], full[:, swapped]]


def row_matrices(rows):
    return np.stack([row_terms(matrix) for matrix in row_orders(rows)])


def own_matrix(rows):
    return row_terms(band(rows + 2 * PAD)[:, PAD : rows + PAD])


def side_matrices(rows):
    both = []
    for matrix in row_orders(rows):
        sides = np.concatenate([matrix[:, :PAD], matrix[:, rows + PAD :]], 1)
        touched = np.concatenate([sides[: 2 * PAD], sides[rows:]], 0)
        both.append(row_terms(np.kron(np.eye(SIDE_GROUP), touched)))
    return np.stack(both)


def two_terms(value, high, low):
    return jnp.dot(value, high, preferred_element_type=jnp.float32) + jnp.dot(
        value, low, preferred_element_type=jnp.float32
    )


def smooth_columns(exact, by):
    half = by.shape[0] // 2
    return two_terms(exact, by[:half], by[half:])


def column_terms(counts, by):
    exact = jnp.concatenate([c.astype(jnp.float32).astype(jnp.bfloat16) for c in counts], 0)
    wide = smooth_columns(exact, by)
    high = wide.astype(jnp.bfloat16)
    return high, (wide - high.astype(jnp.float32)).astype(jnp.bfloat16)


def row_product(matrix, high, low):
    stacked = jnp.concatenate([high, low, high], 0)
    return jnp.dot(matrix, stacked, preferred_element_type=jnp.float32)


def smooth_plane(counts, by, lx):
    rows = counts[0].shape[0]
    high, low = column_terms(counts, by)
    parts = [slice(n * rows, (n + 1) * rows) for n in range(len(counts))]
    return [row_product(lx, high[part], low[part]) for part in parts]


def smooth_depth(read, k):
    total = gauss_taps[4] * read(k)
    for offset in range(1, 5):
        total = total + gauss_taps[4 + offset] * (read(k - offset) + read(k + offset))
    return total


def smooth_depth_layer(flags, read, k, tiles, write):
    for tile in range(tiles):
        rows = pl.ds(tile * 8, 8)
        value = smooth_depth(lambda j: read(j, rows), k)
        if tile == 0:
            value = value * flags[0]
        if tile == tiles - 1:
            value = value * flags[1]
        write(rows, value)


def beside(mid, step):
    lanes = 128
    lane = lax.broadcasted_iota(jnp.int32, (mid.shape[0], lanes), 1)
    parts = [mid[:, at : at + lanes] for at in range(0, mid.shape[1], lanes)]
    turned = [pltpu.roll(part, lanes - 1 if step == 1 else 1, 1) for part in parts]
    zero = jnp.zeros_like(parts[0])
    if step == 1:
        return jnp.concatenate(
            [jnp.where(lane == lanes - 1, y, x) for x, y in zip(turned, turned[1:] + [zero])], 1
        )
    return jnp.concatenate(
        [jnp.where(lane == 0, y, x) for x, y in zip(turned, [zero] + turned[:-1])], 1
    )


def render_layer(layer, k, base, carry, scale):
    total, tilted, green, transmit = carry
    rows = pl.ds(base, 8)
    mid = layer(k, rows)
    before = layer(k, pl.ds(base - 8, 8))
    after = layer(k, pl.ds(base + 8, 8))
    sub = lax.broadcasted_iota(jnp.int32, mid.shape, 0)
    above = pltpu.roll(jnp.where(sub == 7, before, mid), 1, 0)
    below = pltpu.roll(jnp.where(sub == 0, after, mid), 7, 0)
    dz = layer(k + 1, rows) - layer(k - 1, rows)
    dx = below - above
    dy = beside(mid, 1) - beside(mid, -1)
    slope = (1.5 * light_z) * dz + (1.5 * light_x) * dx + (1.5 * light_y) * dy
    shading = jnp.tanh(slope) + (0.55 / 0.45)
    gradient_sq4 = dz * dz + dx * dx + dy * dy
    square = mid * mid
    optical = (square / (1.0 + square)) * (1.0 + gradient_sq4)
    centred = mid - 2.5
    log2e = math.log2(math.e)
    remaining = transmit * jnp.exp2(optical * (-scale * log2e))
    lit = (transmit - remaining) * shading
    return (
        total + lit,
        tilted + lit * jnp.tanh(centred),
        green + lit * jnp.exp2((centred * -log2e) * centred),
        remaining,
    )


def empty_carry(columns):
    zero = jnp.zeros((8, columns), jnp.float32)
    return zero, zero, zero, jnp.ones_like(zero)


def read_tile(ref, tile):
    rows = pl.ds(pl.multiple_of(tile * 8, 8), 8)
    return tuple(ref[n, rows, :] for n in range(4))


def store_tile(ref, tile, values):
    rows = pl.ds(pl.multiple_of(tile * 8, 8), 8)
    for n, value in enumerate(values):
        ref[n, rows, :] = value


def run_copies(copies):
    for copy in copies:
        copy.start()
    for copy in copies:
        copy.wait()


def run_copies(pairs, sems):
    copies = [pltpu.make_async_copy(*pair, sems.at[n]) for n, pair in enumerate(pairs)]
    for copy in copies:
        copy.start()
    for copy in copies:
        copy.wait()


def pack_block_kernel(where, c, block, sems):
    half = block.shape[1] // 2
    layers = pl.ds(where[1], REACH)
    parts = [pl.ds(n * half, half) for n in range(2)]
    run_copies([(c.at[layers, part], block.at[:, part]) for part in parts], sems)


def pack_rest_kernel(where, c, side_b, edge, middle, side_a, sems):
    rows = c.shape[1]
    layers = pl.ds(where[0], REACH)
    pairs = [
        (c.at[:, pl.ds(pl.multiple_of(where[2 + n], PAD), PAD)], side)
        for n, side in enumerate((side_a, side_b))
    ]
    pairs.append((c.at[layers, pl.ds(0, PAD)], edge.at[:, pl.ds(0, PAD)]))
    pairs.append((c.at[layers, pl.ds(rows - PAD, PAD)], edge.at[:, pl.ds(PAD, PAD)]))
    pairs.append((c.at[layers, pl.ds(PAD, rows - 2 * PAD)], middle))
    run_copies(pairs, sems)


def smooth_kernel(group, c_hbm, by, lx, plane, c, sems):
    groups = c.shape[0] // group

    def fetch(g):
        part = pl.ds(g * group, group)
        return pltpu.make_async_copy(c_hbm.at[part], c.at[part], sems.at[g])

    for g in range(groups):
        fetch(g).start()

    def smooth_group(g, _):
        first = g * group
        fetch(g).wait()
        counts = [c[first + n] for n in range(group)]
        for n, value in enumerate(smooth_plane(counts, by, lx[...])):
            plane[first + n] = value
        return 0

    lax.fori_loop(0, groups, smooth_group, 0)


def depth_kernel(flags, order, partial, xa, xb, by, lx, plane, smoothed):
    layers, ext, _ = plane.shape
    group = 4 * SIDE_GROUP
    edge = 2 * PAD
    sides = lx[order[0]]

    def add_sides(g, _):
        first = g * group
        counts = [jnp.concatenate([xa[first + n], xb[first + n]], 0) for n in range(group)]
        high, low = column_terms(counts, by)
        for half in range(4):
            part = slice(half * SIDE_GROUP * edge, (half + 1) * SIDE_GROUP * edge)
            added = row_product(sides, high[part], low[part])
            for n in range(SIDE_GROUP):
                k = first + half * SIDE_GROUP + n
                at = n * 2 * edge
                plane[k, :edge, :] = partial[k, :edge, :] + added[at : at + edge]
                plane[k, ext - edge :, :] = (
                    partial[k, ext - edge :, :] + added[at + edge : at + 2 * edge]
                )
        return 0

    lax.fori_loop(0, layers // group, add_sides, 0)

    def one_layer(j, _):
        def write(rows, value):
            smoothed[j, rows, :] = value

        smooth_depth_layer(flags, lambda k, rows: plane[k, rows, :], j + 4, ext // 8, write)
        return 0

    lax.fori_loop(0, layers - 8, one_layer, 0)


def interior_kernel(scale, smoothed, image):
    held, ext, columns = smoothed.shape

    def one_tile(tile, _):
        base = pl.multiple_of(tile * 8 + 8, 8)
        carry = empty_carry(columns)
        for k in range(1, held - 1):
            carry = render_layer(lambda k, rows: smoothed[k, rows, :], k, base, carry, scale)
        store_tile(image, tile, carry)
        return 0

    lax.fori_loop(0, ext // 8 - 2, one_tile, 0)


def edge_smooth(turn, flags, order, plane, smoothed, tile, ca, cb, by, lx, ends, halo):
    layers, ext, _ = plane.shape
    rows_of = order[0]
    is_front = order[1] == 1 - turn
    sign = jnp.where(is_front, 1, -1)
    counts = [jnp.concatenate([ca[j], tile(j), cb[j]], 0) for j in range(REACH)]
    for j, value in enumerate(smooth_plane(counts, by, lx[rows_of])):
        halo[j] = value
    plane_face = jnp.where(is_front, 0, layers - 1)
    halo_face = jnp.where(is_front, REACH, -1)
    ends_face = jnp.where(is_front, 1, REACH)
    smoothed_face = jnp.where(is_front, -4, layers - 5)
    on_grid = jnp.where(is_front, flags[2], flags[3])

    def counted(v, rows):
        if v < 0:
            return halo[halo_face + sign * v, rows, :]
        return plane[plane_face + sign * v, rows, :]

    for v in range(-1, 4):

        def write(rows, value, v=v):
            ends[ends_face + sign * v, rows, :] = value * on_grid if v < 0 else value

        smooth_depth_layer(flags, counted, v, ext // 8, write)
    for v in (4, 5):
        ends[ends_face + sign * v] = smoothed[smoothed_face + sign * v]


def edge_render(scale, is_front, ends, behind, image, tiles, tile_of, first=0):
    columns = ends.shape[2]

    def one_tile(place, _):
        tile = tile_of(place + first)
        base = pl.multiple_of(tile * 8 + 8, 8)
        carry = empty_carry(columns)
        for k in range(1, REACH + 1):
            carry = render_layer(lambda k, rows: ends[k, rows, :], k, base, carry, scale)
        other = read_tile(behind, tile)
        front = [jnp.where(is_front, x, y) for x, y in zip(carry, other)]
        back = [jnp.where(is_front, y, x) for x, y in zip(carry, other)]
        colors = [front[n] + front[3] * back[n] for n in range(3)]
        colors.append(front[3] * back[3])
        if len(image.shape) == 3:
            store_tile(image, place, colors)
        else:
            owner_tiles = image.shape[2] // 8
            store_tile(image.at[place // owner_tiles], place % owner_tiles, colors)
        return 0

    lax.fori_loop(0, tiles, one_tile, 0)


def half_tiles(order, pairs, owner_tiles, wanted):
    def tile_of(place):
        pair = order[2] ^ (pairs - 1 - place // owner_tiles)
        return (2 * pair + wanted) * owner_tiles + place % owner_tiles

    return tile_of


def first_edge_kernel(scale, flags, order, plane, smoothed, block, ca, cb, by, lx, behind, image,
                      ends, halo):
    tile = lambda j: block[j]
    edge_smooth(1, flags, order, plane, smoothed, tile, ca, cb, by, lx, ends, halo)
    tiles = plane.shape[1] // 8 - 2
    edge_render(scale, order[1] == 0, ends, behind, image, tiles, lambda place: place)


def render_half(scale, is_front, ends, behind, image, tile_of, half):
    places, _, owned, _ = image.shape
    tiles = places * (owned // 8)
    edge_render(scale, is_front, ends, behind, image, tiles, tile_of, half * tiles)


def last_edge_kernel(scale, split, flags, order, plane, smoothed, middle_any, edge, ca, cb,
                     by, lx, behind, *refs):
    images, (ends, halo, middle, sem) = refs[:-4], refs[-4:]
    run_copies([(middle_any, middle)], sem)
    tile = lambda j: jnp.concatenate([edge[j, :PAD], middle[j], edge[j, PAD:]], 0)
    edge_smooth(0, flags, order, plane, smoothed, tile, ca, cb, by, lx, ends, halo)
    if split:
        tile_of = half_tiles(order, *split, 1 - order[1])
        for half, image in enumerate(images):
            render_half(scale, order[1] == 1, ends, behind, image, tile_of, half)
    else:
        tiles = plane.shape[1] // 8 - 2
        edge_render(scale, order[1] == 1, ends, behind, images[0], tiles, lambda place: place)


def kept_edge_kernel(scale, split, half, order, ends, behind, image):
    tile_of = half_tiles(order, *split, order[1])
    render_half(scale, order[1] == 1, ends, behind, image, tile_of, half)


def whole(count):
    return [pl.BlockSpec(memory_space=pltpu.VMEM)] * count


def smem():
    return pl.BlockSpec(memory_space=pltpu.SMEM)


def in_hbm():
    return pl.BlockSpec(memory_space=pltpu.HBM)


def params(mib):
    return pltpu.CompilerParams(vmem_limit_bytes=mib * 1024 * 1024)


def cost(flops):
    return pl.CostEstimate(flops=flops, transcendentals=0, bytes_accessed=4_000_000)


def call_pack_block(where, c):
    _, rows, columns = c.shape
    return pl.pallas_call(
        pack_block_kernel,
        out_shape=jax.ShapeDtypeStruct((REACH, rows, columns), c.dtype),
        in_specs=[smem(), in_hbm()],
        out_specs=whole(1)[0],
        scratch_shapes=[pltpu.SemaphoreType.DMA((2,))],
        compiler_params=params(8),
        name="pack_block",
    )(where, c)


def call_pack_rest(where, c):
    layers, rows, columns = c.shape
    edge = jax.ShapeDtypeStruct((REACH, 2 * PAD, columns), c.dtype)
    side = jax.ShapeDtypeStruct((layers, PAD, columns), c.dtype)
    middle = jax.ShapeDtypeStruct((REACH, rows - 2 * PAD, columns), c.dtype)
    return pl.pallas_call(
        pack_rest_kernel,
        out_shape=(side, edge, middle, side),
        in_specs=[smem(), in_hbm()],
        out_specs=tuple(whole(4)),
        scratch_shapes=[pltpu.SemaphoreType.DMA((5,))],
        compiler_params=params(8),
        name="pack_rest",
    )(where, c)


def call_smooth(c, by, lx):
    layers, rows, columns = c.shape
    ext = rows + 2 * PAD
    group = 8
    return pl.pallas_call(
        functools.partial(smooth_kernel, group),
        out_shape=jax.ShapeDtypeStruct((layers, ext, columns), jnp.float32),
        in_specs=[in_hbm()] + whole(2),
        out_specs=whole(1)[0],
        scratch_shapes=[
            pltpu.VMEM((layers, rows, columns), jnp.int32),
            pltpu.SemaphoreType.DMA((layers // group,)),
        ],
        compiler_params=params(16),
        cost_estimate=cost(1_000_000_000),
        name="smooth",
    )(c, by, lx)


def call_depth(flags, order, partial, *operands):
    layers, ext, columns = partial.shape
    return pl.pallas_call(
        depth_kernel,
        out_shape=(
            jax.ShapeDtypeStruct(partial.shape, jnp.float32),
            jax.ShapeDtypeStruct((layers - 8, ext, columns), jnp.float32),
        ),
        in_specs=[smem(), smem()] + whole(1 + len(operands)),
        out_specs=tuple(whole(2)),
        input_output_aliases={2: 0},
        compiler_params=params(12),
        cost_estimate=cost(500_000_000),
        name="depth",
    )(flags, order, partial, *operands)


def call_interior(scale, smoothed):
    _, ext, columns = smoothed.shape
    return pl.pallas_call(
        functools.partial(interior_kernel, scale),
        out_shape=jax.ShapeDtypeStruct((4, ext - 2 * PAD, columns), jnp.float32),
        in_specs=whole(1),
        out_specs=whole(1)[0],
        compiler_params=params(12),
        cost_estimate=cost(1_000_000_000),
        name="interior",
    )(smoothed)


def call_first_edge(scale, flags, order, plane, *operands):
    _, ext, columns = plane.shape
    f32 = jnp.float32
    return pl.pallas_call(
        functools.partial(first_edge_kernel, scale),
        out_shape=jax.ShapeDtypeStruct((4, ext - 2 * PAD, columns), f32),
        in_specs=[smem(), smem()] + whole(1 + len(operands)),
        out_specs=whole(1)[0],
        scratch_shapes=[
            pltpu.VMEM((REACH + 2, ext, columns), f32),
            pltpu.VMEM((REACH, ext, columns), f32),
        ],
        compiler_params=params(24),
        cost_estimate=cost(300_000_000),
        name="first_edge",
    )(flags, order, plane, *operands)


def half_shape(split, columns):
    pairs, owner_tiles = split
    return pairs // 2, 4, owner_tiles * 8, columns


def call_last_edge(scale, split, flags, order, plane, *operands):
    _, ext, columns = plane.shape
    f32 = jnp.float32
    rows = ext - 2 * PAD
    images = 2 * [half_shape(split, columns)] if split else [(4, rows, columns)]
    shapes = [*images, (REACH + 2, ext, columns)]
    return pl.pallas_call(
        functools.partial(last_edge_kernel, scale, split),
        out_shape=tuple(jax.ShapeDtypeStruct(shape, f32) for shape in shapes),
        in_specs=[smem(), smem()] + whole(2) + [in_hbm()] + whole(len(operands) - 2),
        out_specs=tuple(whole(len(shapes))),
        scratch_shapes=[
            pltpu.VMEM((REACH, ext, columns), f32),
            pltpu.VMEM(operands[1].shape, operands[1].dtype),
            pltpu.SemaphoreType.DMA((1,)),
        ],
        compiler_params=params(12),
        cost_estimate=cost(300_000_000),
        name="last_edge",
    )(flags, order, plane, *operands)


def call_kept_edge(scale, split, half, order, ends, behind):
    image = jax.ShapeDtypeStruct(half_shape(split, ends.shape[2]), jnp.float32)
    return pl.pallas_call(
        functools.partial(kept_edge_kernel, scale, split, half),
        out_shape=image,
        in_specs=[smem()] + whole(2),
        out_specs=whole(1)[0],
        compiler_params=params(12),
        cost_estimate=cost(200_000_000),
    )(order, ends, behind)


def swap(value, axis, first):
    count = lax.axis_size(axis)
    pairs = []
    for low in range(first, count - 1, 2):
        pairs += [(low, low + 1), (low + 1, low)]
    return lax.ppermute(value, axis, pairs)


def over(front, back):
    through = front[:, 3:]
    return jnp.concatenate([front[:, :3] + through * back[:, :3], through * back[:, 3:]], 1)


def halves_of(layers):
    count = lax.axis_size("depth")
    me = lax.axis_index("depth")
    parity, pair, pairs = me % 2, me // 2, count // 2
    _, rows, columns = layers.shape
    pieces = layers.reshape(4, pairs, 2, rows // count, columns)
    ordered = jnp.concatenate(
        [lax.dynamic_slice_in_dim(pieces, pair ^ step, 1, 1) for step in reversed(range(pairs))], 1
    )
    both = []
    for wanted in (1 - parity, parity):
        chosen = lax.dynamic_index_in_dim(ordered, wanted, 2, keepdims=False)
        chosen = jnp.moveaxis(chosen, 1, 0)
        both.append((chosen[: pairs // 2], chosen[pairs // 2 :]))
    return both


def exchange(sends, keeps):
    count = lax.axis_size("depth")
    me = lax.axis_index("depth")
    parity, pair = me % 2, me // 2
    pairs = count // 2
    parts = [None] * pairs
    for half, (send, keep) in enumerate(zip(sends, keeps)):
        owned, columns = send.shape[2:]
        got = swap(send, "depth", 0)
        joined = jnp.where(parity == 0, over(keep, got), over(got, keep))
        for place in range(pairs // 2):
            step = pairs - 1 - half * (pairs // 2) - place
            piece = joined[place]
            if step:
                piece = lax.ppermute(piece, "depth", [(i, i ^ (2 * step)) for i in range(count)])
            parts[step] = piece
    result = jnp.zeros((3, owned, columns), jnp.float32)
    through = jnp.ones((1, owned, columns), jnp.float32)
    for step in range(pairs):
        ahead = jnp.ones((1, owned, columns), jnp.float32)
        for other in range(pairs):
            if other != step:
                nearer = (pair ^ other) < (pair ^ step)
                ahead = ahead * jnp.where(nearer, parts[other][3:], 1.0)
        result = result + ahead * parts[step][:3]
        through = through * parts[step][3:]
    total, tilted, green = 0.225 * result[:1], 0.225 * result[1:2], 0.45 * result[2:]
    return jnp.concatenate([total + tilted, green, total - tilted, 1.0 - through], 0)


def local(counts):
    slab, rows, columns = counts.shape
    img, depth = lax.axis_index("img"), lax.axis_index("depth")
    imgs, depths = lax.axis_size("img"), lax.axis_size("depth")
    scale = 1.5 / (slab * depths)
    row_odd, depth_odd = img % 2, depth % 2
    first_a, first_b = (1 - depth_odd) * (slab - REACH), depth_odd * (slab - REACH)
    row_a, row_b = (1 - row_odd) * (rows - PAD), row_odd * (rows - PAD)
    where = jnp.stack([first_a, first_b, row_a, row_b])
    order = jnp.stack([1 - row_odd, depth_odd, depth // 2])
    one = jnp.float32(1.0)
    flags = jnp.stack(
        [(img > 0) * one, (img < imgs - 1) * one, (depth > 0) * one, (depth < depths - 1) * one]
    )
    by = jnp.asarray(column_matrices(columns))
    lx = jnp.asarray(row_matrices(rows))
    held = pltpu.with_memory_space_constraint(counts, pltpu.HBM)
    block_b = call_pack_block(where, held)
    side_b, edge_a, mid_a, side_a = call_pack_rest(where, held)
    block_b = swap(block_b, "depth", 1)
    xb = swap(side_b, "img", 1)
    edge_a = swap(edge_a, "depth", 0)
    mid_a = swap(mid_a, "depth", 0)
    xa = swap(side_a, "img", 0)

    def corner(far):
        of_a = lax.dynamic_slice_in_dim(edge_a, far * PAD, PAD, 1)
        of_b = lax.dynamic_slice_in_dim(block_b, far * (rows - PAD), PAD, 1)
        return jnp.concatenate([of_a, of_b], 0)

    ca = swap(corner(1 - row_odd), "img", 0)
    cb = swap(corner(row_odd), "img", 1)
    partial = call_smooth(held, by, jnp.asarray(own_matrix(rows)))
    plane, smoothed = call_depth(
        flags, order, partial, xa, xb, by, jnp.asarray(side_matrices(rows))
    )
    inner = call_interior(scale, smoothed)
    owned = rows // depths
    split = (depths // 2, owned // 8) if owned % 8 == 0 else None
    common = (flags, order, plane, smoothed)
    layers = call_first_edge(
        scale, *common, block_b, ca[REACH:], cb[REACH:], by, lx, inner
    )
    mid_a = pltpu.with_memory_space_constraint(mid_a, pltpu.HBM)
    *sends, ends = call_last_edge(
        scale, split, *common, mid_a, edge_a, ca[:REACH], cb[:REACH], by, lx, layers
    )
    if split:
        keeps = [call_kept_edge(scale, split, half, order, ends, layers) for half in range(2)]
    else:
        sends, keeps = halves_of(sends[0])
    return exchange(sends, keeps)


def solution(mesh):
    in_specs = (P("depth", "img", None),)
    out_specs = P(None, ("img", "depth"), None)
    return jax.shard_map(local, mesh=mesh, in_specs=in_specs, out_specs=out_specs, check_vma=False)
```

```python
import functools
import math

import jax
import jax.numpy as jnp
import numpy as np
from jax import lax
from jax.experimental import pallas as pl
from jax.experimental.pallas import tpu as pltpu
from jax.sharding import PartitionSpec as P


gauss_taps = [
    math.exp(-offset * offset / 8.0)
    / sum((math.exp(-other * other / 8.0) for other in range(-4, 5)))
    for offset in range(-4, 5)
]
light_z = 0.48
light_x = 0.6
light_y = 0.64


REACH = 5
SIDE_GROUP = 4
PAD = 8


def band(size):
    index = np.arange(size)
    apart = np.abs(index[:, None] - index[None, :])
    taps = np.array(gauss_taps[4:] + [0.0], np.float64)
    return taps[np.minimum(apart, 5)]


def split_terms(matrix):
    high = matrix.astype(jnp.bfloat16)
    low = (matrix - high.astype(np.float64)).astype(jnp.bfloat16)
    return high, low


def column_matrices(columns):
    return np.concatenate(split_terms(band(columns)), 0)


def row_terms(matrix):
    high, low = split_terms(matrix)
    return np.concatenate([high, high, low], 1)


def row_orders(rows):
    full = band(rows + 2 * PAD)
    order = np.arange(rows + 2 * PAD)
    swapped = np.concatenate([order[rows + PAD :], order[PAD : rows + PAD], order[:PAD]])
    return [full[:, order], full[:, swapped]]


def row_matrices(rows):
    return np.stack([row_terms(matrix) for matrix in row_orders(rows)])


def own_matrix(rows):
    return row_terms(band(rows + 2 * PAD)[:, PAD : rows + PAD])


def side_matrices(rows):
    both = []
    for matrix in row_orders(rows):
        sides = np.concatenate([matrix[:, :PAD], matrix[:, rows + PAD :]], 1)
        touched = np.concatenate([sides[: 2 * PAD], sides[rows:]], 0)
        both.append(row_terms(np.kron(np.eye(SIDE_GROUP), touched)))
    return np.stack(both)


def two_terms(value, high, low):
    return jnp.dot(value, high, preferred_element_type=jnp.float32) + jnp.dot(
        value, low, preferred_element_type=jnp.float32
    )


def smooth_columns(exact, by):
    half = by.shape[0] // 2
    return two_terms(exact, by[:half], by[half:])


def column_terms(counts, by):
    exact = jnp.concatenate([c.astype(jnp.float32).astype(jnp.bfloat16) for c in counts], 0)
    wide = smooth_columns(exact, by)
    high = wide.astype(jnp.bfloat16)
    return high, (wide - high.astype(jnp.float32)).astype(jnp.bfloat16)


def row_product(matrix, high, low):
    stacked = jnp.concatenate([high, low, high], 0)
    return jnp.dot(matrix, stacked, preferred_element_type=jnp.float32)


def smooth_plane(counts, by, lx):
    rows = counts[0].shape[0]
    high, low = column_terms(counts, by)
    parts = [slice(n * rows, (n + 1) * rows) for n in range(len(counts))]
    return [row_product(lx, high[part], low[part]) for part in parts]


def smooth_depth(read, k):
    total = gauss_taps[4] * read(k)
    for offset in range(1, 5):
        total = total + gauss_taps[4 + offset] * (read(k - offset) + read(k + offset))
    return total


def smooth_depth_layer(flags, read, k, tiles, write):
    for tile in range(tiles):
        rows = pl.ds(tile * 8, 8)
        value = smooth_depth(lambda j: read(j, rows), k)
        if tile == 0:
            value = value * flags[0]
        if tile == tiles - 1:
            value = value * flags[1]
        write(rows, value)


def beside(mid, step):
    lanes = 128
    lane = lax.broadcasted_iota(jnp.int32, (mid.shape[0], lanes), 1)
    parts = [mid[:, at : at + lanes] for at in range(0, mid.shape[1], lanes)]
    turned = [pltpu.roll(part, lanes - 1 if step == 1 else 1, 1) for part in parts]
    zero = jnp.zeros_like(parts[0])
    if step == 1:
        return jnp.concatenate(
            [jnp.where(lane == lanes - 1, y, x) for x, y in zip(turned, turned[1:] + [zero])], 1
        )
    return jnp.concatenate(
        [jnp.where(lane == 0, y, x) for x, y in zip(turned, [zero] + turned[:-1])], 1
    )


def render_layer(layer, k, base, carry, scale):
    total, tilted, green, transmit = carry
    rows = pl.ds(base, 8)
    mid = layer(k, rows)
    before = layer(k, pl.ds(base - 8, 8))
    after = layer(k, pl.ds(base + 8, 8))
    sub = lax.broadcasted_iota(jnp.int32, mid.shape, 0)
    above = pltpu.roll(jnp.where(sub == 7, before, mid), 1, 0)
    below = pltpu.roll(jnp.where(sub == 0, after, mid), 7, 0)
    dz = layer(k + 1, rows) - layer(k - 1, rows)
    dx = below - above
    dy = beside(mid, 1) - beside(mid, -1)
    slope = (1.5 * light_z) * dz + (1.5 * light_x) * dx + (1.5 * light_y) * dy
    shading = jnp.tanh(slope) + (0.55 / 0.45)
    gradient_sq4 = dz * dz + dx * dx + dy * dy
    square = mid * mid
    optical = (square / (1.0 + square)) * (1.0 + gradient_sq4)
    centred = mid - 2.5
    log2e = math.log2(math.e)
    remaining = transmit * jnp.exp2(optical * (-scale * log2e))
    lit = (transmit - remaining) * shading
    return (
        total + lit,
        tilted + lit * jnp.tanh(centred),
        green + lit * jnp.exp2((centred * -log2e) * centred),
        remaining,
    )


def empty_carry(columns):
    zero = jnp.zeros((8, columns), jnp.float32)
    return zero, zero, zero, jnp.ones_like(zero)


def read_tile(ref, tile):
    rows = pl.ds(pl.multiple_of(tile * 8, 8), 8)
    return tuple(ref[n, rows, :] for n in range(4))


def store_tile(ref, tile, values):
    rows = pl.ds(pl.multiple_of(tile * 8, 8), 8)
    for n, value in enumerate(values):
        ref[n, rows, :] = value


def run_copies(copies):
    for copy in copies:
        copy.start()
    for copy in copies:
        copy.wait()


def run_copies(pairs, sems):
    copies = [pltpu.make_async_copy(*pair, sems.at[n]) for n, pair in enumerate(pairs)]
    for copy in copies:
        copy.start()
    for copy in copies:
        copy.wait()


def pack_block_kernel(where, c, block, sems):
    half = block.shape[1] // 2
    layers = pl.ds(where[1], REACH)
    parts = [pl.ds(n * half, half) for n in range(2)]
    run_copies([(c.at[layers, part], block.at[:, part]) for part in parts], sems)


def pack_rest_kernel(where, c, side_b, edge, middle, side_a, sems):
    rows = c.shape[1]
    layers = pl.ds(where[0], REACH)
    pairs = [
        (c.at[:, pl.ds(pl.multiple_of(where[2 + n], PAD), PAD)], side)
        for n, side in enumerate((side_a, side_b))
    ]
    pairs.append((c.at[layers, pl.ds(0, PAD)], edge.at[:, pl.ds(0, PAD)]))
    pairs.append((c.at[layers, pl.ds(rows - PAD, PAD)], edge.at[:, pl.ds(PAD, PAD)]))
    pairs.append((c.at[layers, pl.ds(PAD, rows - 2 * PAD)], middle))
    run_copies(pairs, sems)


def smooth_kernel(group, c_hbm, by, lx, plane, c, sems):
    groups = c.shape[0] // group

    def fetch(g):
        part = pl.ds(g * group, group)
        return pltpu.make_async_copy(c_hbm.at[part], c.at[part], sems.at[g])

    for g in range(groups):
        fetch(g).start()

    def smooth_group(g, _):
        first = g * group
        fetch(g).wait()
        counts = [c[first + n] for n in range(group)]
        for n, value in enumerate(smooth_plane(counts, by, lx[...])):
            plane[first + n] = value
        return 0

    lax.fori_loop(0, groups, smooth_group, 0)


def depth_kernel(flags, order, partial, xa, xb, by, lx, plane, smoothed):
    layers, ext, _ = plane.shape
    group = 4 * SIDE_GROUP
    edge = 2 * PAD
    sides = lx[order[0]]

    def add_sides(g, _):
        first = g * group
        counts = [jnp.concatenate([xa[first + n], xb[first + n]], 0) for n in range(group)]
        high, low = column_terms(counts, by)
        for half in range(4):
            part = slice(half * SIDE_GROUP * edge, (half + 1) * SIDE_GROUP * edge)
            added = row_product(sides, high[part], low[part])
            for n in range(SIDE_GROUP):
                k = first + half * SIDE_GROUP + n
                at = n * 2 * edge
                plane[k, :edge, :] = partial[k, :edge, :] + added[at : at + edge]
                plane[k, ext - edge :, :] = (
                    partial[k, ext - edge :, :] + added[at + edge : at + 2 * edge]
                )
        return 0

    lax.fori_loop(0, layers // group, add_sides, 0)

    def one_layer(j, _):
        def write(rows, value):
            smoothed[j, rows, :] = value

        smooth_depth_layer(flags, lambda k, rows: plane[k, rows, :], j + 4, ext // 8, write)
        return 0

    lax.fori_loop(0, layers - 8, one_layer, 0)


def interior_kernel(scale, smoothed, image):
    held, ext, columns = smoothed.shape

    def one_tile(tile, _):
        base = pl.multiple_of(tile * 8 + 8, 8)
        carry = empty_carry(columns)
        for k in range(1, held - 1):
            carry = render_layer(lambda k, rows: smoothed[k, rows, :], k, base, carry, scale)
        store_tile(image, tile, carry)
        return 0

    lax.fori_loop(0, ext // 8 - 2, one_tile, 0)


def edge_smooth(turn, flags, order, plane, smoothed, tile, ca, cb, by, lx, ends, halo):
    layers, ext, _ = plane.shape
    rows_of = order[0]
    is_front = order[1] == 1 - turn
    sign = jnp.where(is_front, 1, -1)
    counts = [jnp.concatenate([ca[j], tile(j), cb[j]], 0) for j in range(REACH)]
    for j, value in enumerate(smooth_plane(counts, by, lx[rows_of])):
        halo[j] = value
    plane_face = jnp.where(is_front, 0, layers - 1)
    halo_face = jnp.where(is_front, REACH, -1)
    ends_face = jnp.where(is_front, 1, REACH)
    smoothed_face = jnp.where(is_front, -4, layers - 5)
    on_grid = jnp.where(is_front, flags[2], flags[3])

    def counted(v, rows):
        if v < 0:
            return halo[halo_face + sign * v, rows, :]
        return plane[plane_face + sign * v, rows, :]

    for v in range(-1, 4):

        def write(rows, value, v=v):
            ends[ends_face + sign * v, rows, :] = value * on_grid if v < 0 else value

        smooth_depth_layer(flags, counted, v, ext // 8, write)
    for v in (4, 5):
        ends[ends_face + sign * v] = smoothed[smoothed_face + sign * v]


def edge_render(scale, is_front, ends, behind, image, tiles, tile_of, first=0):
    columns = ends.shape[2]

    def one_tile(place, _):
        tile = tile_of(place + first)
        base = pl.multiple_of(tile * 8 + 8, 8)
        carry = empty_carry(columns)
        for k in range(1, REACH + 1):
            carry = render_layer(lambda k, rows: ends[k, rows, :], k, base, carry, scale)
        other = read_tile(behind, tile)
        front = [jnp.where(is_front, x, y) for x, y in zip(carry, other)]
        back = [jnp.where(is_front, y, x) for x, y in zip(carry, other)]
        colors = [front[n] + front[3] * back[n] for n in range(3)]
        colors.append(front[3] * back[3])
        if len(image.shape) == 3:
            store_tile(image, place, colors)
        else:
            owner_tiles = image.shape[2] // 8
            store_tile(image.at[place // owner_tiles], place % owner_tiles, colors)
        return 0

    lax.fori_loop(0, tiles, one_tile, 0)


def half_tiles(order, pairs, owner_tiles, wanted):
    def tile_of(place):
        pair = order[2] ^ (pairs - 1 - place // owner_tiles)
        return (2 * pair + wanted) * owner_tiles + place % owner_tiles

    return tile_of


def first_edge_kernel(scale, flags, order, plane, smoothed, block, ca, cb, by, lx, behind, image,
                      ends, halo):
    tile = lambda j: block[j]
    edge_smooth(1, flags, order, plane, smoothed, tile, ca, cb, by, lx, ends, halo)
    tiles = plane.shape[1] // 8 - 2
    edge_render(scale, order[1] == 0, ends, behind, image, tiles, lambda place: place)


def render_half(scale, is_front, ends, behind, image, tile_of, half):
    places, _, owned, _ = image.shape
    tiles = places * (owned // 8)
    edge_render(scale, is_front, ends, behind, image, tiles, tile_of, half * tiles)


def last_edge_kernel(scale, split, flags, order, plane, smoothed, middle_any, edge, ca, cb,
                     by, lx, behind, *refs):
    images, (ends, halo, middle, sem) = refs[:-4], refs[-4:]
    run_copies([(middle_any, middle)], sem)
    tile = lambda j: jnp.concatenate([edge[j, :PAD], middle[j], edge[j, PAD:]], 0)
    edge_smooth(0, flags, order, plane, smoothed, tile, ca, cb, by, lx, ends, halo)
    if split:
        tile_of = half_tiles(order, *split, 1 - order[1])
        render_half(scale, order[1] == 1, ends, behind, images[0], tile_of, 0)
    else:
        tiles = plane.shape[1] // 8 - 2
        edge_render(scale, order[1] == 1, ends, behind, images[0], tiles, lambda place: place)


def part_edge_kernel(scale, split, half, kept, order, ends, behind, image):
    tile_of = half_tiles(order, *split, order[1] if kept else 1 - order[1])
    render_half(scale, order[1] == 1, ends, behind, image, tile_of, half)


def whole(count):
    return [pl.BlockSpec(memory_space=pltpu.VMEM)] * count


def smem():
    return pl.BlockSpec(memory_space=pltpu.SMEM)


def in_hbm():
    return pl.BlockSpec(memory_space=pltpu.HBM)


def params(mib):
    return pltpu.CompilerParams(vmem_limit_bytes=mib * 1024 * 1024)


def cost(flops):
    return pl.CostEstimate(flops=flops, transcendentals=0, bytes_accessed=4_000_000)


def call_pack_block(where, c):
    _, rows, columns = c.shape
    return pl.pallas_call(
        pack_block_kernel,
        out_shape=jax.ShapeDtypeStruct((REACH, rows, columns), c.dtype),
        in_specs=[smem(), in_hbm()],
        out_specs=whole(1)[0],
        scratch_shapes=[pltpu.SemaphoreType.DMA((2,))],
        compiler_params=params(8),
        name="pack_block",
    )(where, c)


def call_pack_rest(where, c):
    layers, rows, columns = c.shape
    edge = jax.ShapeDtypeStruct((REACH, 2 * PAD, columns), c.dtype)
    side = jax.ShapeDtypeStruct((layers, PAD, columns), c.dtype)
    middle = jax.ShapeDtypeStruct((REACH, rows - 2 * PAD, columns), c.dtype)
    return pl.pallas_call(
        pack_rest_kernel,
        out_shape=(side, edge, middle, side),
        in_specs=[smem(), in_hbm()],
        out_specs=tuple(whole(4)),
        scratch_shapes=[pltpu.SemaphoreType.DMA((5,))],
        compiler_params=params(8),
        name="pack_rest",
    )(where, c)


def call_smooth(c, by, lx):
    layers, rows, columns = c.shape
    ext = rows + 2 * PAD
    group = 8
    return pl.pallas_call(
        functools.partial(smooth_kernel, group),
        out_shape=jax.ShapeDtypeStruct((layers, ext, columns), jnp.float32),
        in_specs=[in_hbm()] + whole(2),
        out_specs=whole(1)[0],
        scratch_shapes=[
            pltpu.VMEM((layers, rows, columns), jnp.int32),
            pltpu.SemaphoreType.DMA((layers // group,)),
        ],
        compiler_params=params(16),
        cost_estimate=cost(1_000_000_000),
        name="smooth",
    )(c, by, lx)


def call_depth(flags, order, partial, *operands):
    layers, ext, columns = partial.shape
    return pl.pallas_call(
        depth_kernel,
        out_shape=(
            jax.ShapeDtypeStruct(partial.shape, jnp.float32),
            jax.ShapeDtypeStruct((layers - 8, ext, columns), jnp.float32),
        ),
        in_specs=[smem(), smem()] + whole(1 + len(operands)),
        out_specs=tuple(whole(2)),
        input_output_aliases={2: 0},
        compiler_params=params(12),
        cost_estimate=cost(500_000_000),
        name="depth",
    )(flags, order, partial, *operands)


def call_interior(scale, smoothed):
    _, ext, columns = smoothed.shape
    return pl.pallas_call(
        functools.partial(interior_kernel, scale),
        out_shape=jax.ShapeDtypeStruct((4, ext - 2 * PAD, columns), jnp.float32),
        in_specs=whole(1),
        out_specs=whole(1)[0],
        compiler_params=params(12),
        cost_estimate=cost(1_000_000_000),
        name="interior",
    )(smoothed)


def call_first_edge(scale, flags, order, plane, *operands):
    _, ext, columns = plane.shape
    f32 = jnp.float32
    return pl.pallas_call(
        functools.partial(first_edge_kernel, scale),
        out_shape=jax.ShapeDtypeStruct((4, ext - 2 * PAD, columns), f32),
        in_specs=[smem(), smem()] + whole(1 + len(operands)),
        out_specs=whole(1)[0],
        scratch_shapes=[
            pltpu.VMEM((REACH + 2, ext, columns), f32),
            pltpu.VMEM((REACH, ext, columns), f32),
        ],
        compiler_params=params(24),
        cost_estimate=cost(300_000_000),
        name="first_edge",
    )(flags, order, plane, *operands)


def half_shape(split, columns):
    pairs, owner_tiles = split
    return pairs // 2, 4, owner_tiles * 8, columns


def call_last_edge(scale, split, flags, order, plane, *operands):
    _, ext, columns = plane.shape
    f32 = jnp.float32
    rows = ext - 2 * PAD
    images = [half_shape(split, columns) if split else (4, rows, columns)]
    shapes = [*images, (REACH + 2, ext, columns)]
    return pl.pallas_call(
        functools.partial(last_edge_kernel, scale, split),
        out_shape=tuple(jax.ShapeDtypeStruct(shape, f32) for shape in shapes),
        in_specs=[smem(), smem()] + whole(2) + [in_hbm()] + whole(len(operands) - 2),
        out_specs=tuple(whole(len(shapes))),
        scratch_shapes=[
            pltpu.VMEM((REACH, ext, columns), f32),
            pltpu.VMEM(operands[1].shape, operands[1].dtype),
            pltpu.SemaphoreType.DMA((1,)),
        ],
        compiler_params=params(12),
        cost_estimate=cost(300_000_000),
        name="last_edge",
    )(flags, order, plane, *operands)


def call_part_edge(scale, split, half, kept, order, ends, behind):
    image = jax.ShapeDtypeStruct(half_shape(split, ends.shape[2]), jnp.float32)
    return pl.pallas_call(
        functools.partial(part_edge_kernel, scale, split, half, kept),
        out_shape=image,
        in_specs=[smem()] + whole(2),
        out_specs=whole(1)[0],
        compiler_params=params(12),
        cost_estimate=cost(200_000_000),
    )(order, ends, behind)


def swap(value, axis, first):
    count = lax.axis_size(axis)
    pairs = []
    for low in range(first, count - 1, 2):
        pairs += [(low, low + 1), (low + 1, low)]
    return lax.ppermute(value, axis, pairs)


def over(front, back):
    through = front[:, 3:]
    return jnp.concatenate([front[:, :3] + through * back[:, :3], through * back[:, 3:]], 1)


def halves_of(layers):
    count = lax.axis_size("depth")
    me = lax.axis_index("depth")
    parity, pair, pairs = me % 2, me // 2, count // 2
    _, rows, columns = layers.shape
    pieces = layers.reshape(4, pairs, 2, rows // count, columns)
    ordered = jnp.concatenate(
        [lax.dynamic_slice_in_dim(pieces, pair ^ step, 1, 1) for step in reversed(range(pairs))], 1
    )
    both = []
    for wanted in (1 - parity, parity):
        chosen = lax.dynamic_index_in_dim(ordered, wanted, 2, keepdims=False)
        chosen = jnp.moveaxis(chosen, 1, 0)
        both.append((chosen[: pairs // 2], chosen[pairs // 2 :]))
    return both


def exchange(sends, keeps):
    count = lax.axis_size("depth")
    me = lax.axis_index("depth")
    parity, pair = me % 2, me // 2
    pairs = count // 2
    parts = [None] * pairs
    for half, (send, keep) in enumerate(zip(sends, keeps)):
        owned, columns = send.shape[2:]
        got = swap(send, "depth", 0)
        joined = jnp.where(parity == 0, over(keep, got), over(got, keep))
        for place in range(pairs // 2):
            step = pairs - 1 - half * (pairs // 2) - place
            piece = joined[place]
            if step:
                piece = lax.ppermute(piece, "depth", [(i, i ^ (2 * step)) for i in range(count)])
            parts[step] = piece
    result = jnp.zeros((3, owned, columns), jnp.float32)
    through = jnp.ones((1, owned, columns), jnp.float32)
    for step in range(pairs):
        ahead = jnp.ones((1, owned, columns), jnp.float32)
        for other in range(pairs):
            if other != step:
                nearer = (pair ^ other) < (pair ^ step)
                ahead = ahead * jnp.where(nearer, parts[other][3:], 1.0)
        result = result + ahead * parts[step][:3]
        through = through * parts[step][3:]
    total, tilted, green = 0.225 * result[:1], 0.225 * result[1:2], 0.45 * result[2:]
    return jnp.concatenate([total + tilted, green, total - tilted, 1.0 - through], 0)


def local(counts):
    slab, rows, columns = counts.shape
    img, depth = lax.axis_index("img"), lax.axis_index("depth")
    imgs, depths = lax.axis_size("img"), lax.axis_size("depth")
    scale = 1.5 / (slab * depths)
    row_odd, depth_odd = img % 2, depth % 2
    first_a, first_b = (1 - depth_odd) * (slab - REACH), depth_odd * (slab - REACH)
    row_a, row_b = (1 - row_odd) * (rows - PAD), row_odd * (rows - PAD)
    where = jnp.stack([first_a, first_b, row_a, row_b])
    order = jnp.stack([1 - row_odd, depth_odd, depth // 2])
    one = jnp.float32(1.0)
    flags = jnp.stack(
        [(img > 0) * one, (img < imgs - 1) * one, (depth > 0) * one, (depth < depths - 1) * one]
    )
    by = jnp.asarray(column_matrices(columns))
    lx = jnp.asarray(row_matrices(rows))
    held = pltpu.with_memory_space_constraint(counts, pltpu.HBM)
    block_b = call_pack_block(where, held)
    side_b, edge_a, mid_a, side_a = call_pack_rest(where, held)
    block_b = swap(block_b, "depth", 1)
    xb = swap(side_b, "img", 1)
    edge_a = swap(edge_a, "depth", 0)
    mid_a = swap(mid_a, "depth", 0)
    xa = swap(side_a, "img", 0)

    def corner(far):
        of_a = lax.dynamic_slice_in_dim(edge_a, far * PAD, PAD, 1)
        of_b = lax.dynamic_slice_in_dim(block_b, far * (rows - PAD), PAD, 1)
        return jnp.concatenate([of_a, of_b], 0)

    ca = swap(corner(1 - row_odd), "img", 0)
    cb = swap(corner(row_odd), "img", 1)
    partial = call_smooth(held, by, jnp.asarray(own_matrix(rows)))
    plane, smoothed = call_depth(
        flags, order, partial, xa, xb, by, jnp.asarray(side_matrices(rows))
    )
    inner = call_interior(scale, smoothed)
    owned = rows // depths
    split = (depths // 2, owned // 8) if owned % 8 == 0 else None
    common = (flags, order, plane, smoothed)
    layers = call_first_edge(
        scale, *common, block_b, ca[REACH:], cb[REACH:], by, lx, inner
    )
    mid_a = pltpu.with_memory_space_constraint(mid_a, pltpu.HBM)
    *sends, ends = call_last_edge(
        scale, split, *common, mid_a, edge_a, ca[:REACH], cb[:REACH], by, lx, layers
    )
    if split:
        last = (order, ends, layers)
        sends.append(call_part_edge(scale, split, 1, False, *last))
        keeps = [call_part_edge(scale, split, half, True, *last) for half in range(2)]
    else:
        sends, keeps = halves_of(sends[0])
    return exchange(sends, keeps)


def solution(mesh):
    in_specs = (P("depth", "img", None),)
    out_specs = P(None, ("img", "depth"), None)
    return jax.shard_map(local, mesh=mesh, in_specs=in_specs, out_specs=out_specs, check_vma=False)
```

```python
import functools
import math

import jax
import jax.numpy as jnp
import numpy as np
from jax import lax
from jax.experimental import pallas as pl
from jax.experimental.pallas import tpu as pltpu
from jax.sharding import PartitionSpec as P


gauss_taps = [
    math.exp(-offset * offset / 8.0)
    / sum((math.exp(-other * other / 8.0) for other in range(-4, 5)))
    for offset in range(-4, 5)
]
light_z = 0.48
light_x = 0.6
light_y = 0.64


REACH = 5
SIDE_GROUP = 4
PAD = 8


def band(size):
    index = np.arange(size)
    apart = np.abs(index[:, None] - index[None, :])
    taps = np.array(gauss_taps[4:] + [0.0], np.float64)
    return taps[np.minimum(apart, 5)]


def split_terms(matrix):
    high = matrix.astype(jnp.bfloat16)
    low = (matrix - high.astype(np.float64)).astype(jnp.bfloat16)
    return high, low


def column_matrices(columns):
    return np.concatenate(split_terms(band(columns)), 0)


def row_terms(matrix):
    high, low = split_terms(matrix)
    return np.concatenate([high, high, low], 1)


def row_orders(rows):
    full = band(rows + 2 * PAD)
    order = np.arange(rows + 2 * PAD)
    swapped = np.concatenate([order[rows + PAD :], order[PAD : rows + PAD], order[:PAD]])
    return [full[:, order], full[:, swapped]]


def row_matrices(rows):
    return np.stack([row_terms(matrix) for matrix in row_orders(rows)])


def own_matrix(rows):
    return row_terms(band(rows + 2 * PAD)[:, PAD : rows + PAD])


def side_matrices(rows):
    both = []
    for matrix in row_orders(rows):
        sides = np.concatenate([matrix[:, :PAD], matrix[:, rows + PAD :]], 1)
        touched = np.concatenate([sides[: 2 * PAD], sides[rows:]], 0)
        both.append(row_terms(np.kron(np.eye(SIDE_GROUP), touched)))
    return np.stack(both)


def two_terms(value, high, low):
    return jnp.dot(value, high, preferred_element_type=jnp.float32) + jnp.dot(
        value, low, preferred_element_type=jnp.float32
    )


def smooth_columns(exact, by):
    half = by.shape[0] // 2
    return two_terms(exact, by[:half], by[half:])


def column_terms(counts, by):
    exact = jnp.concatenate([c.astype(jnp.float32).astype(jnp.bfloat16) for c in counts], 0)
    wide = smooth_columns(exact, by)
    high = wide.astype(jnp.bfloat16)
    return high, (wide - high.astype(jnp.float32)).astype(jnp.bfloat16)


def row_product(matrix, high, low):
    stacked = jnp.concatenate([high, low, high], 0)
    return jnp.dot(matrix, stacked, preferred_element_type=jnp.float32)


def smooth_plane(counts, by, lx):
    rows = counts[0].shape[0]
    high, low = column_terms(counts, by)
    parts = [slice(n * rows, (n + 1) * rows) for n in range(len(counts))]
    return [row_product(lx, high[part], low[part]) for part in parts]


def smooth_depth(read, k):
    total = gauss_taps[4] * read(k)
    for offset in range(1, 5):
        total = total + gauss_taps[4 + offset] * (read(k - offset) + read(k + offset))
    return total


def smooth_depth_layers(flags, read, ks, tiles, write):
    for tile in range(tiles):
        rows = pl.ds(tile * 8, 8)
        for n, k in enumerate(ks):
            value = smooth_depth(lambda j: read(j, rows), k)
            if tile == 0:
                value = value * flags[0]
            if tile == tiles - 1:
                value = value * flags[1]
            write(n, rows, value)


def beside(mid, step):
    lanes = 128
    lane = lax.broadcasted_iota(jnp.int32, (mid.shape[0], lanes), 1)
    parts = [mid[:, at : at + lanes] for at in range(0, mid.shape[1], lanes)]
    turned = [pltpu.roll(part, lanes - 1 if step == 1 else 1, 1) for part in parts]
    zero = jnp.zeros_like(parts[0])
    if step == 1:
        return jnp.concatenate(
            [jnp.where(lane == lanes - 1, y, x) for x, y in zip(turned, turned[1:] + [zero])], 1
        )
    return jnp.concatenate(
        [jnp.where(lane == 0, y, x) for x, y in zip(turned, [zero] + turned[:-1])], 1
    )


def render_layer(layer, k, base, carry, scale):
    total, tilted, green, transmit = carry
    rows = pl.ds(base, 8)
    mid = layer(k, rows)
    before = layer(k, pl.ds(base - 8, 8))
    after = layer(k, pl.ds(base + 8, 8))
    sub = lax.broadcasted_iota(jnp.int32, mid.shape, 0)
    above = pltpu.roll(jnp.where(sub == 7, before, mid), 1, 0)
    below = pltpu.roll(jnp.where(sub == 0, after, mid), 7, 0)
    dz = layer(k + 1, rows) - layer(k - 1, rows)
    dx = below - above
    dy = beside(mid, 1) - beside(mid, -1)
    slope = (1.5 * light_z) * dz + (1.5 * light_x) * dx + (1.5 * light_y) * dy
    shading = jnp.tanh(slope) + (0.55 / 0.45)
    gradient_sq4 = dz * dz + dx * dx + dy * dy
    square = mid * mid
    optical = (square / (1.0 + square)) * (1.0 + gradient_sq4)
    centred = mid - 2.5
    log2e = math.log2(math.e)
    remaining = transmit * jnp.exp2(optical * (-scale * log2e))
    lit = (transmit - remaining) * shading
    return (
        total + lit,
        tilted + lit * jnp.tanh(centred),
        green + lit * jnp.exp2((centred * -log2e) * centred),
        remaining,
    )


def empty_carry(columns):
    zero = jnp.zeros((8, columns), jnp.float32)
    return zero, zero, zero, jnp.ones_like(zero)


def read_tile(ref, tile):
    rows = pl.ds(pl.multiple_of(tile * 8, 8), 8)
    return tuple(ref[n, rows, :] for n in range(4))


def store_tile(ref, tile, values):
    rows = pl.ds(pl.multiple_of(tile * 8, 8), 8)
    for n, value in enumerate(values):
        ref[n, rows, :] = value


def run_copies(copies):
    for copy in copies:
        copy.start()
    for copy in copies:
        copy.wait()


def run_copies(pairs, sems):
    copies = [pltpu.make_async_copy(*pair, sems.at[n]) for n, pair in enumerate(pairs)]
    for copy in copies:
        copy.start()
    for copy in copies:
        copy.wait()


def pack_block_kernel(where, c, block, sems):
    half = block.shape[1] // 2
    layers = pl.ds(where[1], REACH)
    parts = [pl.ds(n * half, half) for n in range(2)]
    run_copies([(c.at[layers, part], block.at[:, part]) for part in parts], sems)


def pack_rest_kernel(where, c, side_b, edge, middle, side_a, sems):
    rows = c.shape[1]
    layers = pl.ds(where[0], REACH)
    pairs = [
        (c.at[:, pl.ds(pl.multiple_of(where[2 + n], PAD), PAD)], side)
        for n, side in enumerate((side_a, side_b))
    ]
    pairs.append((c.at[layers, pl.ds(0, PAD)], edge.at[:, pl.ds(0, PAD)]))
    pairs.append((c.at[layers, pl.ds(rows - PAD, PAD)], edge.at[:, pl.ds(PAD, PAD)]))
    pairs.append((c.at[layers, pl.ds(PAD, rows - 2 * PAD)], middle))
    run_copies(pairs, sems)


def smooth_kernel(group, c_hbm, by, lx, plane, c, sems):
    groups = c.shape[0] // group

    def fetch(g):
        part = pl.ds(g * group, group)
        return pltpu.make_async_copy(c_hbm.at[part], c.at[part], sems.at[g])

    for g in range(groups):
        fetch(g).start()

    def smooth_group(g, _):
        first = g * group
        fetch(g).wait()
        counts = [c[first + n] for n in range(group)]
        for n, value in enumerate(smooth_plane(counts, by, lx[...])):
            plane[first + n] = value
        return 0

    lax.fori_loop(0, groups, smooth_group, 0)


def depth_kernel(flags, order, partial, xa, xb, by, lx, plane, smoothed):
    layers, ext, _ = plane.shape
    group = 4 * SIDE_GROUP
    edge = 2 * PAD
    sides = lx[order[0]]

    def add_sides(g, _):
        first = g * group
        counts = [jnp.concatenate([xa[first + n], xb[first + n]], 0) for n in range(group)]
        high, low = column_terms(counts, by)
        for half in range(4):
            part = slice(half * SIDE_GROUP * edge, (half + 1) * SIDE_GROUP * edge)
            added = row_product(sides, high[part], low[part])
            for n in range(SIDE_GROUP):
                k = first + half * SIDE_GROUP + n
                at = n * 2 * edge
                plane[k, :edge, :] = partial[k, :edge, :] + added[at : at + edge]
                plane[k, ext - edge :, :] = (
                    partial[k, ext - edge :, :] + added[at + edge : at + 2 * edge]
                )
        return 0

    lax.fori_loop(0, layers // group, add_sides, 0)

    together = 2 if layers % 2 == 0 else 1

    def some_layers(m, _):
        first = m * together

        def write(n, rows, value):
            smoothed[first + n, rows, :] = value

        ks = [first + n + 4 for n in range(together)]
        smooth_depth_layers(flags, lambda k, rows: plane[k, rows, :], ks, ext // 8, write)
        return 0

    lax.fori_loop(0, (layers - 8) // together, some_layers, 0)


def interior_kernel(scale, smoothed, image):
    held, ext, columns = smoothed.shape

    def one_tile(tile, _):
        base = pl.multiple_of(tile * 8 + 8, 8)
        carry = empty_carry(columns)
        for k in range(1, held - 1):
            carry = render_layer(lambda k, rows: smoothed[k, rows, :], k, base, carry, scale)
        store_tile(image, tile, carry)
        return 0

    lax.fori_loop(0, ext // 8 - 2, one_tile, 0)


def edge_smooth(turn, flags, order, plane, smoothed, planes, ends, halo):
    layers, ext, _ = plane.shape
    is_front = order[1] == 1 - turn
    sign = jnp.where(is_front, 1, -1)
    for j, value in enumerate(planes):
        halo[j] = value
    plane_face = jnp.where(is_front, 0, layers - 1)
    halo_face = jnp.where(is_front, REACH, -1)
    ends_face = jnp.where(is_front, 1, REACH)
    smoothed_face = jnp.where(is_front, -4, layers - 5)
    on_grid = jnp.where(is_front, flags[2], flags[3])

    def counted(v, rows):
        if v < 0:
            return halo[halo_face + sign * v, rows, :]
        return plane[plane_face + sign * v, rows, :]

    def write(n, rows, value):
        ends[ends_face + sign * (n - 1), rows, :] = value * on_grid if n == 0 else value

    smooth_depth_layers(flags, counted, range(-1, 4), ext // 8, write)
    for v in (4, 5):
        ends[ends_face + sign * v] = smoothed[smoothed_face + sign * v]


def edge_render(scale, is_front, ends, behind, image, tiles, tile_of, first=0):
    columns = ends.shape[2]

    def one_tile(place):
        tile = tile_of(place + first)
        base = pl.multiple_of(tile * 8 + 8, 8)
        carry = empty_carry(columns)
        for k in range(1, REACH + 1):
            carry = render_layer(lambda k, rows: ends[k, rows, :], k, base, carry, scale)
        other = read_tile(behind, tile)
        front = [jnp.where(is_front, x, y) for x, y in zip(carry, other)]
        back = [jnp.where(is_front, y, x) for x, y in zip(carry, other)]
        colors = [front[n] + front[3] * back[n] for n in range(3)]
        colors.append(front[3] * back[3])
        if len(image.shape) == 3:
            store_tile(image, place, colors)
        else:
            owner_tiles = image.shape[2] // 8
            store_tile(image.at[place // owner_tiles], place % owner_tiles, colors)

    together = 2 if tiles % 2 == 0 else 1

    def some_tiles(n, _):
        for m in range(together):
            one_tile(n * together + m)
        return 0

    lax.fori_loop(0, tiles // together, some_tiles, 0)


def half_tiles(order, pairs, owner_tiles, wanted):
    def tile_of(place):
        pair = order[2] ^ (pairs - 1 - place // owner_tiles)
        return (2 * pair + wanted) * owner_tiles + place % owner_tiles

    return tile_of


def first_edge_kernel(scale, flags, order, plane, smoothed, block, ca, cb, by, lx, behind, image,
                      ends, halo):
    counts = [jnp.concatenate([ca[j], block[j], cb[j]], 0) for j in range(REACH)]
    planes = smooth_plane(counts, by, lx[order[0]])
    edge_smooth(1, flags, order, plane, smoothed, planes, ends, halo)
    tiles = plane.shape[1] // 8 - 2
    edge_render(scale, order[1] == 0, ends, behind, image, tiles, lambda place: place)


def render_half(scale, is_front, ends, behind, image, tile_of, half):
    places, _, owned, _ = image.shape
    tiles = places * (owned // 8)
    edge_render(scale, is_front, ends, behind, image, tiles, tile_of, half * tiles)


def last_edge_kernel(scale, split, flags, order, plane, smoothed, middle_any, edge, ca, cb,
                     by, lx, behind, *refs):
    images, (ends, halo, middle, sem) = refs[:-4], refs[-4:]
    fetch = pltpu.make_async_copy(middle_any, middle, sem.at[0])
    fetch.start()
    two = 2 * PAD
    outer = [
        jnp.concatenate([ca[j], edge[j, :PAD], edge[j, PAD:], cb[j]], 0) for j in range(REACH)
    ]
    outer = column_terms(outer, by)
    fetch.wait()
    inner = column_terms([middle[j] for j in range(REACH)], by)
    rows = middle.shape[1]
    planes = []
    for j in range(REACH):
        high, low = (
            jnp.concatenate(
                [
                    out[2 * two * j : 2 * two * j + two],
                    mid[rows * j : rows * (j + 1)],
                    out[2 * two * j + two : 2 * two * (j + 1)],
                ],
                0,
            )
            for out, mid in zip(outer, inner)
        )
        planes.append(row_product(lx[order[0]], high, low))
    edge_smooth(0, flags, order, plane, smoothed, planes, ends, halo)
    if split:
        tile_of = half_tiles(order, *split, 1 - order[1])
        render_half(scale, order[1] == 1, ends, behind, images[0], tile_of, 0)
    else:
        tiles = plane.shape[1] // 8 - 2
        edge_render(scale, order[1] == 1, ends, behind, images[0], tiles, lambda place: place)


def part_edge_kernel(scale, split, half, kept, order, ends, behind, image):
    tile_of = half_tiles(order, *split, order[1] if kept else 1 - order[1])
    render_half(scale, order[1] == 1, ends, behind, image, tile_of, half)


def whole(count):
    return [pl.BlockSpec(memory_space=pltpu.VMEM)] * count


def smem():
    return pl.BlockSpec(memory_space=pltpu.SMEM)


def in_hbm():
    return pl.BlockSpec(memory_space=pltpu.HBM)


def params(mib):
    return pltpu.CompilerParams(vmem_limit_bytes=mib * 1024 * 1024)


def cost(flops):
    return pl.CostEstimate(flops=flops, transcendentals=0, bytes_accessed=4_000_000)


def call_pack_block(where, c):
    _, rows, columns = c.shape
    return pl.pallas_call(
        pack_block_kernel,
        out_shape=jax.ShapeDtypeStruct((REACH, rows, columns), c.dtype),
        in_specs=[smem(), in_hbm()],
        out_specs=whole(1)[0],
        scratch_shapes=[pltpu.SemaphoreType.DMA((2,))],
        compiler_params=params(8),
        name="pack_block",
    )(where, c)


def call_pack_rest(where, c):
    layers, rows, columns = c.shape
    edge = jax.ShapeDtypeStruct((REACH, 2 * PAD, columns), c.dtype)
    side = jax.ShapeDtypeStruct((layers, PAD, columns), c.dtype)
    middle = jax.ShapeDtypeStruct((REACH, rows - 2 * PAD, columns), c.dtype)
    return pl.pallas_call(
        pack_rest_kernel,
        out_shape=(side, edge, middle, side),
        in_specs=[smem(), in_hbm()],
        out_specs=tuple(whole(4)),
        scratch_shapes=[pltpu.SemaphoreType.DMA((5,))],
        compiler_params=params(8),
        name="pack_rest",
    )(where, c)


def call_smooth(c, by, lx):
    layers, rows, columns = c.shape
    ext = rows + 2 * PAD
    group = 8
    return pl.pallas_call(
        functools.partial(smooth_kernel, group),
        out_shape=jax.ShapeDtypeStruct((layers, ext, columns), jnp.float32),
        in_specs=[in_hbm()] + whole(2),
        out_specs=whole(1)[0],
        scratch_shapes=[
            pltpu.VMEM((layers, rows, columns), jnp.int32),
            pltpu.SemaphoreType.DMA((layers // group,)),
        ],
        compiler_params=params(16),
        cost_estimate=cost(1_000_000_000),
        name="smooth",
    )(c, by, lx)


def call_depth(flags, order, partial, *operands):
    layers, ext, columns = partial.shape
    return pl.pallas_call(
        depth_kernel,
        out_shape=(
            jax.ShapeDtypeStruct(partial.shape, jnp.float32),
            jax.ShapeDtypeStruct((layers - 8, ext, columns), jnp.float32),
        ),
        in_specs=[smem(), smem()] + whole(1 + len(operands)),
        out_specs=tuple(whole(2)),
        input_output_aliases={2: 0},
        compiler_params=params(12),
        cost_estimate=cost(500_000_000),
        name="depth",
    )(flags, order, partial, *operands)


def call_interior(scale, smoothed):
    _, ext, columns = smoothed.shape
    return pl.pallas_call(
        functools.partial(interior_kernel, scale),
        out_shape=jax.ShapeDtypeStruct((4, ext - 2 * PAD, columns), jnp.float32),
        in_specs=whole(1),
        out_specs=whole(1)[0],
        compiler_params=params(12),
        cost_estimate=cost(1_000_000_000),
        name="interior",
    )(smoothed)


def call_first_edge(scale, flags, order, plane, *operands):
    _, ext, columns = plane.shape
    f32 = jnp.float32
    return pl.pallas_call(
        functools.partial(first_edge_kernel, scale),
        out_shape=jax.ShapeDtypeStruct((4, ext - 2 * PAD, columns), f32),
        in_specs=[smem(), smem()] + whole(1 + len(operands)),
        out_specs=whole(1)[0],
        scratch_shapes=[
            pltpu.VMEM((REACH + 2, ext, columns), f32),
            pltpu.VMEM((REACH, ext, columns), f32),
        ],
        compiler_params=params(24),
        cost_estimate=cost(300_000_000),
        name="first_edge",
    )(flags, order, plane, *operands)


def half_shape(split, columns):
    pairs, owner_tiles = split
    return pairs // 2, 4, owner_tiles * 8, columns


def call_last_edge(scale, split, flags, order, plane, *operands):
    _, ext, columns = plane.shape
    f32 = jnp.float32
    rows = ext - 2 * PAD
    images = [half_shape(split, columns) if split else (4, rows, columns)]
    shapes = [*images, (REACH + 2, ext, columns)]
    return pl.pallas_call(
        functools.partial(last_edge_kernel, scale, split),
        out_shape=tuple(jax.ShapeDtypeStruct(shape, f32) for shape in shapes),
        in_specs=[smem(), smem()] + whole(2) + [in_hbm()] + whole(len(operands) - 2),
        out_specs=tuple(whole(len(shapes))),
        scratch_shapes=[
            pltpu.VMEM((REACH, ext, columns), f32),
            pltpu.VMEM(operands[1].shape, operands[1].dtype),
            pltpu.SemaphoreType.DMA((1,)),
        ],
        compiler_params=params(12),
        cost_estimate=cost(300_000_000),
        name="last_edge",
    )(flags, order, plane, *operands)


def call_part_edge(scale, split, half, kept, order, ends, behind):
    image = jax.ShapeDtypeStruct(half_shape(split, ends.shape[2]), jnp.float32)
    return pl.pallas_call(
        functools.partial(part_edge_kernel, scale, split, half, kept),
        out_shape=image,
        in_specs=[smem()] + whole(2),
        out_specs=whole(1)[0],
        compiler_params=params(12),
        cost_estimate=cost(200_000_000),
    )(order, ends, behind)


def swap(value, axis, first):
    count = lax.axis_size(axis)
    pairs = []
    for low in range(first, count - 1, 2):
        pairs += [(low, low + 1), (low + 1, low)]
    return lax.ppermute(value, axis, pairs)


def over(front, back):
    through = front[:, 3:]
    return jnp.concatenate([front[:, :3] + through * back[:, :3], through * back[:, 3:]], 1)


def halves_of(layers):
    count = lax.axis_size("depth")
    me = lax.axis_index("depth")
    parity, pair, pairs = me % 2, me // 2, count // 2
    _, rows, columns = layers.shape
    pieces = layers.reshape(4, pairs, 2, rows // count, columns)
    ordered = jnp.concatenate(
        [lax.dynamic_slice_in_dim(pieces, pair ^ step, 1, 1) for step in reversed(range(pairs))], 1
    )
    both = []
    for wanted in (1 - parity, parity):
        chosen = lax.dynamic_index_in_dim(ordered, wanted, 2, keepdims=False)
        chosen = jnp.moveaxis(chosen, 1, 0)
        both.append((chosen[: pairs // 2], chosen[pairs // 2 :]))
    return both


def exchange(sends, keeps):
    count = lax.axis_size("depth")
    me = lax.axis_index("depth")
    parity, pair = me % 2, me // 2
    pairs = count // 2
    parts = [None] * pairs
    for half, (send, keep) in enumerate(zip(sends, keeps)):
        owned, columns = send.shape[2:]
        got = swap(send, "depth", 0)
        joined = jnp.where(parity == 0, over(keep, got), over(got, keep))
        for place in range(pairs // 2):
            step = pairs - 1 - half * (pairs // 2) - place
            piece = joined[place]
            if step:
                piece = lax.ppermute(piece, "depth", [(i, i ^ (2 * step)) for i in range(count)])
            parts[step] = piece
    result = jnp.zeros((3, owned, columns), jnp.float32)
    through = jnp.ones((1, owned, columns), jnp.float32)
    for step in range(pairs):
        ahead = jnp.ones((1, owned, columns), jnp.float32)
        for other in range(pairs):
            if other != step:
                nearer = (pair ^ other) < (pair ^ step)
                ahead = ahead * jnp.where(nearer, parts[other][3:], 1.0)
        result = result + ahead * parts[step][:3]
        through = through * parts[step][3:]
    total, tilted, green = 0.225 * result[:1], 0.225 * result[1:2], 0.45 * result[2:]
    return jnp.concatenate([total + tilted, green, total - tilted, 1.0 - through], 0)


def local(counts):
    slab, rows, columns = counts.shape
    img, depth = lax.axis_index("img"), lax.axis_index("depth")
    imgs, depths = lax.axis_size("img"), lax.axis_size("depth")
    scale = 1.5 / (slab * depths)
    row_odd, depth_odd = img % 2, depth % 2
    first_a, first_b = (1 - depth_odd) * (slab - REACH), depth_odd * (slab - REACH)
    row_a, row_b = (1 - row_odd) * (rows - PAD), row_odd * (rows - PAD)
    where = jnp.stack([first_a, first_b, row_a, row_b])
    order = jnp.stack([1 - row_odd, depth_odd, depth // 2])
    one = jnp.float32(1.0)
    flags = jnp.stack(
        [(img > 0) * one, (img < imgs - 1) * one, (depth > 0) * one, (depth < depths - 1) * one]
    )
    by = jnp.asarray(column_matrices(columns))
    lx = jnp.asarray(row_matrices(rows))
    held = pltpu.with_memory_space_constraint(counts, pltpu.HBM)
    block_b = call_pack_block(where, held)
    side_b, edge_a, mid_a, side_a = call_pack_rest(where, held)
    block_b = swap(block_b, "depth", 1)
    xb = swap(side_b, "img", 1)
    edge_a = swap(edge_a, "depth", 0)
    mid_a = swap(mid_a, "depth", 0)
    xa = swap(side_a, "img", 0)

    def corner(far):
        of_a = lax.dynamic_slice_in_dim(edge_a, far * PAD, PAD, 1)
        of_b = lax.dynamic_slice_in_dim(block_b, far * (rows - PAD), PAD, 1)
        return jnp.concatenate([of_a, of_b], 0)

    ca = swap(corner(1 - row_odd), "img", 0)
    cb = swap(corner(row_odd), "img", 1)
    partial = call_smooth(held, by, jnp.asarray(own_matrix(rows)))
    plane, smoothed = call_depth(
        flags, order, partial, xa, xb, by, jnp.asarray(side_matrices(rows))
    )
    inner = call_interior(scale, smoothed)
    owned = rows // depths
    split = (depths // 2, owned // 8) if owned % 8 == 0 else None
    common = (flags, order, plane, smoothed)
    layers = call_first_edge(
        scale, *common, block_b, ca[REACH:], cb[REACH:], by, lx, inner
    )
    mid_a = pltpu.with_memory_space_constraint(mid_a, pltpu.HBM)
    *sends, ends = call_last_edge(
        scale, split, *common, mid_a, edge_a, ca[:REACH], cb[:REACH], by, lx, layers
    )
    if split:
        last = (order, ends, layers)
        sends.append(call_part_edge(scale, split, 1, False, *last))
        keeps = [call_part_edge(scale, split, half, True, *last) for half in range(2)]
    else:
        sends, keeps = halves_of(sends[0])
    return exchange(sends, keeps)


def solution(mesh):
    in_specs = (P("depth", "img", None),)
    out_specs = P(None, ("img", "depth"), None)
    return jax.shard_map(local, mesh=mesh, in_specs=in_specs, out_specs=out_specs, check_vma=False)
```

```python
import functools
import math

import jax
import jax.numpy as jnp
import numpy as np
from jax import lax
from jax.experimental import pallas as pl
from jax.experimental.pallas import tpu as pltpu
from jax.sharding import PartitionSpec as P


gauss_taps = [
    math.exp(-offset * offset / 8.0)
    / sum((math.exp(-other * other / 8.0) for other in range(-4, 5)))
    for offset in range(-4, 5)
]
light_z = 0.48
light_x = 0.6
light_y = 0.64


REACH = 5
FIRST_PART = 1
SIDE_GROUP = 4
PAD = 8


def band(size):
    index = np.arange(size)
    apart = np.abs(index[:, None] - index[None, :])
    taps = np.array(gauss_taps[4:] + [0.0], np.float64)
    return taps[np.minimum(apart, 5)]


def split_terms(matrix):
    high = matrix.astype(jnp.bfloat16)
    low = (matrix - high.astype(np.float64)).astype(jnp.bfloat16)
    return high, low


def column_matrices(columns):
    return np.concatenate(split_terms(band(columns)), 0)


def row_terms(matrix):
    high, low = split_terms(matrix)
    return np.concatenate([high, high, low], 1)


def row_orders(rows):
    full = band(rows + 2 * PAD)
    order = np.arange(rows + 2 * PAD)
    swapped = np.concatenate([order[rows + PAD :], order[PAD : rows + PAD], order[:PAD]])
    return [full[:, order], full[:, swapped]]


def row_matrices(rows):
    return np.stack([row_terms(matrix) for matrix in row_orders(rows)])


def own_matrix(rows):
    return row_terms(band(rows + 2 * PAD)[:, PAD : rows + PAD])


def side_matrices(rows):
    both = []
    for matrix in row_orders(rows):
        sides = np.concatenate([matrix[:, :PAD], matrix[:, rows + PAD :]], 1)
        touched = np.concatenate([sides[: 2 * PAD], sides[rows:]], 0)
        both.append(row_terms(np.kron(np.eye(SIDE_GROUP), touched)))
    return np.stack(both)


def two_terms(value, high, low):
    return jnp.dot(value, high, preferred_element_type=jnp.float32) + jnp.dot(
        value, low, preferred_element_type=jnp.float32
    )


def smooth_columns(exact, by):
    half = by.shape[0] // 2
    return two_terms(exact, by[:half], by[half:])


def column_terms(counts, by):
    exact = jnp.concatenate([c.astype(jnp.float32).astype(jnp.bfloat16) for c in counts], 0)
    wide = smooth_columns(exact, by)
    high = wide.astype(jnp.bfloat16)
    return high, (wide - high.astype(jnp.float32)).astype(jnp.bfloat16)


def row_product(matrix, high, low):
    stacked = jnp.concatenate([high, low, high], 0)
    return jnp.dot(matrix, stacked, preferred_element_type=jnp.float32)


def smooth_plane(counts, by, lx):
    rows = counts[0].shape[0]
    high, low = column_terms(counts, by)
    parts = [slice(n * rows, (n + 1) * rows) for n in range(len(counts))]
    return [row_product(lx, high[part], low[part]) for part in parts]


def smooth_depth(read, k):
    total = gauss_taps[4] * read(k)
    for offset in range(1, 5):
        total = total + gauss_taps[4 + offset] * (read(k - offset) + read(k + offset))
    return total


def smooth_depth_layers(flags, read, ks, tiles, write):
    for tile in range(tiles):
        rows = pl.ds(tile * 8, 8)
        for n, k in enumerate(ks):
            value = smooth_depth(lambda j: read(j, rows), k)
            if tile == 0:
                value = value * flags[0]
            if tile == tiles - 1:
                value = value * flags[1]
            write(n, rows, value)


def beside(mid, step):
    lanes = 128
    lane = lax.broadcasted_iota(jnp.int32, (mid.shape[0], lanes), 1)
    parts = [mid[:, at : at + lanes] for at in range(0, mid.shape[1], lanes)]
    turned = [pltpu.roll(part, lanes - 1 if step == 1 else 1, 1) for part in parts]
    zero = jnp.zeros_like(parts[0])
    if step == 1:
        return jnp.concatenate(
            [jnp.where(lane == lanes - 1, y, x) for x, y in zip(turned, turned[1:] + [zero])], 1
        )
    return jnp.concatenate(
        [jnp.where(lane == 0, y, x) for x, y in zip(turned, [zero] + turned[:-1])], 1
    )


def render_layer(layer, k, base, carry, scale):
    total, tilted, green, transmit = carry
    rows = pl.ds(base, 8)
    mid = layer(k, rows)
    before = layer(k, pl.ds(base - 8, 8))
    after = layer(k, pl.ds(base + 8, 8))
    sub = lax.broadcasted_iota(jnp.int32, mid.shape, 0)
    above = pltpu.roll(jnp.where(sub == 7, before, mid), 1, 0)
    below = pltpu.roll(jnp.where(sub == 0, after, mid), 7, 0)
    dz = layer(k + 1, rows) - layer(k - 1, rows)
    dx = below - above
    dy = beside(mid, 1) - beside(mid, -1)
    slope = (1.5 * light_z) * dz + (1.5 * light_x) * dx + (1.5 * light_y) * dy
    shading = jnp.tanh(slope) + (0.55 / 0.45)
    gradient_sq4 = dz * dz + dx * dx + dy * dy
    square = mid * mid
    optical = (square / (1.0 + square)) * (1.0 + gradient_sq4)
    centred = mid - 2.5
    log2e = math.log2(math.e)
    remaining = transmit * jnp.exp2(optical * (-scale * log2e))
    lit = (transmit - remaining) * shading
    return (
        total + lit,
        tilted + lit * jnp.tanh(centred),
        green + lit * jnp.exp2((centred * -log2e) * centred),
        remaining,
    )


def empty_carry(columns):
    zero = jnp.zeros((8, columns), jnp.float32)
    return zero, zero, zero, jnp.ones_like(zero)


def read_tile(ref, tile):
    rows = pl.ds(pl.multiple_of(tile * 8, 8), 8)
    return tuple(ref[n, rows, :] for n in range(4))


def store_tile(ref, tile, values):
    rows = pl.ds(pl.multiple_of(tile * 8, 8), 8)
    for n, value in enumerate(values):
        ref[n, rows, :] = value


def run_copies(copies):
    for copy in copies:
        copy.start()
    for copy in copies:
        copy.wait()


def run_copies(pairs, sems):
    copies = [pltpu.make_async_copy(*pair, sems.at[n]) for n, pair in enumerate(pairs)]
    for copy in copies:
        copy.start()
    for copy in copies:
        copy.wait()


def pack_rest_kernel(where, c, side_b, edge, middle, side_a, sems):
    rows = c.shape[1]
    layers = pl.ds(where[0], REACH)
    pairs = [
        (c.at[:, pl.ds(pl.multiple_of(where[2 + n], PAD), PAD)], side)
        for n, side in enumerate((side_a, side_b))
    ]
    pairs.append((c.at[layers, pl.ds(0, PAD)], edge.at[:, pl.ds(0, PAD)]))
    pairs.append((c.at[layers, pl.ds(rows - PAD, PAD)], edge.at[:, pl.ds(PAD, PAD)]))
    pairs.append((c.at[layers, pl.ds(PAD, rows - 2 * PAD)], middle))
    run_copies(pairs, sems)


def smooth_kernel(group, c_hbm, by, lx, plane, c, sems):
    groups = c.shape[0] // group

    def fetch(g):
        part = pl.ds(g * group, group)
        return pltpu.make_async_copy(c_hbm.at[part], c.at[part], sems.at[g])

    for g in range(groups):
        fetch(g).start()

    def smooth_group(g, _):
        first = g * group
        fetch(g).wait()
        counts = [c[first + n] for n in range(group)]
        for n, value in enumerate(smooth_plane(counts, by, lx[...])):
            plane[first + n] = value
        return 0

    lax.fori_loop(0, groups, smooth_group, 0)


def depth_kernel(flags, order, partial, xa, xb, by, lx, plane, smoothed):
    layers, ext, _ = plane.shape
    group = 4 * SIDE_GROUP
    edge = 2 * PAD
    sides = lx[order[0]]

    def add_sides(g, _):
        first = g * group
        counts = [jnp.concatenate([xa[first + n], xb[first + n]], 0) for n in range(group)]
        high, low = column_terms(counts, by)
        for half in range(4):
            part = slice(half * SIDE_GROUP * edge, (half + 1) * SIDE_GROUP * edge)
            added = row_product(sides, high[part], low[part])
            for n in range(SIDE_GROUP):
                k = first + half * SIDE_GROUP + n
                at = n * 2 * edge
                plane[k, :edge, :] = partial[k, :edge, :] + added[at : at + edge]
                plane[k, ext - edge :, :] = (
                    partial[k, ext - edge :, :] + added[at + edge : at + 2 * edge]
                )
        return 0

    lax.fori_loop(0, layers // group, add_sides, 0)

    together = 2 if layers % 2 == 0 else 1

    def some_layers(m, _):
        first = m * together

        def write(n, rows, value):
            smoothed[first + n, rows, :] = value

        ks = [first + n + 4 for n in range(together)]
        smooth_depth_layers(flags, lambda k, rows: plane[k, rows, :], ks, ext // 8, write)
        return 0

    lax.fori_loop(0, (layers - 8) // together, some_layers, 0)


def interior_kernel(scale, smoothed, image):
    held, ext, columns = smoothed.shape

    def one_tile(tile, _):
        base = pl.multiple_of(tile * 8 + 8, 8)
        carry = empty_carry(columns)
        for k in range(1, held - 1):
            carry = render_layer(lambda k, rows: smoothed[k, rows, :], k, base, carry, scale)
        store_tile(image, tile, carry)
        return 0

    lax.fori_loop(0, ext // 8 - 2, one_tile, 0)


def edge_smooth(turn, flags, order, plane, smoothed, planes, ends, halo):
    layers, ext, _ = plane.shape
    is_front = order[1] == 1 - turn
    sign = jnp.where(is_front, 1, -1)
    for j, value in enumerate(planes):
        halo[j] = value
    plane_face = jnp.where(is_front, 0, layers - 1)
    halo_face = jnp.where(is_front, REACH, -1)
    ends_face = jnp.where(is_front, 1, REACH)
    smoothed_face = jnp.where(is_front, -4, layers - 5)
    on_grid = jnp.where(is_front, flags[2], flags[3])

    def counted(v, rows):
        if v < 0:
            return halo[halo_face + sign * v, rows, :]
        return plane[plane_face + sign * v, rows, :]

    def write(n, rows, value):
        ends[ends_face + sign * (n - 1), rows, :] = value * on_grid if n == 0 else value

    smooth_depth_layers(flags, counted, range(-1, 4), ext // 8, write)
    for v in (4, 5):
        ends[ends_face + sign * v] = smoothed[smoothed_face + sign * v]


def edge_render(scale, is_front, ends, behind, image, tiles, tile_of, first=0):
    columns = ends.shape[2]

    def one_tile(place):
        tile = tile_of(place + first)
        base = pl.multiple_of(tile * 8 + 8, 8)
        carry = empty_carry(columns)
        for k in range(1, REACH + 1):
            carry = render_layer(lambda k, rows: ends[k, rows, :], k, base, carry, scale)
        other = read_tile(behind, tile)
        front = [jnp.where(is_front, x, y) for x, y in zip(carry, other)]
        back = [jnp.where(is_front, y, x) for x, y in zip(carry, other)]
        colors = [front[n] + front[3] * back[n] for n in range(3)]
        colors.append(front[3] * back[3])
        if len(image.shape) == 3:
            store_tile(image, place, colors)
        else:
            owner_tiles = image.shape[2] // 8
            store_tile(image.at[place // owner_tiles], place % owner_tiles, colors)

    together = 2 if tiles % 2 == 0 else 1

    def some_tiles(n, _):
        for m in range(together):
            one_tile(n * together + m)
        return 0

    lax.fori_loop(0, tiles // together, some_tiles, 0)


def half_tiles(order, pairs, owner_tiles, wanted):
    def tile_of(place):
        pair = order[2] ^ (pairs - 1 - place // owner_tiles)
        return (2 * pair + wanted) * owner_tiles + place % owner_tiles

    return tile_of


def first_edge_kernel(scale, flags, order, plane, smoothed, block, ca, cb, by, lx, behind, image,
                      ends, halo):
    counts = [jnp.concatenate([ca[j], block[j], cb[j]], 0) for j in range(REACH)]
    planes = smooth_plane(counts, by, lx[order[0]])
    edge_smooth(1, flags, order, plane, smoothed, planes, ends, halo)
    tiles = plane.shape[1] // 8 - 2
    edge_render(scale, order[1] == 0, ends, behind, image, tiles, lambda place: place)


def render_half(scale, is_front, ends, behind, image, tile_of, half):
    places, _, owned, _ = image.shape
    owner_tiles = owned // 8
    first = half * FIRST_PART * owner_tiles
    edge_render(scale, is_front, ends, behind, image, places * owner_tiles, tile_of, first)


def last_edge_kernel(scale, split, flags, order, plane, smoothed, middle_any, edge, ca, cb,
                     by, lx, behind, *refs):
    images, (ends, halo, middle, sem) = refs[:-4], refs[-4:]
    fetch = pltpu.make_async_copy(middle_any, middle, sem.at[0])
    fetch.start()
    two = 2 * PAD
    outer = [
        jnp.concatenate([ca[j], edge[j, :PAD], edge[j, PAD:], cb[j]], 0) for j in range(REACH)
    ]
    outer = column_terms(outer, by)
    fetch.wait()
    inner = column_terms([middle[j] for j in range(REACH)], by)
    rows = middle.shape[1]
    planes = []
    for j in range(REACH):
        high, low = (
            jnp.concatenate(
                [
                    out[2 * two * j : 2 * two * j + two],
                    mid[rows * j : rows * (j + 1)],
                    out[2 * two * j + two : 2 * two * (j + 1)],
                ],
                0,
            )
            for out, mid in zip(outer, inner)
        )
        planes.append(row_product(lx[order[0]], high, low))
    edge_smooth(0, flags, order, plane, smoothed, planes, ends, halo)
    if split:
        tile_of = half_tiles(order, *split, 1 - order[1])
        render_half(scale, order[1] == 1, ends, behind, images[0], tile_of, 0)
    else:
        tiles = plane.shape[1] // 8 - 2
        edge_render(scale, order[1] == 1, ends, behind, images[0], tiles, lambda place: place)


def part_edge_kernel(scale, split, half, kept, order, ends, behind, image):
    tile_of = half_tiles(order, *split, order[1] if kept else 1 - order[1])
    render_half(scale, order[1] == 1, ends, behind, image, tile_of, half)


def whole(count):
    return [pl.BlockSpec(memory_space=pltpu.VMEM)] * count


def smem():
    return pl.BlockSpec(memory_space=pltpu.SMEM)


def in_hbm():
    return pl.BlockSpec(memory_space=pltpu.HBM)


def params(mib):
    return pltpu.CompilerParams(vmem_limit_bytes=mib * 1024 * 1024)


def cost(flops):
    return pl.CostEstimate(flops=flops, transcendentals=0, bytes_accessed=4_000_000)


def call_pack_rest(where, c):
    layers, rows, columns = c.shape
    edge = jax.ShapeDtypeStruct((REACH, 2 * PAD, columns), c.dtype)
    side = jax.ShapeDtypeStruct((layers, PAD, columns), c.dtype)
    middle = jax.ShapeDtypeStruct((REACH, rows - 2 * PAD, columns), c.dtype)
    return pl.pallas_call(
        pack_rest_kernel,
        out_shape=(side, edge, middle, side),
        in_specs=[smem(), in_hbm()],
        out_specs=tuple(whole(4)),
        scratch_shapes=[pltpu.SemaphoreType.DMA((5,))],
        compiler_params=params(8),
        name="pack_rest",
    )(where, c)


def call_smooth(c, by, lx):
    layers, rows, columns = c.shape
    ext = rows + 2 * PAD
    group = 8
    return pl.pallas_call(
        functools.partial(smooth_kernel, group),
        out_shape=jax.ShapeDtypeStruct((layers, ext, columns), jnp.float32),
        in_specs=[in_hbm()] + whole(2),
        out_specs=whole(1)[0],
        scratch_shapes=[
            pltpu.VMEM((layers, rows, columns), jnp.int32),
            pltpu.SemaphoreType.DMA((layers // group,)),
        ],
        compiler_params=params(16),
        cost_estimate=cost(1_000_000_000),
        name="smooth",
    )(c, by, lx)


def call_depth(flags, order, partial, *operands):
    layers, ext, columns = partial.shape
    return pl.pallas_call(
        depth_kernel,
        out_shape=(
            jax.ShapeDtypeStruct(partial.shape, jnp.float32),
            jax.ShapeDtypeStruct((layers - 8, ext, columns), jnp.float32),
        ),
        in_specs=[smem(), smem()] + whole(1 + len(operands)),
        out_specs=tuple(whole(2)),
        input_output_aliases={2: 0},
        compiler_params=params(12),
        cost_estimate=cost(500_000_000),
        name="depth",
    )(flags, order, partial, *operands)


def call_interior(scale, smoothed):
    _, ext, columns = smoothed.shape
    return pl.pallas_call(
        functools.partial(interior_kernel, scale),
        out_shape=jax.ShapeDtypeStruct((4, ext - 2 * PAD, columns), jnp.float32),
        in_specs=whole(1),
        out_specs=whole(1)[0],
        compiler_params=params(12),
        cost_estimate=cost(1_000_000_000),
        name="interior",
    )(smoothed)


def call_first_edge(scale, flags, order, plane, *operands):
    _, ext, columns = plane.shape
    f32 = jnp.float32
    return pl.pallas_call(
        functools.partial(first_edge_kernel, scale),
        out_shape=jax.ShapeDtypeStruct((4, ext - 2 * PAD, columns), f32),
        in_specs=[smem(), smem()] + whole(1 + len(operands)),
        out_specs=whole(1)[0],
        scratch_shapes=[
            pltpu.VMEM((REACH + 2, ext, columns), f32),
            pltpu.VMEM((REACH, ext, columns), f32),
        ],
        compiler_params=params(24),
        cost_estimate=cost(300_000_000),
        name="first_edge",
    )(flags, order, plane, *operands)


def half_shape(split, half, columns):
    pairs, owner_tiles = split
    return pairs - FIRST_PART if half else FIRST_PART, 4, owner_tiles * 8, columns


def call_last_edge(scale, split, flags, order, plane, *operands):
    _, ext, columns = plane.shape
    f32 = jnp.float32
    rows = ext - 2 * PAD
    images = [half_shape(split, 0, columns) if split else (4, rows, columns)]
    shapes = [*images, (REACH + 2, ext, columns)]
    return pl.pallas_call(
        functools.partial(last_edge_kernel, scale, split),
        out_shape=tuple(jax.ShapeDtypeStruct(shape, f32) for shape in shapes),
        in_specs=[smem(), smem()] + whole(2) + [in_hbm()] + whole(len(operands) - 2),
        out_specs=tuple(whole(len(shapes))),
        scratch_shapes=[
            pltpu.VMEM((REACH, ext, columns), f32),
            pltpu.VMEM(operands[1].shape, operands[1].dtype),
            pltpu.SemaphoreType.DMA((1,)),
        ],
        compiler_params=params(12),
        cost_estimate=cost(300_000_000),
        name="last_edge",
    )(flags, order, plane, *operands)


def call_part_edge(scale, split, half, kept, order, ends, behind):
    image = jax.ShapeDtypeStruct(half_shape(split, half, ends.shape[2]), jnp.float32)
    return pl.pallas_call(
        functools.partial(part_edge_kernel, scale, split, half, kept),
        out_shape=image,
        in_specs=[smem()] + whole(2),
        out_specs=whole(1)[0],
        compiler_params=params(12),
        cost_estimate=cost(200_000_000),
    )(order, ends, behind)


def swap(value, axis, first):
    count = lax.axis_size(axis)
    pairs = []
    for low in range(first, count - 1, 2):
        pairs += [(low, low + 1), (low + 1, low)]
    return lax.ppermute(value, axis, pairs)


def over(front, back):
    through = front[:, 3:]
    return jnp.concatenate([front[:, :3] + through * back[:, :3], through * back[:, 3:]], 1)


def halves_of(layers):
    count = lax.axis_size("depth")
    me = lax.axis_index("depth")
    parity, pair, pairs = me % 2, me // 2, count // 2
    _, rows, columns = layers.shape
    pieces = layers.reshape(4, pairs, 2, rows // count, columns)
    ordered = jnp.concatenate(
        [lax.dynamic_slice_in_dim(pieces, pair ^ step, 1, 1) for step in reversed(range(pairs))], 1
    )
    both = []
    for wanted in (1 - parity, parity):
        chosen = lax.dynamic_index_in_dim(ordered, wanted, 2, keepdims=False)
        chosen = jnp.moveaxis(chosen, 1, 0)
        both.append((chosen[:FIRST_PART], chosen[FIRST_PART:]))
    return both


def exchange(sends, keeps):
    count = lax.axis_size("depth")
    me = lax.axis_index("depth")
    parity, pair = me % 2, me // 2
    pairs = count // 2
    parts = [None] * pairs
    for half, (send, keep) in enumerate(zip(sends, keeps)):
        owned, columns = send.shape[2:]
        got = swap(send, "depth", 0)
        joined = jnp.where(parity == 0, over(keep, got), over(got, keep))
        for place in range(send.shape[0]):
            step = pairs - 1 - half * FIRST_PART - place
            piece = joined[place]
            if step:
                piece = lax.ppermute(piece, "depth", [(i, i ^ (2 * step)) for i in range(count)])
            parts[step] = piece
    result = jnp.zeros((3, owned, columns), jnp.float32)
    through = jnp.ones((1, owned, columns), jnp.float32)
    for step in range(pairs):
        ahead = jnp.ones((1, owned, columns), jnp.float32)
        for other in range(pairs):
            if other != step:
                nearer = (pair ^ other) < (pair ^ step)
                ahead = ahead * jnp.where(nearer, parts[other][3:], 1.0)
        result = result + ahead * parts[step][:3]
        through = through * parts[step][3:]
    total, tilted, green = 0.225 * result[:1], 0.225 * result[1:2], 0.45 * result[2:]
    return jnp.concatenate([total + tilted, green, total - tilted, 1.0 - through], 0)


def local(counts):
    slab, rows, columns = counts.shape
    img, depth = lax.axis_index("img"), lax.axis_index("depth")
    imgs, depths = lax.axis_size("img"), lax.axis_size("depth")
    scale = 1.5 / (slab * depths)
    row_odd, depth_odd = img % 2, depth % 2
    first_a, first_b = (1 - depth_odd) * (slab - REACH), depth_odd * (slab - REACH)
    row_a, row_b = (1 - row_odd) * (rows - PAD), row_odd * (rows - PAD)
    where = jnp.stack([first_a, first_b, row_a, row_b])
    order = jnp.stack([1 - row_odd, depth_odd, depth // 2])
    one = jnp.float32(1.0)
    flags = jnp.stack(
        [(img > 0) * one, (img < imgs - 1) * one, (depth > 0) * one, (depth < depths - 1) * one]
    )
    by = jnp.asarray(column_matrices(columns))
    lx = jnp.asarray(row_matrices(rows))
    held = pltpu.with_memory_space_constraint(counts, pltpu.HBM)
    block_b = lax.dynamic_slice_in_dim(counts, first_b, REACH, 0)
    side_b, edge_a, mid_a, side_a = call_pack_rest(where, held)
    block_b = swap(block_b, "depth", 1)
    xb = swap(side_b, "img", 1)
    edge_a = swap(edge_a, "depth", 0)
    mid_a = swap(mid_a, "depth", 0)
    xa = swap(side_a, "img", 0)

    def corner(far):
        of_a = lax.dynamic_slice_in_dim(edge_a, far * PAD, PAD, 1)
        of_b = lax.dynamic_slice_in_dim(block_b, far * (rows - PAD), PAD, 1)
        return jnp.concatenate([of_a, of_b], 0)

    ca = swap(corner(1 - row_odd), "img", 0)
    cb = swap(corner(row_odd), "img", 1)
    partial = call_smooth(held, by, jnp.asarray(own_matrix(rows)))
    plane, smoothed = call_depth(
        flags, order, partial, xa, xb, by, jnp.asarray(side_matrices(rows))
    )
    inner = call_interior(scale, smoothed)
    owned = rows // depths
    split = (depths // 2, owned // 8) if owned % 8 == 0 else None
    common = (flags, order, plane, smoothed)
    layers = call_first_edge(
        scale, *common, block_b, ca[REACH:], cb[REACH:], by, lx, inner
    )
    mid_a = pltpu.with_memory_space_constraint(mid_a, pltpu.HBM)
    *sends, ends = call_last_edge(
        scale, split, *common, mid_a, edge_a, ca[:REACH], cb[:REACH], by, lx, layers
    )
    if split:
        last = (order, ends, layers)
        sends.append(call_part_edge(scale, split, 1, False, *last))
        keeps = [call_part_edge(scale, split, half, True, *last) for half in range(2)]
    else:
        sends, keeps = halves_of(sends[0])
    return exchange(sends, keeps)


def solution(mesh):
    in_specs = (P("depth", "img", None),)
    out_specs = P(None, ("img", "depth"), None)
    return jax.shard_map(local, mesh=mesh, in_specs=in_specs, out_specs=out_specs, check_vma=False)
```

```python
import functools
import math

import jax
import jax.numpy as jnp
import numpy as np
from jax import lax
from jax.experimental import pallas as pl
from jax.experimental.pallas import tpu as pltpu
from jax.sharding import PartitionSpec as P


gauss_taps = [
    math.exp(-offset * offset / 8.0)
    / sum((math.exp(-other * other / 8.0) for other in range(-4, 5)))
    for offset in range(-4, 5)
]
light_z = 0.48
light_x = 0.6
light_y = 0.64


REACH = 5
SIDE_GROUP = 4
PAD = 8


def band(size):
    index = np.arange(size)
    apart = np.abs(index[:, None] - index[None, :])
    taps = np.array(gauss_taps[4:] + [0.0], np.float64)
    return taps[np.minimum(apart, 5)]


def split_terms(matrix):
    high = matrix.astype(jnp.bfloat16)
    low = (matrix - high.astype(np.float64)).astype(jnp.bfloat16)
    return high, low


def column_matrices(columns):
    return np.concatenate(split_terms(band(columns)), 0)


def row_terms(matrix):
    high, low = split_terms(matrix)
    return np.concatenate([high, high, low], 1)


def row_orders(rows):
    full = band(rows + 2 * PAD)
    order = np.arange(rows + 2 * PAD)
    swapped = np.concatenate([order[rows + PAD :], order[PAD : rows + PAD], order[:PAD]])
    return [full[:, order], full[:, swapped]]


def row_matrices(rows):
    return np.stack([row_terms(matrix) for matrix in row_orders(rows)])


def own_matrix(rows):
    return row_terms(band(rows + 2 * PAD)[:, PAD : rows + PAD])


def side_matrices(rows):
    both = []
    for matrix in row_orders(rows):
        sides = np.concatenate([matrix[:, :PAD], matrix[:, rows + PAD :]], 1)
        touched = np.concatenate([sides[: 2 * PAD], sides[rows:]], 0)
        both.append(row_terms(np.kron(np.eye(SIDE_GROUP), touched)))
    return np.stack(both)


def two_terms(value, high, low):
    return jnp.dot(value, high, preferred_element_type=jnp.float32) + jnp.dot(
        value, low, preferred_element_type=jnp.float32
    )


def smooth_columns(exact, by):
    half = by.shape[0] // 2
    return two_terms(exact, by[:half], by[half:])


def column_terms(counts, by):
    exact = jnp.concatenate([c.astype(jnp.float32).astype(jnp.bfloat16) for c in counts], 0)
    wide = smooth_columns(exact, by)
    high = wide.astype(jnp.bfloat16)
    return high, (wide - high.astype(jnp.float32)).astype(jnp.bfloat16)


def row_product(matrix, high, low):
    stacked = jnp.concatenate([high, low, high], 0)
    return jnp.dot(matrix, stacked, preferred_element_type=jnp.float32)


def smooth_plane(counts, by, lx):
    rows = counts[0].shape[0]
    high, low = column_terms(counts, by)
    parts = [slice(n * rows, (n + 1) * rows) for n in range(len(counts))]
    return [row_product(lx, high[part], low[part]) for part in parts]


def smooth_depth(read, k):
    total = gauss_taps[4] * read(k)
    for offset in range(1, 5):
        total = total + gauss_taps[4 + offset] * (read(k - offset) + read(k + offset))
    return total


def smooth_depth_layers(flags, read, ks, tiles, write):
    for tile in range(tiles):
        rows = pl.ds(tile * 8, 8)
        for n, k in enumerate(ks):
            value = smooth_depth(lambda j: read(j, rows), k)
            if tile == 0:
                value = value * flags[0]
            if tile == tiles - 1:
                value = value * flags[1]
            write(n, rows, value)


def beside(mid, step):
    lanes = 128
    lane = lax.broadcasted_iota(jnp.int32, (mid.shape[0], lanes), 1)
    parts = [mid[:, at : at + lanes] for at in range(0, mid.shape[1], lanes)]
    turned = [pltpu.roll(part, lanes - 1 if step == 1 else 1, 1) for part in parts]
    zero = jnp.zeros_like(parts[0])
    if step == 1:
        return jnp.concatenate(
            [jnp.where(lane == lanes - 1, y, x) for x, y in zip(turned, turned[1:] + [zero])], 1
        )
    return jnp.concatenate(
        [jnp.where(lane == 0, y, x) for x, y in zip(turned, [zero] + turned[:-1])], 1
    )


def render_layer(layer, k, base, carry, scale):
    total, tilted, green, transmit = carry
    rows = pl.ds(base, 8)
    mid = layer(k, rows)
    before = layer(k, pl.ds(base - 8, 8))
    after = layer(k, pl.ds(base + 8, 8))
    sub = lax.broadcasted_iota(jnp.int32, mid.shape, 0)
    above = pltpu.roll(jnp.where(sub == 7, before, mid), 1, 0)
    below = pltpu.roll(jnp.where(sub == 0, after, mid), 7, 0)
    dz = layer(k + 1, rows) - layer(k - 1, rows)
    dx = below - above
    dy = beside(mid, 1) - beside(mid, -1)
    slope = (1.5 * light_z) * dz + (1.5 * light_x) * dx + (1.5 * light_y) * dy
    shading = jnp.tanh(slope) + (0.55 / 0.45)
    gradient_sq4 = dz * dz + dx * dx + dy * dy
    square = mid * mid
    optical = (square / (1.0 + square)) * (1.0 + gradient_sq4)
    centred = mid - 2.5
    log2e = math.log2(math.e)
    remaining = transmit * jnp.exp2(optical * (-scale * log2e))
    lit = (transmit - remaining) * shading
    return (
        total + lit,
        tilted + lit * jnp.tanh(centred),
        green + lit * jnp.exp2((centred * -log2e) * centred),
        remaining,
    )


def empty_carry(columns):
    zero = jnp.zeros((8, columns), jnp.float32)
    return zero, zero, zero, jnp.ones_like(zero)


def read_tile(ref, tile):
    rows = pl.ds(pl.multiple_of(tile * 8, 8), 8)
    return tuple(ref[n, rows, :] for n in range(4))


def store_tile(ref, tile, values):
    rows = pl.ds(pl.multiple_of(tile * 8, 8), 8)
    for n, value in enumerate(values):
        ref[n, rows, :] = value


def run_copies(copies):
    for copy in copies:
        copy.start()
    for copy in copies:
        copy.wait()


def run_copies(pairs, sems):
    copies = [pltpu.make_async_copy(*pair, sems.at[n]) for n, pair in enumerate(pairs)]
    for copy in copies:
        copy.start()
    for copy in copies:
        copy.wait()


def pack_block_kernel(where, c, block, sems):
    run_copies([(c.at[where[1] + n], block.at[n]) for n in range(REACH)], sems)


def pack_rest_kernel(where, c, side_b, edge, middle, side_a, sems):
    rows = c.shape[1]
    layers = pl.ds(where[0], REACH)
    pairs = [
        (c.at[:, pl.ds(pl.multiple_of(where[2 + n], PAD), PAD)], side)
        for n, side in enumerate((side_a, side_b))
    ]
    pairs.append((c.at[layers, pl.ds(0, PAD)], edge.at[:, pl.ds(0, PAD)]))
    pairs.append((c.at[layers, pl.ds(rows - PAD, PAD)], edge.at[:, pl.ds(PAD, PAD)]))
    pairs.append((c.at[layers, pl.ds(PAD, rows - 2 * PAD)], middle))
    run_copies(pairs, sems)


def smooth_kernel(group, c_hbm, by, lx, plane, c, sems):
    groups = c.shape[0] // group

    def fetch(g):
        part = pl.ds(g * group, group)
        return pltpu.make_async_copy(c_hbm.at[part], c.at[part], sems.at[g])

    for g in range(groups):
        fetch(g).start()

    def smooth_group(g, _):
        first = g * group
        fetch(g).wait()
        counts = [c[first + n] for n in range(group)]
        for n, value in enumerate(smooth_plane(counts, by, lx[...])):
            plane[first + n] = value
        return 0

    lax.fori_loop(0, groups, smooth_group, 0)


def depth_kernel(flags, order, partial, xa, xb, by, lx, plane, smoothed):
    layers, ext, _ = plane.shape
    group = 4 * SIDE_GROUP
    edge = 2 * PAD
    sides = lx[order[0]]

    def add_sides(g, _):
        first = g * group
        counts = [jnp.concatenate([xa[first + n], xb[first + n]], 0) for n in range(group)]
        high, low = column_terms(counts, by)
        for half in range(4):
            part = slice(half * SIDE_GROUP * edge, (half + 1) * SIDE_GROUP * edge)
            added = row_product(sides, high[part], low[part])
            for n in range(SIDE_GROUP):
                k = first + half * SIDE_GROUP + n
                at = n * 2 * edge
                plane[k, :edge, :] = partial[k, :edge, :] + added[at : at + edge]
                plane[k, ext - edge :, :] = (
                    partial[k, ext - edge :, :] + added[at + edge : at + 2 * edge]
                )
        return 0

    lax.fori_loop(0, layers // group, add_sides, 0)

    together = 2 if layers % 2 == 0 else 1

    def some_layers(m, _):
        first = m * together

        def write(n, rows, value):
            smoothed[first + n, rows, :] = value

        ks = [first + n + 4 for n in range(together)]
        smooth_depth_layers(flags, lambda k, rows: plane[k, rows, :], ks, ext // 8, write)
        return 0

    lax.fori_loop(0, (layers - 8) // together, some_layers, 0)


def interior_kernel(scale, smoothed, image):
    held, ext, columns = smoothed.shape

    def one_tile(tile, _):
        base = pl.multiple_of(tile * 8 + 8, 8)
        carry = empty_carry(columns)
        for k in range(1, held - 1):
            carry = render_layer(lambda k, rows: smoothed[k, rows, :], k, base, carry, scale)
        store_tile(image, tile, carry)
        return 0

    lax.fori_loop(0, ext // 8 - 2, one_tile, 0)


def edge_smooth(turn, flags, order, plane, smoothed, planes, ends, halo):
    layers, ext, _ = plane.shape
    is_front = order[1] == 1 - turn
    sign = jnp.where(is_front, 1, -1)
    for j, value in enumerate(planes):
        halo[j] = value
    plane_face = jnp.where(is_front, 0, layers - 1)
    halo_face = jnp.where(is_front, REACH, -1)
    ends_face = jnp.where(is_front, 1, REACH)
    smoothed_face = jnp.where(is_front, -4, layers - 5)
    on_grid = jnp.where(is_front, flags[2], flags[3])

    def counted(v, rows):
        if v < 0:
            return halo[halo_face + sign * v, rows, :]
        return plane[plane_face + sign * v, rows, :]

    def write(n, rows, value):
        ends[ends_face + sign * (n - 1), rows, :] = value * on_grid if n == 0 else value

    smooth_depth_layers(flags, counted, range(-1, 4), ext // 8, write)
    for v in (4, 5):
        ends[ends_face + sign * v] = smoothed[smoothed_face + sign * v]


def edge_render(scale, is_front, ends, behind, image, tiles, tile_of, first=0):
    columns = ends.shape[2]

    def one_tile(place):
        tile = tile_of(place + first)
        base = pl.multiple_of(tile * 8 + 8, 8)
        carry = empty_carry(columns)
        for k in range(1, REACH + 1):
            carry = render_layer(lambda k, rows: ends[k, rows, :], k, base, carry, scale)
        other = read_tile(behind, tile)
        front = [jnp.where(is_front, x, y) for x, y in zip(carry, other)]
        back = [jnp.where(is_front, y, x) for x, y in zip(carry, other)]
        colors = [front[n] + front[3] * back[n] for n in range(3)]
        colors.append(front[3] * back[3])
        if len(image.shape) == 3:
            store_tile(image, place, colors)
        else:
            owner_tiles = image.shape[2] // 8
            store_tile(image.at[place // owner_tiles], place % owner_tiles, colors)

    together = 2 if tiles % 2 == 0 else 1

    def some_tiles(n, _):
        for m in range(together):
            one_tile(n * together + m)
        return 0

    lax.fori_loop(0, tiles // together, some_tiles, 0)


def half_tiles(order, pairs, owner_tiles, wanted):
    def tile_of(place):
        pair = order[2] ^ (pairs - 1 - place // owner_tiles)
        return (2 * pair + wanted) * owner_tiles + place % owner_tiles

    return tile_of


def first_edge_kernel(scale, flags, order, plane, smoothed, block, ca, cb, by, lx, behind, image,
                      ends, halo):
    counts = [jnp.concatenate([ca[j], block[j], cb[j]], 0) for j in range(REACH)]
    planes = smooth_plane(counts, by, lx[order[0]])
    edge_smooth(1, flags, order, plane, smoothed, planes, ends, halo)
    tiles = plane.shape[1] // 8 - 2
    edge_render(scale, order[1] == 0, ends, behind, image, tiles, lambda place: place)


def render_half(scale, is_front, ends, behind, image, tile_of, half):
    places, _, owned, _ = image.shape
    owner_tiles = owned // 8
    first = half * owner_tiles
    edge_render(scale, is_front, ends, behind, image, places * owner_tiles, tile_of, first)


def last_edge_kernel(scale, split, flags, order, plane, smoothed, middle_any, edge, ca, cb,
                     by, lx, behind, *refs):
    images, (ends, halo, middle, sem) = refs[:-4], refs[-4:]
    fetch = pltpu.make_async_copy(middle_any, middle, sem.at[0])
    fetch.start()
    two = 2 * PAD
    outer = [
        jnp.concatenate([ca[j], edge[j, :PAD], edge[j, PAD:], cb[j]], 0) for j in range(REACH)
    ]
    outer = column_terms(outer, by)
    fetch.wait()
    inner = column_terms([middle[j] for j in range(REACH)], by)
    rows = middle.shape[1]
    planes = []
    for j in range(REACH):
        high, low = (
            jnp.concatenate(
                [
                    out[2 * two * j : 2 * two * j + two],
                    mid[rows * j : rows * (j + 1)],
                    out[2 * two * j + two : 2 * two * (j + 1)],
                ],
                0,
            )
            for out, mid in zip(outer, inner)
        )
        planes.append(row_product(lx[order[0]], high, low))
    edge_smooth(0, flags, order, plane, smoothed, planes, ends, halo)
    if split:
        tile_of = half_tiles(order, *split, 1 - order[1])
        render_half(scale, order[1] == 1, ends, behind, images[0], tile_of, 0)
    else:
        tiles = plane.shape[1] // 8 - 2
        edge_render(scale, order[1] == 1, ends, behind, images[0], tiles, lambda place: place)


def part_edge_kernel(scale, split, half, kept, order, ends, behind, image):
    tile_of = half_tiles(order, *split, order[1] if kept else 1 - order[1])
    render_half(scale, order[1] == 1, ends, behind, image, tile_of, half)


def whole(count):
    return [pl.BlockSpec(memory_space=pltpu.VMEM)] * count


def smem():
    return pl.BlockSpec(memory_space=pltpu.SMEM)


def in_hbm():
    return pl.BlockSpec(memory_space=pltpu.HBM)


def params(mib):
    return pltpu.CompilerParams(vmem_limit_bytes=mib * 1024 * 1024)


def cost(flops):
    return pl.CostEstimate(flops=flops, transcendentals=0, bytes_accessed=4_000_000)


def call_pack_block(where, c):
    _, rows, columns = c.shape
    return pl.pallas_call(
        pack_block_kernel,
        out_shape=jax.ShapeDtypeStruct((REACH, rows, columns), c.dtype),
        in_specs=[smem(), in_hbm()],
        out_specs=whole(1)[0],
        scratch_shapes=[pltpu.SemaphoreType.DMA((REACH,))],
        compiler_params=params(8),
        name="pack_block",
    )(where, c)


def call_pack_rest(where, c):
    layers, rows, columns = c.shape
    edge = jax.ShapeDtypeStruct((REACH, 2 * PAD, columns), c.dtype)
    side = jax.ShapeDtypeStruct((layers, PAD, columns), c.dtype)
    middle = jax.ShapeDtypeStruct((REACH, rows - 2 * PAD, columns), c.dtype)
    return pl.pallas_call(
        pack_rest_kernel,
        out_shape=(side, edge, middle, side),
        in_specs=[smem(), in_hbm()],
        out_specs=tuple(whole(4)),
        scratch_shapes=[pltpu.SemaphoreType.DMA((5,))],
        compiler_params=params(8),
        name="pack_rest",
    )(where, c)


def call_smooth(c, by, lx):
    layers, rows, columns = c.shape
    ext = rows + 2 * PAD
    group = 8
    return pl.pallas_call(
        functools.partial(smooth_kernel, group),
        out_shape=jax.ShapeDtypeStruct((layers, ext, columns), jnp.float32),
        in_specs=[in_hbm()] + whole(2),
        out_specs=whole(1)[0],
        scratch_shapes=[
            pltpu.VMEM((layers, rows, columns), jnp.int32),
            pltpu.SemaphoreType.DMA((layers // group,)),
        ],
        compiler_params=params(16),
        cost_estimate=cost(1_000_000_000),
        name="smooth",
    )(c, by, lx)


def call_depth(flags, order, partial, *operands):
    layers, ext, columns = partial.shape
    return pl.pallas_call(
        depth_kernel,
        out_shape=(
            jax.ShapeDtypeStruct(partial.shape, jnp.float32),
            jax.ShapeDtypeStruct((layers - 8, ext, columns), jnp.float32),
        ),
        in_specs=[smem(), smem()] + whole(1 + len(operands)),
        out_specs=tuple(whole(2)),
        input_output_aliases={2: 0},
        compiler_params=params(12),
        cost_estimate=cost(500_000_000),
        name="depth",
    )(flags, order, partial, *operands)


def call_interior(scale, smoothed):
    _, ext, columns = smoothed.shape
    return pl.pallas_call(
        functools.partial(interior_kernel, scale),
        out_shape=jax.ShapeDtypeStruct((4, ext - 2 * PAD, columns), jnp.float32),
        in_specs=whole(1),
        out_specs=whole(1)[0],
        compiler_params=params(12),
        cost_estimate=cost(1_000_000_000),
        name="interior",
    )(smoothed)


def call_first_edge(scale, flags, order, plane, *operands):
    _, ext, columns = plane.shape
    f32 = jnp.float32
    return pl.pallas_call(
        functools.partial(first_edge_kernel, scale),
        out_shape=jax.ShapeDtypeStruct((4, ext - 2 * PAD, columns), f32),
        in_specs=[smem(), smem()] + whole(1 + len(operands)),
        out_specs=whole(1)[0],
        scratch_shapes=[
            pltpu.VMEM((REACH + 2, ext, columns), f32),
            pltpu.VMEM((REACH, ext, columns), f32),
        ],
        compiler_params=params(24),
        cost_estimate=cost(300_000_000),
        name="first_edge",
    )(flags, order, plane, *operands)


def part_sizes(pairs):
    return 1, 1, pairs - 2


def part_shape(split, part, columns):
    pairs, owner_tiles = split
    return part_sizes(pairs)[part], 4, owner_tiles * 8, columns


def call_last_edge(scale, split, flags, order, plane, *operands):
    _, ext, columns = plane.shape
    f32 = jnp.float32
    rows = ext - 2 * PAD
    images = [part_shape(split, 0, columns) if split else (4, rows, columns)]
    shapes = [*images, (REACH + 2, ext, columns)]
    return pl.pallas_call(
        functools.partial(last_edge_kernel, scale, split),
        out_shape=tuple(jax.ShapeDtypeStruct(shape, f32) for shape in shapes),
        in_specs=[smem(), smem()] + whole(2) + [in_hbm()] + whole(len(operands) - 2),
        out_specs=tuple(whole(len(shapes))),
        scratch_shapes=[
            pltpu.VMEM((REACH, ext, columns), f32),
            pltpu.VMEM(operands[1].shape, operands[1].dtype),
            pltpu.SemaphoreType.DMA((1,)),
        ],
        compiler_params=params(12),
        cost_estimate=cost(300_000_000),
        name="last_edge",
    )(flags, order, plane, *operands)


def call_part_edge(scale, split, half, kept, order, ends, behind):
    image = jax.ShapeDtypeStruct(part_shape(split, half, ends.shape[2]), jnp.float32)
    return pl.pallas_call(
        functools.partial(part_edge_kernel, scale, split, half, kept),
        out_shape=image,
        in_specs=[smem()] + whole(2),
        out_specs=whole(1)[0],
        compiler_params=params(12),
        cost_estimate=cost(200_000_000),
    )(order, ends, behind)


def swap(value, axis, first):
    count = lax.axis_size(axis)
    pairs = []
    for low in range(first, count - 1, 2):
        pairs += [(low, low + 1), (low + 1, low)]
    return lax.ppermute(value, axis, pairs)


def over(front, back):
    through = front[:, 3:]
    return jnp.concatenate([front[:, :3] + through * back[:, :3], through * back[:, 3:]], 1)


def halves_of(layers):
    count = lax.axis_size("depth")
    me = lax.axis_index("depth")
    parity, pair, pairs = me % 2, me // 2, count // 2
    _, rows, columns = layers.shape
    pieces = layers.reshape(4, pairs, 2, rows // count, columns)
    ordered = jnp.concatenate(
        [lax.dynamic_slice_in_dim(pieces, pair ^ step, 1, 1) for step in reversed(range(pairs))], 1
    )
    both = []
    for wanted in (1 - parity, parity):
        chosen = lax.dynamic_index_in_dim(ordered, wanted, 2, keepdims=False)
        chosen = jnp.moveaxis(chosen, 1, 0)
        both.append((chosen[:1], chosen[1:2], chosen[2:]))
    return both


def exchange(sends, keeps):
    count = lax.axis_size("depth")
    me = lax.axis_index("depth")
    parity, pair = me % 2, me // 2
    pairs = count // 2
    parts = [None] * pairs
    for half, (send, keep) in enumerate(zip(sends, keeps)):
        owned, columns = send.shape[2:]
        got = swap(send, "depth", 0)
        joined = jnp.where(parity == 0, over(keep, got), over(got, keep))
        for place in range(send.shape[0]):
            step = pairs - 1 - half - place
            piece = joined[place]
            if step:
                piece = lax.ppermute(piece, "depth", [(i, i ^ (2 * step)) for i in range(count)])
            parts[step] = piece
    result = jnp.zeros((3, owned, columns), jnp.float32)
    through = jnp.ones((1, owned, columns), jnp.float32)
    for step in range(pairs):
        ahead = jnp.ones((1, owned, columns), jnp.float32)
        for other in range(pairs):
            if other != step:
                nearer = (pair ^ other) < (pair ^ step)
                ahead = ahead * jnp.where(nearer, parts[other][3:], 1.0)
        result = result + ahead * parts[step][:3]
        through = through * parts[step][3:]
    total, tilted, green = 0.225 * result[:1], 0.225 * result[1:2], 0.45 * result[2:]
    return jnp.concatenate([total + tilted, green, total - tilted, 1.0 - through], 0)


def local(counts):
    slab, rows, columns = counts.shape
    img, depth = lax.axis_index("img"), lax.axis_index("depth")
    imgs, depths = lax.axis_size("img"), lax.axis_size("depth")
    scale = 1.5 / (slab * depths)
    row_odd, depth_odd = img % 2, depth % 2
    first_a, first_b = (1 - depth_odd) * (slab - REACH), depth_odd * (slab - REACH)
    row_a, row_b = (1 - row_odd) * (rows - PAD), row_odd * (rows - PAD)
    where = jnp.stack([first_a, first_b, row_a, row_b])
    order = jnp.stack([1 - row_odd, depth_odd, depth // 2])
    one = jnp.float32(1.0)
    flags = jnp.stack(
        [(img > 0) * one, (img < imgs - 1) * one, (depth > 0) * one, (depth < depths - 1) * one]
    )
    by = jnp.asarray(column_matrices(columns))
    lx = jnp.asarray(row_matrices(rows))
    held = pltpu.with_memory_space_constraint(counts, pltpu.HBM)
    block_b = call_pack_block(where, held)
    side_b, edge_a, mid_a, side_a = call_pack_rest(where, held)
    block_b = swap(block_b, "depth", 1)
    xb = swap(side_b, "img", 1)
    edge_a = swap(edge_a, "depth", 0)
    mid_a = swap(mid_a, "depth", 0)
    xa = swap(side_a, "img", 0)

    def corner(far):
        of_a = lax.dynamic_slice_in_dim(edge_a, far * PAD, PAD, 1)
        of_b = lax.dynamic_slice_in_dim(block_b, far * (rows - PAD), PAD, 1)
        return jnp.concatenate([of_a, of_b], 0)

    ca = swap(corner(1 - row_odd), "img", 0)
    cb = swap(corner(row_odd), "img", 1)
    partial = call_smooth(held, by, jnp.asarray(own_matrix(rows)))
    plane, smoothed = call_depth(
        flags, order, partial, xa, xb, by, jnp.asarray(side_matrices(rows))
    )
    inner = call_interior(scale, smoothed)
    owned = rows // depths
    split = (depths // 2, owned // 8) if owned % 8 == 0 else None
    common = (flags, order, plane, smoothed)
    layers = call_first_edge(
        scale, *common, block_b, ca[REACH:], cb[REACH:], by, lx, inner
    )
    mid_a = pltpu.with_memory_space_constraint(mid_a, pltpu.HBM)
    *sends, ends = call_last_edge(
        scale, split, *common, mid_a, edge_a, ca[:REACH], cb[:REACH], by, lx, layers
    )
    if split:
        last = (order, ends, layers)
        sends += [call_part_edge(scale, split, part, False, *last) for part in (1, 2)]
        keeps = [call_part_edge(scale, split, part, True, *last) for part in range(3)]
    else:
        sends, keeps = halves_of(sends[0])
    return exchange(sends, keeps)


def solution(mesh):
    in_specs = (P("depth", "img", None),)
    out_specs = P(None, ("img", "depth"), None)
    return jax.shard_map(local, mesh=mesh, in_specs=in_specs, out_specs=out_specs, check_vma=False)
```

```python
import functools
import math

import jax
import jax.numpy as jnp
import numpy as np
from jax import lax
from jax.experimental import pallas as pl
from jax.experimental.pallas import tpu as pltpu
from jax.sharding import PartitionSpec as P


gauss_taps = [
    math.exp(-offset * offset / 8.0)
    / sum((math.exp(-other * other / 8.0) for other in range(-4, 5)))
    for offset in range(-4, 5)
]
light_z = 0.48
light_x = 0.6
light_y = 0.64


REACH = 5
SIDE_GROUP = 4
PAD = 8


def band(size):
    index = np.arange(size)
    apart = np.abs(index[:, None] - index[None, :])
    taps = np.array(gauss_taps[4:] + [0.0], np.float64)
    return taps[np.minimum(apart, 5)]


def split_terms(matrix):
    high = matrix.astype(jnp.bfloat16)
    low = (matrix - high.astype(np.float64)).astype(jnp.bfloat16)
    return high, low


def column_matrices(columns):
    return np.concatenate(split_terms(band(columns)), 0)


def row_terms(matrix):
    high, low = split_terms(matrix)
    return np.concatenate([high, high, low], 1)


def row_orders(rows):
    full = band(rows + 2 * PAD)
    order = np.arange(rows + 2 * PAD)
    swapped = np.concatenate([order[rows + PAD :], order[PAD : rows + PAD], order[:PAD]])
    return [full[:, order], full[:, swapped]]


def row_matrices(rows):
    return np.stack([row_terms(matrix) for matrix in row_orders(rows)])


def own_matrix(rows):
    return row_terms(band(rows + 2 * PAD)[:, PAD : rows + PAD])


def side_matrices(rows):
    both = []
    for matrix in row_orders(rows):
        sides = np.concatenate([matrix[:, :PAD], matrix[:, rows + PAD :]], 1)
        touched = np.concatenate([sides[: 2 * PAD], sides[rows:]], 0)
        both.append(row_terms(np.kron(np.eye(SIDE_GROUP), touched)))
    return np.stack(both)


def two_terms(value, high, low):
    return jnp.dot(value, high, preferred_element_type=jnp.float32) + jnp.dot(
        value, low, preferred_element_type=jnp.float32
    )


def smooth_columns(exact, by):
    half = by.shape[0] // 2
    return two_terms(exact, by[:half], by[half:])


def column_terms(counts, by):
    exact = jnp.concatenate([c.astype(jnp.float32).astype(jnp.bfloat16) for c in counts], 0)
    wide = smooth_columns(exact, by)
    high = wide.astype(jnp.bfloat16)
    return high, (wide - high.astype(jnp.float32)).astype(jnp.bfloat16)


def row_product(matrix, high, low):
    stacked = jnp.concatenate([high, low, high], 0)
    return jnp.dot(matrix, stacked, preferred_element_type=jnp.float32)


def smooth_plane(counts, by, lx):
    rows = counts[0].shape[0]
    high, low = column_terms(counts, by)
    parts = [slice(n * rows, (n + 1) * rows) for n in range(len(counts))]
    return [row_product(lx, high[part], low[part]) for part in parts]


def smooth_depth(read, k):
    total = gauss_taps[4] * read(k)
    for offset in range(1, 5):
        total = total + gauss_taps[4 + offset] * (read(k - offset) + read(k + offset))
    return total


def smooth_depth_layers(flags, read, ks, tiles, write):
    for tile in range(tiles):
        rows = pl.ds(tile * 8, 8)
        for n, k in enumerate(ks):
            value = smooth_depth(lambda j: read(j, rows), k)
            if tile == 0:
                value = value * flags[0]
            if tile == tiles - 1:
                value = value * flags[1]
            write(n, rows, value)


def beside(mid, step):
    lanes = 128
    lane = lax.broadcasted_iota(jnp.int32, (mid.shape[0], lanes), 1)
    parts = [mid[:, at : at + lanes] for at in range(0, mid.shape[1], lanes)]
    turned = [pltpu.roll(part, lanes - 1 if step == 1 else 1, 1) for part in parts]
    zero = jnp.zeros_like(parts[0])
    if step == 1:
        return jnp.concatenate(
            [jnp.where(lane == lanes - 1, y, x) for x, y in zip(turned, turned[1:] + [zero])], 1
        )
    return jnp.concatenate(
        [jnp.where(lane == 0, y, x) for x, y in zip(turned, [zero] + turned[:-1])], 1
    )


def render_layer(layer, k, base, carry, scale):
    total, tilted, green, transmit = carry
    rows = pl.ds(base, 8)
    mid = layer(k, rows)
    before = layer(k, pl.ds(base - 8, 8))
    after = layer(k, pl.ds(base + 8, 8))
    sub = lax.broadcasted_iota(jnp.int32, mid.shape, 0)
    above = pltpu.roll(jnp.where(sub == 7, before, mid), 1, 0)
    below = pltpu.roll(jnp.where(sub == 0, after, mid), 7, 0)
    dz = layer(k + 1, rows) - layer(k - 1, rows)
    dx = below - above
    dy = beside(mid, 1) - beside(mid, -1)
    slope = (1.5 * light_z) * dz + (1.5 * light_x) * dx + (1.5 * light_y) * dy
    shading = jnp.tanh(slope) + (0.55 / 0.45)
    gradient_sq4 = dz * dz + dx * dx + dy * dy
    square = mid * mid
    optical = (square / (1.0 + square)) * (1.0 + gradient_sq4)
    centred = mid - 2.5
    log2e = math.log2(math.e)
    remaining = transmit * jnp.exp2(optical * (-scale * log2e))
    lit = (transmit - remaining) * shading
    return (
        total + lit,
        tilted + lit * jnp.tanh(centred),
        green + lit * jnp.exp2((centred * -log2e) * centred),
        remaining,
    )


def empty_carry(columns):
    zero = jnp.zeros((8, columns), jnp.float32)
    return zero, zero, zero, jnp.ones_like(zero)


def read_tile(ref, tile):
    rows = pl.ds(pl.multiple_of(tile * 8, 8), 8)
    return tuple(ref[n, rows, :] for n in range(4))


def store_tile(ref, tile, values):
    rows = pl.ds(pl.multiple_of(tile * 8, 8), 8)
    for n, value in enumerate(values):
        ref[n, rows, :] = value


def run_copies(copies):
    for copy in copies:
        copy.start()
    for copy in copies:
        copy.wait()


def run_copies(pairs, sems):
    copies = [pltpu.make_async_copy(*pair, sems.at[n]) for n, pair in enumerate(pairs)]
    for copy in copies:
        copy.start()
    for copy in copies:
        copy.wait()


def pack_block_kernel(where, c, block, sems):
    run_copies([(c.at[where[1] + n], block.at[n]) for n in range(REACH)], sems)


def pack_rest_kernel(where, c, side_b, edge, middle, side_a, sems):
    rows = c.shape[1]
    layers = pl.ds(where[0], REACH)
    pairs = [
        (c.at[:, pl.ds(pl.multiple_of(where[2 + n], PAD), PAD)], side)
        for n, side in enumerate((side_a, side_b))
    ]
    pairs.append((c.at[layers, pl.ds(0, PAD)], edge.at[:, pl.ds(0, PAD)]))
    pairs.append((c.at[layers, pl.ds(rows - PAD, PAD)], edge.at[:, pl.ds(PAD, PAD)]))
    pairs.append((c.at[layers, pl.ds(PAD, rows - 2 * PAD)], middle))
    run_copies(pairs, sems)


def smooth_kernel(group, c_hbm, by, lx, plane, c, sems):
    groups = c.shape[0] // group

    def fetch(g):
        part = pl.ds(g * group, group)
        return pltpu.make_async_copy(c_hbm.at[part], c.at[part], sems.at[g])

    for g in range(groups):
        fetch(g).start()

    def smooth_group(g, _):
        first = g * group
        fetch(g).wait()
        counts = [c[first + n] for n in range(group)]
        for n, value in enumerate(smooth_plane(counts, by, lx[...])):
            plane[first + n] = value
        return 0

    lax.fori_loop(0, groups, smooth_group, 0)


def depth_kernel(flags, order, partial, xa, xb, by, lx, plane, smoothed):
    layers, ext, _ = plane.shape
    group = 4 * SIDE_GROUP
    edge = 2 * PAD
    sides = lx[order[0]]

    def add_sides(g, _):
        first = g * group
        counts = [jnp.concatenate([xa[first + n], xb[first + n]], 0) for n in range(group)]
        high, low = column_terms(counts, by)
        for half in range(4):
            part = slice(half * SIDE_GROUP * edge, (half + 1) * SIDE_GROUP * edge)
            added = row_product(sides, high[part], low[part])
            for n in range(SIDE_GROUP):
                k = first + half * SIDE_GROUP + n
                at = n * 2 * edge
                plane[k, :edge, :] = partial[k, :edge, :] + added[at : at + edge]
                plane[k, ext - edge :, :] = (
                    partial[k, ext - edge :, :] + added[at + edge : at + 2 * edge]
                )
        return 0

    lax.fori_loop(0, layers // group, add_sides, 0)

    together = 2 if layers % 2 == 0 else 1

    def some_layers(m, _):
        first = m * together

        def write(n, rows, value):
            smoothed[first + n, rows, :] = value

        ks = [first + n + 4 for n in range(together)]
        smooth_depth_layers(flags, lambda k, rows: plane[k, rows, :], ks, ext // 8, write)
        return 0

    lax.fori_loop(0, (layers - 8) // together, some_layers, 0)


def interior_kernel(scale, smoothed, image):
    held, ext, columns = smoothed.shape

    def one_tile(tile, _):
        base = pl.multiple_of(tile * 8 + 8, 8)
        carry = empty_carry(columns)
        for k in range(1, held - 1):
            carry = render_layer(lambda k, rows: smoothed[k, rows, :], k, base, carry, scale)
        store_tile(image, tile, carry)
        return 0

    lax.fori_loop(0, ext // 8 - 2, one_tile, 0)


def edge_smooth(turn, flags, order, plane, smoothed, planes, ends, halo):
    layers, ext, _ = plane.shape
    is_front = order[1] == 1 - turn
    sign = jnp.where(is_front, 1, -1)
    for j, value in enumerate(planes):
        halo[j] = value
    plane_face = jnp.where(is_front, 0, layers - 1)
    halo_face = jnp.where(is_front, REACH, -1)
    ends_face = jnp.where(is_front, 1, REACH)
    smoothed_face = jnp.where(is_front, -4, layers - 5)
    on_grid = jnp.where(is_front, flags[2], flags[3])

    def counted(v, rows):
        if v < 0:
            return halo[halo_face + sign * v, rows, :]
        return plane[plane_face + sign * v, rows, :]

    def write(n, rows, value):
        ends[ends_face + sign * (n - 1), rows, :] = value * on_grid if n == 0 else value

    smooth_depth_layers(flags, counted, range(-1, 4), ext // 8, write)
    for v in (4, 5):
        ends[ends_face + sign * v] = smoothed[smoothed_face + sign * v]


def edge_render(scale, is_front, ends, behind, image, tiles, tile_of, first=0):
    columns = ends.shape[2]

    def one_tile(place):
        tile = tile_of(place + first)
        base = pl.multiple_of(tile * 8 + 8, 8)
        carry = empty_carry(columns)
        for k in range(1, REACH + 1):
            carry = render_layer(lambda k, rows: ends[k, rows, :], k, base, carry, scale)
        other = read_tile(behind, tile)
        front = [jnp.where(is_front, x, y) for x, y in zip(carry, other)]
        back = [jnp.where(is_front, y, x) for x, y in zip(carry, other)]
        colors = [front[n] + front[3] * back[n] for n in range(3)]
        colors.append(front[3] * back[3])
        if len(image.shape) == 3:
            store_tile(image, place, colors)
        else:
            owner_tiles = image.shape[2] // 8
            store_tile(image.at[place // owner_tiles], place % owner_tiles, colors)

    together = 2 if tiles % 2 == 0 else 1

    def some_tiles(n, _):
        for m in range(together):
            one_tile(n * together + m)
        return 0

    lax.fori_loop(0, tiles // together, some_tiles, 0)


def half_tiles(order, pairs, owner_tiles, wanted):
    def tile_of(place):
        pair = order[2] ^ (pairs - 1 - place // owner_tiles)
        return (2 * pair + wanted) * owner_tiles + place % owner_tiles

    return tile_of


def first_edge_kernel(scale, flags, order, plane, smoothed, block, ca, cb, by, lx, behind, image,
                      ends, halo):
    counts = [jnp.concatenate([ca[j], block[j], cb[j]], 0) for j in range(REACH)]
    planes = smooth_plane(counts, by, lx[order[0]])
    edge_smooth(1, flags, order, plane, smoothed, planes, ends, halo)
    tiles = plane.shape[1] // 8 - 2
    edge_render(scale, order[1] == 0, ends, behind, image, tiles, lambda place: place)


def render_half(scale, is_front, ends, behind, image, tile_of, half):
    places, _, owned, _ = image.shape
    owner_tiles = owned // 8
    first = half * owner_tiles
    edge_render(scale, is_front, ends, behind, image, places * owner_tiles, tile_of, first)


def last_edge_kernel(scale, split, flags, order, plane, smoothed, middle_any, edge, ca, cb,
                     by, lx, behind, *refs):
    images, (ends, halo, middle, sem) = refs[:-4], refs[-4:]
    fetch = pltpu.make_async_copy(middle_any, middle, sem.at[0])
    fetch.start()
    two = 2 * PAD
    outer = [
        jnp.concatenate([ca[j], edge[j, :PAD], edge[j, PAD:], cb[j]], 0) for j in range(REACH)
    ]
    outer = column_terms(outer, by)
    fetch.wait()
    inner = column_terms([middle[j] for j in range(REACH)], by)
    rows = middle.shape[1]
    planes = []
    for j in range(REACH):
        high, low = (
            jnp.concatenate(
                [
                    out[2 * two * j : 2 * two * j + two],
                    mid[rows * j : rows * (j + 1)],
                    out[2 * two * j + two : 2 * two * (j + 1)],
                ],
                0,
            )
            for out, mid in zip(outer, inner)
        )
        planes.append(row_product(lx[order[0]], high, low))
    edge_smooth(0, flags, order, plane, smoothed, planes, ends, halo)
    if split:
        tile_of = half_tiles(order, *split, 1 - order[1])
        for part, image in enumerate(images):
            render_half(scale, order[1] == 1, ends, behind, image, tile_of, part)
    else:
        tiles = plane.shape[1] // 8 - 2
        edge_render(scale, order[1] == 1, ends, behind, images[0], tiles, lambda place: place)


def part_edge_kernel(scale, split, parts, order, ends, behind, *images):
    for (kept, part), image in zip(parts, images):
        tile_of = half_tiles(order, *split, order[1] if kept else 1 - order[1])
        render_half(scale, order[1] == 1, ends, behind, image, tile_of, part)


def whole(count):
    return [pl.BlockSpec(memory_space=pltpu.VMEM)] * count


def smem():
    return pl.BlockSpec(memory_space=pltpu.SMEM)


def in_hbm():
    return pl.BlockSpec(memory_space=pltpu.HBM)


def params(mib):
    return pltpu.CompilerParams(vmem_limit_bytes=mib * 1024 * 1024)


def cost(flops):
    return pl.CostEstimate(flops=flops, transcendentals=0, bytes_accessed=4_000_000)


def call_pack_block(where, c):
    _, rows, columns = c.shape
    return pl.pallas_call(
        pack_block_kernel,
        out_shape=jax.ShapeDtypeStruct((REACH, rows, columns), c.dtype),
        in_specs=[smem(), in_hbm()],
        out_specs=whole(1)[0],
        scratch_shapes=[pltpu.SemaphoreType.DMA((REACH,))],
        compiler_params=params(8),
        name="pack_block",
    )(where, c)


def call_pack_rest(where, c):
    layers, rows, columns = c.shape
    edge = jax.ShapeDtypeStruct((REACH, 2 * PAD, columns), c.dtype)
    side = jax.ShapeDtypeStruct((layers, PAD, columns), c.dtype)
    middle = jax.ShapeDtypeStruct((REACH, rows - 2 * PAD, columns), c.dtype)
    return pl.pallas_call(
        pack_rest_kernel,
        out_shape=(side, edge, middle, side),
        in_specs=[smem(), in_hbm()],
        out_specs=tuple(whole(4)),
        scratch_shapes=[pltpu.SemaphoreType.DMA((5,))],
        compiler_params=params(8),
        name="pack_rest",
    )(where, c)


def call_smooth(c, by, lx):
    layers, rows, columns = c.shape
    ext = rows + 2 * PAD
    group = 8
    return pl.pallas_call(
        functools.partial(smooth_kernel, group),
        out_shape=jax.ShapeDtypeStruct((layers, ext, columns), jnp.float32),
        in_specs=[in_hbm()] + whole(2),
        out_specs=whole(1)[0],
        scratch_shapes=[
            pltpu.VMEM((layers, rows, columns), jnp.int32),
            pltpu.SemaphoreType.DMA((layers // group,)),
        ],
        compiler_params=params(16),
        cost_estimate=cost(1_000_000_000),
        name="smooth",
    )(c, by, lx)


def call_depth(flags, order, partial, *operands):
    layers, ext, columns = partial.shape
    return pl.pallas_call(
        depth_kernel,
        out_shape=(
            jax.ShapeDtypeStruct(partial.shape, jnp.float32),
            jax.ShapeDtypeStruct((layers - 8, ext, columns), jnp.float32),
        ),
        in_specs=[smem(), smem()] + whole(1 + len(operands)),
        out_specs=tuple(whole(2)),
        input_output_aliases={2: 0},
        compiler_params=params(12),
        cost_estimate=cost(500_000_000),
        name="depth",
    )(flags, order, partial, *operands)


def call_interior(scale, smoothed):
    _, ext, columns = smoothed.shape
    return pl.pallas_call(
        functools.partial(interior_kernel, scale),
        out_shape=jax.ShapeDtypeStruct((4, ext - 2 * PAD, columns), jnp.float32),
        in_specs=whole(1),
        out_specs=whole(1)[0],
        compiler_params=params(12),
        cost_estimate=cost(1_000_000_000),
        name="interior",
    )(smoothed)


def call_first_edge(scale, flags, order, plane, *operands):
    _, ext, columns = plane.shape
    f32 = jnp.float32
    return pl.pallas_call(
        functools.partial(first_edge_kernel, scale),
        out_shape=jax.ShapeDtypeStruct((4, ext - 2 * PAD, columns), f32),
        in_specs=[smem(), smem()] + whole(1 + len(operands)),
        out_specs=whole(1)[0],
        scratch_shapes=[
            pltpu.VMEM((REACH + 2, ext, columns), f32),
            pltpu.VMEM((REACH, ext, columns), f32),
        ],
        compiler_params=params(24),
        cost_estimate=cost(300_000_000),
        name="first_edge",
    )(flags, order, plane, *operands)


def part_sizes(pairs):
    return 1, 1, pairs - 2


def part_shape(split, part, columns):
    pairs, owner_tiles = split
    return part_sizes(pairs)[part], 4, owner_tiles * 8, columns


def call_last_edge(scale, split, flags, order, plane, *operands):
    _, ext, columns = plane.shape
    f32 = jnp.float32
    rows = ext - 2 * PAD
    images = [(4, rows, columns)]
    if split:
        images = [part_shape(split, part, columns) for part in range(2)]
    shapes = [*images, (REACH + 2, ext, columns)]
    return pl.pallas_call(
        functools.partial(last_edge_kernel, scale, split),
        out_shape=tuple(jax.ShapeDtypeStruct(shape, f32) for shape in shapes),
        in_specs=[smem(), smem()] + whole(2) + [in_hbm()] + whole(len(operands) - 2),
        out_specs=tuple(whole(len(shapes))),
        scratch_shapes=[
            pltpu.VMEM((REACH, ext, columns), f32),
            pltpu.VMEM(operands[1].shape, operands[1].dtype),
            pltpu.SemaphoreType.DMA((1,)),
        ],
        compiler_params=params(12),
        cost_estimate=cost(300_000_000),
        name="last_edge",
    )(flags, order, plane, *operands)


def call_part_edge(scale, split, parts, order, ends, behind):
    shapes = [part_shape(split, part, ends.shape[2]) for _, part in parts]
    return pl.pallas_call(
        functools.partial(part_edge_kernel, scale, split, parts),
        out_shape=tuple(jax.ShapeDtypeStruct(shape, jnp.float32) for shape in shapes),
        in_specs=[smem()] + whole(2),
        out_specs=tuple(whole(len(shapes))),
        compiler_params=params(12),
        cost_estimate=cost(200_000_000),
    )(order, ends, behind)


def swap(value, axis, first):
    count = lax.axis_size(axis)
    pairs = []
    for low in range(first, count - 1, 2):
        pairs += [(low, low + 1), (low + 1, low)]
    return lax.ppermute(value, axis, pairs)


def over(front, back):
    through = front[:, 3:]
    return jnp.concatenate([front[:, :3] + through * back[:, :3], through * back[:, 3:]], 1)


def halves_of(layers):
    count = lax.axis_size("depth")
    me = lax.axis_index("depth")
    parity, pair, pairs = me % 2, me // 2, count // 2
    _, rows, columns = layers.shape
    pieces = layers.reshape(4, pairs, 2, rows // count, columns)
    ordered = jnp.concatenate(
        [lax.dynamic_slice_in_dim(pieces, pair ^ step, 1, 1) for step in reversed(range(pairs))], 1
    )
    both = []
    for wanted in (1 - parity, parity):
        chosen = lax.dynamic_index_in_dim(ordered, wanted, 2, keepdims=False)
        chosen = jnp.moveaxis(chosen, 1, 0)
        both.append((chosen[:1], chosen[1:2], chosen[2:]))
    return both


def exchange(sends, keeps):
    count = lax.axis_size("depth")
    me = lax.axis_index("depth")
    parity, pair = me % 2, me // 2
    pairs = count // 2
    parts = [None] * pairs
    for half, (send, keep) in enumerate(zip(sends, keeps)):
        owned, columns = send.shape[2:]
        got = swap(send, "depth", 0)
        joined = jnp.where(parity == 0, over(keep, got), over(got, keep))
        for place in range(send.shape[0]):
            step = pairs - 1 - half - place
            piece = joined[place]
            if step:
                piece = lax.ppermute(piece, "depth", [(i, i ^ (2 * step)) for i in range(count)])
            parts[step] = piece
    result = jnp.zeros((3, owned, columns), jnp.float32)
    through = jnp.ones((1, owned, columns), jnp.float32)
    for step in range(pairs):
        ahead = jnp.ones((1, owned, columns), jnp.float32)
        for other in range(pairs):
            if other != step:
                nearer = (pair ^ other) < (pair ^ step)
                ahead = ahead * jnp.where(nearer, parts[other][3:], 1.0)
        result = result + ahead * parts[step][:3]
        through = through * parts[step][3:]
    total, tilted, green = 0.225 * result[:1], 0.225 * result[1:2], 0.45 * result[2:]
    return jnp.concatenate([total + tilted, green, total - tilted, 1.0 - through], 0)


def local(counts):
    slab, rows, columns = counts.shape
    img, depth = lax.axis_index("img"), lax.axis_index("depth")
    imgs, depths = lax.axis_size("img"), lax.axis_size("depth")
    scale = 1.5 / (slab * depths)
    row_odd, depth_odd = img % 2, depth % 2
    first_a, first_b = (1 - depth_odd) * (slab - REACH), depth_odd * (slab - REACH)
    row_a, row_b = (1 - row_odd) * (rows - PAD), row_odd * (rows - PAD)
    where = jnp.stack([first_a, first_b, row_a, row_b])
    order = jnp.stack([1 - row_odd, depth_odd, depth // 2])
    one = jnp.float32(1.0)
    flags = jnp.stack(
        [(img > 0) * one, (img < imgs - 1) * one, (depth > 0) * one, (depth < depths - 1) * one]
    )
    by = jnp.asarray(column_matrices(columns))
    lx = jnp.asarray(row_matrices(rows))
    held = pltpu.with_memory_space_constraint(counts, pltpu.HBM)
    block_b = call_pack_block(where, held)
    side_b, edge_a, mid_a, side_a = call_pack_rest(where, held)
    block_b = swap(block_b, "depth", 1)
    xb = swap(side_b, "img", 1)
    edge_a = swap(edge_a, "depth", 0)
    mid_a = swap(mid_a, "depth", 0)
    xa = swap(side_a, "img", 0)

    def corner(far):
        of_a = lax.dynamic_slice_in_dim(edge_a, far * PAD, PAD, 1)
        of_b = lax.dynamic_slice_in_dim(block_b, far * (rows - PAD), PAD, 1)
        return jnp.concatenate([of_a, of_b], 0)

    ca = swap(corner(1 - row_odd), "img", 0)
    cb = swap(corner(row_odd), "img", 1)
    partial = call_smooth(held, by, jnp.asarray(own_matrix(rows)))
    plane, smoothed = call_depth(
        flags, order, partial, xa, xb, by, jnp.asarray(side_matrices(rows))
    )
    inner = call_interior(scale, smoothed)
    owned = rows // depths
    split = (depths // 2, owned // 8) if owned % 8 == 0 else None
    common = (flags, order, plane, smoothed)
    layers = call_first_edge(
        scale, *common, block_b, ca[REACH:], cb[REACH:], by, lx, inner
    )
    mid_a = pltpu.with_memory_space_constraint(mid_a, pltpu.HBM)
    *sends, ends = call_last_edge(
        scale, split, *common, mid_a, edge_a, ca[:REACH], cb[:REACH], by, lx, layers
    )
    if split:
        last = (order, ends, layers)
        sent_2, kept_0 = call_part_edge(scale, split, ((False, 2), (True, 0)), *last)
        (kept_1,) = call_part_edge(scale, split, ((True, 1),), *last)
        (kept_2,) = call_part_edge(scale, split, ((True, 2),), *last)
        sends.append(sent_2)
        keeps = [kept_0, kept_1, kept_2]
    else:
        sends, keeps = halves_of(sends[0])
    return exchange(sends, keeps)


def solution(mesh):
    in_specs = (P("depth", "img", None),)
    out_specs = P(None, ("img", "depth"), None)
    return jax.shard_map(local, mesh=mesh, in_specs=in_specs, out_specs=out_specs, check_vma=False)
```

```python
import functools
import math

import jax
import jax.numpy as jnp
import numpy as np
from jax import lax
from jax.experimental import pallas as pl
from jax.experimental.pallas import tpu as pltpu
from jax.sharding import PartitionSpec as P


gauss_taps = [
    math.exp(-offset * offset / 8.0)
    / sum((math.exp(-other * other / 8.0) for other in range(-4, 5)))
    for offset in range(-4, 5)
]
light_z = 0.48
light_x = 0.6
light_y = 0.64


REACH = 5
SIDE_GROUP = 4
PAD = 8


def band(size):
    index = np.arange(size)
    apart = np.abs(index[:, None] - index[None, :])
    taps = np.array(gauss_taps[4:] + [0.0], np.float64)
    return taps[np.minimum(apart, 5)]


def split_terms(matrix):
    high = matrix.astype(jnp.bfloat16)
    low = (matrix - high.astype(np.float64)).astype(jnp.bfloat16)
    return high, low


def column_matrices(columns):
    return np.concatenate(split_terms(band(columns)), 0)


def row_terms(matrix):
    high, low = split_terms(matrix)
    return np.concatenate([high, high, low], 1)


def row_orders(rows):
    full = band(rows + 2 * PAD)
    order = np.arange(rows + 2 * PAD)
    swapped = np.concatenate([order[rows + PAD :], order[PAD : rows + PAD], order[:PAD]])
    return [full[:, order], full[:, swapped]]


def row_matrices(rows):
    return np.stack([row_terms(matrix) for matrix in row_orders(rows)])


def own_matrix(rows):
    return row_terms(band(rows + 2 * PAD)[:, PAD : rows + PAD])


def side_matrices(rows):
    both = []
    for matrix in row_orders(rows):
        sides = np.concatenate([matrix[:, :PAD], matrix[:, rows + PAD :]], 1)
        touched = np.concatenate([sides[: 2 * PAD], sides[rows:]], 0)
        both.append(row_terms(np.kron(np.eye(SIDE_GROUP), touched)))
    return np.stack(both)


def two_terms(value, high, low):
    return jnp.dot(value, high, preferred_element_type=jnp.float32) + jnp.dot(
        value, low, preferred_element_type=jnp.float32
    )


def smooth_columns(exact, by):
    half = by.shape[0] // 2
    return two_terms(exact, by[:half], by[half:])


def column_terms(counts, by):
    exact = jnp.concatenate([c.astype(jnp.float32).astype(jnp.bfloat16) for c in counts], 0)
    wide = smooth_columns(exact, by)
    high = wide.astype(jnp.bfloat16)
    return high, (wide - high.astype(jnp.float32)).astype(jnp.bfloat16)


def row_product(matrix, high, low):
    stacked = jnp.concatenate([high, low, high], 0)
    return jnp.dot(matrix, stacked, preferred_element_type=jnp.float32)


def smooth_plane(counts, by, lx):
    rows = counts[0].shape[0]
    high, low = column_terms(counts, by)
    parts = [slice(n * rows, (n + 1) * rows) for n in range(len(counts))]
    return [row_product(lx, high[part], low[part]) for part in parts]


def smooth_depth(read, k):
    total = gauss_taps[4] * read(k)
    for offset in range(1, 5):
        total = total + gauss_taps[4 + offset] * (read(k - offset) + read(k + offset))
    return total


def smooth_depth_layers(flags, read, ks, tiles, write):
    for tile in range(tiles):
        rows = pl.ds(tile * 8, 8)
        for n, k in enumerate(ks):
            value = smooth_depth(lambda j: read(j, rows), k)
            if tile == 0:
                value = value * flags[0]
            if tile == tiles - 1:
                value = value * flags[1]
            write(n, rows, value)


def beside(mid, step):
    lanes = 128
    lane = lax.broadcasted_iota(jnp.int32, (mid.shape[0], lanes), 1)
    parts = [mid[:, at : at + lanes] for at in range(0, mid.shape[1], lanes)]
    turned = [pltpu.roll(part, lanes - 1 if step == 1 else 1, 1) for part in parts]
    zero = jnp.zeros_like(parts[0])
    if step == 1:
        return jnp.concatenate(
            [jnp.where(lane == lanes - 1, y, x) for x, y in zip(turned, turned[1:] + [zero])], 1
        )
    return jnp.concatenate(
        [jnp.where(lane == 0, y, x) for x, y in zip(turned, [zero] + turned[:-1])], 1
    )


def render_layer(layer, k, base, carry, scale):
    total, tilted, green, transmit = carry
    rows = pl.ds(base, 8)
    mid = layer(k, rows)
    before = layer(k, pl.ds(base - 8, 8))
    after = layer(k, pl.ds(base + 8, 8))
    sub = lax.broadcasted_iota(jnp.int32, mid.shape, 0)
    above = pltpu.roll(jnp.where(sub == 7, before, mid), 1, 0)
    below = pltpu.roll(jnp.where(sub == 0, after, mid), 7, 0)
    dz = layer(k + 1, rows) - layer(k - 1, rows)
    dx = below - above
    dy = beside(mid, 1) - beside(mid, -1)
    slope = (1.5 * light_z) * dz + (1.5 * light_x) * dx + (1.5 * light_y) * dy
    shading = jnp.tanh(slope) + (0.55 / 0.45)
    gradient_sq4 = dz * dz + dx * dx + dy * dy
    square = mid * mid
    optical = (square / (1.0 + square)) * (1.0 + gradient_sq4)
    centred = mid - 2.5
    log2e = math.log2(math.e)
    remaining = transmit * jnp.exp2(optical * (-scale * log2e))
    lit = (transmit - remaining) * shading
    return (
        total + lit,
        tilted + lit * jnp.tanh(centred),
        green + lit * jnp.exp2((centred * -log2e) * centred),
        remaining,
    )


def empty_carry(columns):
    zero = jnp.zeros((8, columns), jnp.float32)
    return zero, zero, zero, jnp.ones_like(zero)


def read_tile(ref, tile):
    rows = pl.ds(pl.multiple_of(tile * 8, 8), 8)
    return tuple(ref[n, rows, :] for n in range(4))


def store_tile(ref, tile, values):
    rows = pl.ds(pl.multiple_of(tile * 8, 8), 8)
    for n, value in enumerate(values):
        ref[n, rows, :] = value


def run_copies(copies):
    for copy in copies:
        copy.start()
    for copy in copies:
        copy.wait()


def run_copies(pairs, sems):
    copies = [pltpu.make_async_copy(*pair, sems.at[n]) for n, pair in enumerate(pairs)]
    for copy in copies:
        copy.start()
    for copy in copies:
        copy.wait()


def pack_block_kernel(where, c, block, sems):
    run_copies([(c.at[where[1] + n], block.at[n]) for n in range(REACH)], sems)


def pack_rest_kernel(where, c, side_b, edge, middle, side_a, sems):
    rows = c.shape[1]
    layers = pl.ds(where[0], REACH)
    pairs = [
        (c.at[:, pl.ds(pl.multiple_of(where[2 + n], PAD), PAD)], side)
        for n, side in enumerate((side_a, side_b))
    ]
    pairs.append((c.at[layers, pl.ds(0, PAD)], edge.at[:, pl.ds(0, PAD)]))
    pairs.append((c.at[layers, pl.ds(rows - PAD, PAD)], edge.at[:, pl.ds(PAD, PAD)]))
    pairs.append((c.at[layers, pl.ds(PAD, rows - 2 * PAD)], middle))
    run_copies(pairs, sems)


def smooth_kernel(group, c_hbm, by, lx, plane, c, sems):
    groups = c.shape[0] // group

    def fetch(g):
        part = pl.ds(g * group, group)
        return pltpu.make_async_copy(c_hbm.at[part], c.at[part], sems.at[g])

    for g in range(groups):
        fetch(g).start()

    def smooth_group(g, _):
        first = g * group
        fetch(g).wait()
        counts = [c[first + n] for n in range(group)]
        for n, value in enumerate(smooth_plane(counts, by, lx[...])):
            plane[first + n] = value
        return 0

    lax.fori_loop(0, groups, smooth_group, 0)


def depth_kernel(flags, order, partial, xa, xb, by, lx, plane, smoothed):
    layers, ext, _ = plane.shape
    group = 4 * SIDE_GROUP
    edge = 2 * PAD
    sides = lx[order[0]]

    def add_sides(g, _):
        first = g * group
        counts = [jnp.concatenate([xa[first + n], xb[first + n]], 0) for n in range(group)]
        high, low = column_terms(counts, by)
        for half in range(4):
            part = slice(half * SIDE_GROUP * edge, (half + 1) * SIDE_GROUP * edge)
            added = row_product(sides, high[part], low[part])
            for n in range(SIDE_GROUP):
                k = first + half * SIDE_GROUP + n
                at = n * 2 * edge
                plane[k, :edge, :] = partial[k, :edge, :] + added[at : at + edge]
                plane[k, ext - edge :, :] = (
                    partial[k, ext - edge :, :] + added[at + edge : at + 2 * edge]
                )
        return 0

    lax.fori_loop(0, layers // group, add_sides, 0)

    together = 2 if layers % 2 == 0 else 1

    def some_layers(m, _):
        first = m * together

        def write(n, rows, value):
            smoothed[first + n, rows, :] = value

        ks = [first + n + 4 for n in range(together)]
        smooth_depth_layers(flags, lambda k, rows: plane[k, rows, :], ks, ext // 8, write)
        return 0

    lax.fori_loop(0, (layers - 8) // together, some_layers, 0)


def interior_kernel(scale, smoothed, image):
    held, ext, columns = smoothed.shape

    def one_tile(tile, _):
        base = pl.multiple_of(tile * 8 + 8, 8)
        carry = empty_carry(columns)
        for k in range(1, held - 1):
            carry = render_layer(lambda k, rows: smoothed[k, rows, :], k, base, carry, scale)
        store_tile(image, tile, carry)
        return 0

    lax.fori_loop(0, ext // 8 - 2, one_tile, 0)


def edge_smooth(turn, flags, order, plane, smoothed, planes, ends, halo):
    layers, ext, _ = plane.shape
    is_front = order[1] == 1 - turn
    sign = jnp.where(is_front, 1, -1)
    for j, value in enumerate(planes):
        halo[j] = value
    plane_face = jnp.where(is_front, 0, layers - 1)
    halo_face = jnp.where(is_front, REACH, -1)
    ends_face = jnp.where(is_front, 1, REACH)
    smoothed_face = jnp.where(is_front, -4, layers - 5)
    on_grid = jnp.where(is_front, flags[2], flags[3])

    def counted(v, rows):
        if v < 0:
            return halo[halo_face + sign * v, rows, :]
        return plane[plane_face + sign * v, rows, :]

    def write(n, rows, value):
        ends[ends_face + sign * (n - 1), rows, :] = value * on_grid if n == 0 else value

    smooth_depth_layers(flags, counted, range(-1, 4), ext // 8, write)
    for v in (4, 5):
        ends[ends_face + sign * v] = smoothed[smoothed_face + sign * v]


def edge_render(scale, is_front, ends, behind, image, tiles, tile_of, first=0):
    columns = ends.shape[2]

    def one_tile(place):
        tile = tile_of(place + first)
        base = pl.multiple_of(tile * 8 + 8, 8)
        carry = empty_carry(columns)
        for k in range(1, REACH + 1):
            carry = render_layer(lambda k, rows: ends[k, rows, :], k, base, carry, scale)
        other = read_tile(behind, tile)
        front = [jnp.where(is_front, x, y) for x, y in zip(carry, other)]
        back = [jnp.where(is_front, y, x) for x, y in zip(carry, other)]
        colors = [front[n] + front[3] * back[n] for n in range(3)]
        colors.append(front[3] * back[3])
        if len(image.shape) == 3:
            store_tile(image, place, colors)
        else:
            owner_tiles = image.shape[2] // 8
            store_tile(image.at[place // owner_tiles], place % owner_tiles, colors)

    together = 2 if tiles % 2 == 0 else 1

    def some_tiles(n, _):
        for m in range(together):
            one_tile(n * together + m)
        return 0

    lax.fori_loop(0, tiles // together, some_tiles, 0)


def step_at(pairs, index):
    return jnp.where(index < 2, pairs - 2 + index, pairs - 1 - index)


def half_tiles(order, pairs, owner_tiles, wanted):
    def tile_of(place):
        pair = order[2] ^ step_at(pairs, place // owner_tiles)
        return (2 * pair + wanted) * owner_tiles + place % owner_tiles

    return tile_of


def first_edge_kernel(scale, flags, order, plane, smoothed, block, ca, cb, by, lx, behind, image,
                      ends, halo):
    counts = [jnp.concatenate([ca[j], block[j], cb[j]], 0) for j in range(REACH)]
    planes = smooth_plane(counts, by, lx[order[0]])
    edge_smooth(1, flags, order, plane, smoothed, planes, ends, halo)
    tiles = plane.shape[1] // 8 - 2
    edge_render(scale, order[1] == 0, ends, behind, image, tiles, lambda place: place)


def render_half(scale, is_front, ends, behind, image, tile_of, half):
    places, _, owned, _ = image.shape
    owner_tiles = owned // 8
    first = half * owner_tiles
    edge_render(scale, is_front, ends, behind, image, places * owner_tiles, tile_of, first)


def last_edge_kernel(scale, split, flags, order, plane, smoothed, middle_any, edge, ca, cb,
                     by, lx, behind, *refs):
    images, (ends, halo, middle, sem) = refs[:-4], refs[-4:]
    fetch = pltpu.make_async_copy(middle_any, middle, sem.at[0])
    fetch.start()
    two = 2 * PAD
    outer = [
        jnp.concatenate([ca[j], edge[j, :PAD], edge[j, PAD:], cb[j]], 0) for j in range(REACH)
    ]
    outer = column_terms(outer, by)
    fetch.wait()
    inner = column_terms([middle[j] for j in range(REACH)], by)
    rows = middle.shape[1]
    planes = []
    for j in range(REACH):
        high, low = (
            jnp.concatenate(
                [
                    out[2 * two * j : 2 * two * j + two],
                    mid[rows * j : rows * (j + 1)],
                    out[2 * two * j + two : 2 * two * (j + 1)],
                ],
                0,
            )
            for out, mid in zip(outer, inner)
        )
        planes.append(row_product(lx[order[0]], high, low))
    edge_smooth(0, flags, order, plane, smoothed, planes, ends, halo)
    if split:
        tile_of = half_tiles(order, *split, 1 - order[1])
        for part, image in enumerate(images):
            render_half(scale, order[1] == 1, ends, behind, image, tile_of, part)
    else:
        tiles = plane.shape[1] // 8 - 2
        edge_render(scale, order[1] == 1, ends, behind, images[0], tiles, lambda place: place)


def part_edge_kernel(scale, split, parts, order, ends, behind, *images):
    for (kept, part), image in zip(parts, images):
        tile_of = half_tiles(order, *split, order[1] if kept else 1 - order[1])
        render_half(scale, order[1] == 1, ends, behind, image, tile_of, part)


def whole(count):
    return [pl.BlockSpec(memory_space=pltpu.VMEM)] * count


def smem():
    return pl.BlockSpec(memory_space=pltpu.SMEM)


def in_hbm():
    return pl.BlockSpec(memory_space=pltpu.HBM)


def params(mib):
    return pltpu.CompilerParams(vmem_limit_bytes=mib * 1024 * 1024)


def cost(flops):
    return pl.CostEstimate(flops=flops, transcendentals=0, bytes_accessed=4_000_000)


def call_pack_block(where, c):
    _, rows, columns = c.shape
    return pl.pallas_call(
        pack_block_kernel,
        out_shape=jax.ShapeDtypeStruct((REACH, rows, columns), c.dtype),
        in_specs=[smem(), in_hbm()],
        out_specs=whole(1)[0],
        scratch_shapes=[pltpu.SemaphoreType.DMA((REACH,))],
        compiler_params=params(8),
        name="pack_block",
    )(where, c)


def call_pack_rest(where, c):
    layers, rows, columns = c.shape
    edge = jax.ShapeDtypeStruct((REACH, 2 * PAD, columns), c.dtype)
    side = jax.ShapeDtypeStruct((layers, PAD, columns), c.dtype)
    middle = jax.ShapeDtypeStruct((REACH, rows - 2 * PAD, columns), c.dtype)
    return pl.pallas_call(
        pack_rest_kernel,
        out_shape=(side, edge, middle, side),
        in_specs=[smem(), in_hbm()],
        out_specs=tuple(whole(4)),
        scratch_shapes=[pltpu.SemaphoreType.DMA((5,))],
        compiler_params=params(8),
        name="pack_rest",
    )(where, c)


def call_smooth(c, by, lx):
    layers, rows, columns = c.shape
    ext = rows + 2 * PAD
    group = 8
    return pl.pallas_call(
        functools.partial(smooth_kernel, group),
        out_shape=jax.ShapeDtypeStruct((layers, ext, columns), jnp.float32),
        in_specs=[in_hbm()] + whole(2),
        out_specs=whole(1)[0],
        scratch_shapes=[
            pltpu.VMEM((layers, rows, columns), jnp.int32),
            pltpu.SemaphoreType.DMA((layers // group,)),
        ],
        compiler_params=params(16),
        cost_estimate=cost(1_000_000_000),
        name="smooth",
    )(c, by, lx)


def call_depth(flags, order, partial, *operands):
    layers, ext, columns = partial.shape
    return pl.pallas_call(
        depth_kernel,
        out_shape=(
            jax.ShapeDtypeStruct(partial.shape, jnp.float32),
            jax.ShapeDtypeStruct((layers - 8, ext, columns), jnp.float32),
        ),
        in_specs=[smem(), smem()] + whole(1 + len(operands)),
        out_specs=tuple(whole(2)),
        input_output_aliases={2: 0},
        compiler_params=params(12),
        cost_estimate=cost(500_000_000),
        name="depth",
    )(flags, order, partial, *operands)


def call_interior(scale, smoothed):
    _, ext, columns = smoothed.shape
    return pl.pallas_call(
        functools.partial(interior_kernel, scale),
        out_shape=jax.ShapeDtypeStruct((4, ext - 2 * PAD, columns), jnp.float32),
        in_specs=whole(1),
        out_specs=whole(1)[0],
        compiler_params=params(12),
        cost_estimate=cost(1_000_000_000),
        name="interior",
    )(smoothed)


def call_first_edge(scale, flags, order, plane, *operands):
    _, ext, columns = plane.shape
    f32 = jnp.float32
    return pl.pallas_call(
        functools.partial(first_edge_kernel, scale),
        out_shape=jax.ShapeDtypeStruct((4, ext - 2 * PAD, columns), f32),
        in_specs=[smem(), smem()] + whole(1 + len(operands)),
        out_specs=whole(1)[0],
        scratch_shapes=[
            pltpu.VMEM((REACH + 2, ext, columns), f32),
            pltpu.VMEM((REACH, ext, columns), f32),
        ],
        compiler_params=params(24),
        cost_estimate=cost(300_000_000),
        name="first_edge",
    )(flags, order, plane, *operands)


def part_sizes(pairs):
    return 1, 1, pairs - 2


def part_shape(split, part, columns):
    pairs, owner_tiles = split
    return part_sizes(pairs)[part], 4, owner_tiles * 8, columns


def call_last_edge(scale, split, flags, order, plane, *operands):
    _, ext, columns = plane.shape
    f32 = jnp.float32
    rows = ext - 2 * PAD
    images = [(4, rows, columns)]
    if split:
        images = [part_shape(split, part, columns) for part in range(2)]
    shapes = [*images, (REACH + 2, ext, columns)]
    return pl.pallas_call(
        functools.partial(last_edge_kernel, scale, split),
        out_shape=tuple(jax.ShapeDtypeStruct(shape, f32) for shape in shapes),
        in_specs=[smem(), smem()] + whole(2) + [in_hbm()] + whole(len(operands) - 2),
        out_specs=tuple(whole(len(shapes))),
        scratch_shapes=[
            pltpu.VMEM((REACH, ext, columns), f32),
            pltpu.VMEM(operands[1].shape, operands[1].dtype),
            pltpu.SemaphoreType.DMA((1,)),
        ],
        compiler_params=params(12),
        cost_estimate=cost(300_000_000),
        name="last_edge",
    )(flags, order, plane, *operands)


def call_part_edge(scale, split, parts, order, ends, behind):
    shapes = [part_shape(split, part, ends.shape[2]) for _, part in parts]
    return pl.pallas_call(
        functools.partial(part_edge_kernel, scale, split, parts),
        out_shape=tuple(jax.ShapeDtypeStruct(shape, jnp.float32) for shape in shapes),
        in_specs=[smem()] + whole(2),
        out_specs=tuple(whole(len(shapes))),
        compiler_params=params(12),
        cost_estimate=cost(200_000_000),
    )(order, ends, behind)


def swap(value, axis, first):
    count = lax.axis_size(axis)
    pairs = []
    for low in range(first, count - 1, 2):
        pairs += [(low, low + 1), (low + 1, low)]
    return lax.ppermute(value, axis, pairs)


def over(front, back):
    through = front[:, 3:]
    return jnp.concatenate([front[:, :3] + through * back[:, :3], through * back[:, 3:]], 1)


def served(pairs):
    return [pairs - 2, pairs - 1, *reversed(range(pairs - 2))]


def halves_of(layers):
    count = lax.axis_size("depth")
    me = lax.axis_index("depth")
    parity, pair, pairs = me % 2, me // 2, count // 2
    _, rows, columns = layers.shape
    pieces = layers.reshape(4, pairs, 2, rows // count, columns)
    ordered = jnp.concatenate(
        [lax.dynamic_slice_in_dim(pieces, pair ^ step, 1, 1) for step in served(pairs)], 1
    )
    both = []
    for wanted in (1 - parity, parity):
        chosen = lax.dynamic_index_in_dim(ordered, wanted, 2, keepdims=False)
        chosen = jnp.moveaxis(chosen, 1, 0)
        both.append((chosen[:1], chosen[1:2], chosen[2:]))
    return both


def exchange(sends, keeps):
    count = lax.axis_size("depth")
    me = lax.axis_index("depth")
    parity, pair = me % 2, me // 2
    pairs = count // 2
    parts = [None] * pairs
    for half, (send, keep) in enumerate(zip(sends, keeps)):
        owned, columns = send.shape[2:]
        got = swap(send, "depth", 0)
        joined = jnp.where(parity == 0, over(keep, got), over(got, keep))
        for place in range(send.shape[0]):
            step = served(pairs)[half + place]
            piece = joined[place]
            if step:
                piece = lax.ppermute(piece, "depth", [(i, i ^ (2 * step)) for i in range(count)])
            parts[step] = piece
    result = jnp.zeros((3, owned, columns), jnp.float32)
    through = jnp.ones((1, owned, columns), jnp.float32)
    for step in range(pairs):
        ahead = jnp.ones((1, owned, columns), jnp.float32)
        for other in range(pairs):
            if other != step:
                nearer = (pair ^ other) < (pair ^ step)
                ahead = ahead * jnp.where(nearer, parts[other][3:], 1.0)
        result = result + ahead * parts[step][:3]
        through = through * parts[step][3:]
    total, tilted, green = 0.225 * result[:1], 0.225 * result[1:2], 0.45 * result[2:]
    return jnp.concatenate([total + tilted, green, total - tilted, 1.0 - through], 0)


def local(counts):
    slab, rows, columns = counts.shape
    img, depth = lax.axis_index("img"), lax.axis_index("depth")
    imgs, depths = lax.axis_size("img"), lax.axis_size("depth")
    scale = 1.5 / (slab * depths)
    row_odd, depth_odd = img % 2, depth % 2
    first_a, first_b = (1 - depth_odd) * (slab - REACH), depth_odd * (slab - REACH)
    row_a, row_b = (1 - row_odd) * (rows - PAD), row_odd * (rows - PAD)
    where = jnp.stack([first_a, first_b, row_a, row_b])
    order = jnp.stack([1 - row_odd, depth_odd, depth // 2])
    one = jnp.float32(1.0)
    flags = jnp.stack(
        [(img > 0) * one, (img < imgs - 1) * one, (depth > 0) * one, (depth < depths - 1) * one]
    )
    by = jnp.asarray(column_matrices(columns))
    lx = jnp.asarray(row_matrices(rows))
    held = pltpu.with_memory_space_constraint(counts, pltpu.HBM)
    block_b = call_pack_block(where, held)
    side_b, edge_a, mid_a, side_a = call_pack_rest(where, held)
    block_b = swap(block_b, "depth", 1)
    xb = swap(side_b, "img", 1)
    edge_a = swap(edge_a, "depth", 0)
    mid_a = swap(mid_a, "depth", 0)
    xa = swap(side_a, "img", 0)

    def corner(far):
        of_a = lax.dynamic_slice_in_dim(edge_a, far * PAD, PAD, 1)
        of_b = lax.dynamic_slice_in_dim(block_b, far * (rows - PAD), PAD, 1)
        return jnp.concatenate([of_a, of_b], 0)

    ca = swap(corner(1 - row_odd), "img", 0)
    cb = swap(corner(row_odd), "img", 1)
    partial = call_smooth(held, by, jnp.asarray(own_matrix(rows)))
    plane, smoothed = call_depth(
        flags, order, partial, xa, xb, by, jnp.asarray(side_matrices(rows))
    )
    inner = call_interior(scale, smoothed)
    owned = rows // depths
    split = (depths // 2, owned // 8) if owned % 8 == 0 else None
    common = (flags, order, plane, smoothed)
    layers = call_first_edge(
        scale, *common, block_b, ca[REACH:], cb[REACH:], by, lx, inner
    )
    mid_a = pltpu.with_memory_space_constraint(mid_a, pltpu.HBM)
    *sends, ends = call_last_edge(
        scale, split, *common, mid_a, edge_a, ca[:REACH], cb[:REACH], by, lx, layers
    )
    if split:
        last = (order, ends, layers)
        sent_2, kept_0 = call_part_edge(scale, split, ((False, 2), (True, 0)), *last)
        (kept_1,) = call_part_edge(scale, split, ((True, 1),), *last)
        (kept_2,) = call_part_edge(scale, split, ((True, 2),), *last)
        sends.append(sent_2)
        keeps = [kept_0, kept_1, kept_2]
    else:
        sends, keeps = halves_of(sends[0])
    return exchange(sends, keeps)


def solution(mesh):
    in_specs = (P("depth", "img", None),)
    out_specs = P(None, ("img", "depth"), None)
    return jax.shard_map(local, mesh=mesh, in_specs=in_specs, out_specs=out_specs, check_vma=False)
```
